256 devices in a mesh: rep: 16 (over x, z_hi, core), stripe: 16 (over y, z_lo).
Axes of the slice: x: 4, y: 4, z: 8 (z_hi: 2, z_lo: 4; z = z_hi * 4 + z_lo), core: 2. Of those that a mesh axis runs over, the one named last changes fastest.
Arguments:
- activations: bfloat16 [4096, 4096], P('rep'), may hold values from -6 to 6
- out_grads: bfloat16 [4096, 8192], P('rep', 'stripe'), may hold values from -4 to 4
- statistics: float32 [16, 16, 512, 512], P('rep', 'stripe'), may hold values from -48 to 4608, as said below
- owner_blocks: int32 [16, 8], P('stripe'), may hold values from 0 to 7, each once within a row
Outputs:
- preconditioned: float32 [4096, 8192], P(None, 'stripe')
- new_stats: float32 [16, 16, 512, 512], P('rep', 'stripe')
The draws below stay inside these ranges and needn't reach their ends.
Inputs may be any that keep to these rules, and one draw needn't show every extreme that they name: statistics[p, s] is symmetric positive definite for every p and s. `owner_blocks`: each row lists every row block 0 to 7 exactly once.
All inputs are finite; a program needn't handle non-finite values.
Results may differ from the reference program's by a relative error of at most 0.0003.
Values sent between devices are 32-bit elements; how exact they have to be, the bound alone decides.
A program may use at most 128 MiB of HBM per device.

```python
import math
import jax
import jax.numpy as jnp
from jax import lax

BLOCK = 512
ITERS = 2
PAIRS = 8
STRIPES = 16
DIN = 4096
DOUT = 8192
TOKENS = 4096
N_REP = 16
N_STRIPE = 16


def draw_statistics(key, part):
    key_diag = jax.random.fold_in(key, 101)
    key_noise = jax.random.fold_in(key, 202)
    owners = 2 * PAIRS
    diagonal = BLOCK * jnp.exp(jax.random.uniform(key_diag, (owners, STRIPES, BLOCK), jnp.float32, math.log(0.3), math.log(3.0)))
    rising = 3.0 ** (jnp.arange(owners, dtype=jnp.float32) / max(owners - 1, 1))
    diagonal = diagonal * rising[:, None, None]
    noise = jnp.clip(jax.random.normal(key_noise, (owners, STRIPES, BLOCK, BLOCK), jnp.float32), -6.0, 6.0)
    symmetric = (noise + jnp.swapaxes(noise, -1, -2)) / math.sqrt(2.0)
    root_diag = jnp.sqrt(diagonal)
    offdiag = 0.5 * symmetric * root_diag[..., :, None] * root_diag[..., None, :] / BLOCK
    identity = jnp.eye(BLOCK, dtype=jnp.float32)
    return offdiag * (1.0 - identity) + diagonal[..., :, None] * identity


def draw_out_grads(key, part):
    key_base = jax.random.fold_in(key, 303)
    key_cols = jax.random.fold_in(key, 404)
    base = jnp.clip(jax.random.normal(key_base, (TOKENS, DOUT), jnp.float32), -6.0, 6.0)
    columns = jnp.exp(jax.random.uniform(key_cols, (DOUT,), jnp.float32, -0.7, 0.7))
    stripe_pos = (jnp.arange(DOUT, dtype=jnp.int32) // BLOCK).astype(jnp.float32)
    rising = math.sqrt(3.0) ** (stripe_pos / max(STRIPES - 1, 1))
    return (base * columns * rising / math.sqrt(TOKENS)).astype(jnp.bfloat16)


def level_of(rng, extent, split, least, high):
    def one(position, blocks):
        heights = jax.random.uniform(jax.random.fold_in(jax.random.fold_in(rng, 6), position), (blocks,), jnp.float32, least / len(split), high / len(split))
        return jnp.repeat(jnp.exp(heights), extent[position] // blocks).reshape((-1,) + (1,) * (len(extent) - position - 1))

    gain = one(*split[0])
    for cut in split[1:]:
        gain = gain * one(*cut)
    return gain


def scatter_about(stream_key, dims, width, limit, pieces=(), held_as=jnp.bfloat16):
    gain = level_of(stream_key, dims, pieces, -0.22, 0.18) if pieces else 1.0
    drawn = jax.random.normal(stream_key, dims, jnp.float32) * width * gain
    return jnp.minimum(jnp.maximum(drawn, -limit), limit).astype(held_as)


def setup_inputs(seed: int = 0) -> dict:
    arg_keys = jax.random.split(jax.random.key(seed), 5)
    return {
        "activations": scatter_about(arg_keys[0], (TOKENS, DIN), 1.0, 6.0, ((0, 16),)),
        "out_grads": draw_out_grads(jax.random.fold_in(arg_keys[4], 71), 0),
        "statistics": draw_statistics(jax.random.fold_in(arg_keys[4], 71), 0),
        "owner_blocks": jax.vmap(lambda own: jax.random.permutation(own, PAIRS))(jax.random.split(arg_keys[3], STRIPES)).reshape((STRIPES, PAIRS)).astype(jnp.int32),
    }


decay_rate = 0.95
damping = 0.25
epsilon = 1e-06
highest = lax.Precision.HIGHEST

def inverse_root(damped):
    identity = jnp.eye(damped.shape[-1], dtype=damped.dtype)
    frob_norm = jnp.sqrt(lax.optimization_barrier(jnp.sum(damped * damped, axis=(-2, -1), keepdims=True)) + epsilon)
    scaled = damped / frob_norm
    root_now = identity * frob_norm ** (-0.25)
    for sweep in range(ITERS):
        factor = (5.0 * identity - scaled) * 0.25
        root_now = jnp.matmul(root_now, factor, precision=highest)
        if sweep + 1 < ITERS:
            square = jnp.matmul(factor, factor, precision=highest)
            fourth = jnp.matmul(square, square, precision=highest)
            scaled = jnp.matmul(fourth, scaled, precision=highest)
    return root_now

def reference(activations, out_grads, statistics, owner_blocks):
    pair_count = N_REP // 2
    stripe_count = N_STRIPE
    gradient = jnp.dot(activations.T, out_grads, preferred_element_type=jnp.float32)
    blocks = gradient.reshape(pair_count, BLOCK, stripe_count, BLOCK).transpose(0, 2, 1, 3)
    stripe_ids = jnp.arange(stripe_count, dtype=jnp.int32)[None, :]
    owned_blocks = blocks[owner_blocks.T, stripe_ids]
    flipped = jnp.swapaxes(owned_blocks, -1, -2)
    left_stats = decay_rate * statistics[:pair_count] + jnp.matmul(owned_blocks, flipped, precision=highest)
    right_stats = decay_rate * statistics[pair_count:] + jnp.matmul(flipped, owned_blocks, precision=highest)
    new_stats = jnp.concatenate([left_stats, right_stats], axis=0)
    trace_sum = jnp.sum(jnp.diagonal(new_stats, axis1=-2, axis2=-1))
    mean_diag = trace_sum / (N_REP * N_STRIPE * BLOCK)
    identity = jnp.eye(BLOCK, dtype=new_stats.dtype)
    left_root = inverse_root(left_stats + damping * mean_diag * identity)
    right_root = inverse_root(right_stats + damping * mean_diag * identity)
    precond = jnp.matmul(jnp.matmul(left_root, owned_blocks, precision=highest), right_root, precision=highest)
    grad_sq = jnp.sum(gradient * gradient)
    prec_sq = jnp.sum(precond * precond)
    precond = precond * jnp.sqrt(grad_sq / (prec_sq + epsilon))
    pair_ids = jnp.arange(pair_count, dtype=jnp.int32)
    inverse = lax.optimization_barrier(jnp.sum(pair_ids[None, :, None] * (owner_blocks[:, :, None] == pair_ids[None, None, :]).astype(jnp.int32), axis=1))
    placed = precond[inverse.T, stripe_ids]
    placed = placed.transpose(0, 2, 1, 3).reshape(pair_count * BLOCK, stripe_count * BLOCK)
    return (placed, new_stats)
```

```python
import functools

import jax
import jax.numpy as jnp
from jax import lax
from jax.experimental import pallas as pl
from jax.experimental.pallas import tpu as pltpu
from jax.sharding import PartitionSpec as P

MESH = pl.DeviceIdType.MESH
f32 = jnp.float32
bf16 = jnp.bfloat16

BLOCK = 512
HALF = 256
DECAY = 0.95
DAMPING = 0.25
EPS = 1e-06
COUNT = 131072.0

RELATIVE = (3, 1, 2, 0)
SEQUENCE = ((0, 2, 1, 3), (1, 2, 0, 3))
QS = 2
ROWS = HALF // 2 // QS
PIECES = 2 * QS


def position():
    rep = lax.axis_index("rep")
    stripe = lax.axis_index("stripe")
    return rep // 4, stripe // 4, (rep // 2) % 2, stripe % 4, rep % 2


def device(x, y, z, c):
    return (x * 4 + (z // 4) * 2 + c, y * 4 + z % 4)


def split(a):
    high = a.astype(bf16)
    low = (a - high.astype(f32)).astype(bf16)
    return high, low


def product(a, b, dims=((1,), (0,))):
    (ah, al), (bh, bl) = a, b

    def dot(u, v):
        return lax.dot_general(u, v, (dims, ((), ())), preferred_element_type=f32)

    return dot(ah, bh) + (dot(ah, bl) + dot(al, bh))


def total(a):
    return jnp.sum(jnp.sum(a, axis=0, keepdims=True), axis=1, keepdims=True)


def eye_mask(n):
    return lax.broadcasted_iota(jnp.int32, (n, n), 0) == lax.broadcasted_iota(jnp.int32, (n, n), 1)


def rows_of(piece):
    return pl.ds(piece * ROWS, ROWS)


def main_kernel(
    blocks, act, og, stat_in,
    gath, new_stat, scale_out,
    acc, psend, precv, ring, zbuf, grad, stat, norm, roots, precond, sums,
    ps_s, ps_r, ring_s, ring_r, z_s, z_r, g_s, g_r, st_s, st_r, ns_s, ns_r, rt_s, rt_r,
    gr_s, gr_r, gz_s, gz_r, gd_s, gd_r, own_s, sum_s, sum_r,
):
    x, y, zh, zl, c = position()
    z = zh * 4 + zl
    sibling = device(x, y, z, 1 - c)
    side = (device((x + 1) % 4, y, z, c), device((x + 3) % 4, y, z, c))
    zmate = device(x, y, (z + 4) % 8, c)
    owner = device((x + 2) % 4, y, z, 1 - c)
    stays = c == x // 2
    moves = c != x // 2

    def remote(src, dst, send, recv, to):
        return pltpu.make_async_remote_copy(
            src_ref=src, dst_ref=dst, send_sem=send, recv_sem=recv, device_id=to, device_id_type=MESH
        )

    groups = (
        [(o, device(((x * 2 + c + o) % 8) // 2, y, z, (x * 2 + c + o) % 2)) for o in range(1, 8)],
        [(o, device(x, (y + o) % 4, z, c)) for o in range(1, 4)],
        [(o, device(x, y, (z + o) % 8, c)) for o in range(1, 8)],
    )
    places = (x * 2 + c, y, z)
    sizes = (8, 4, 8)

    barrier = pltpu.get_barrier_semaphore()
    for group in groups:
        for _, peer in group:
            pl.semaphore_signal(barrier, inc=1, device_id=peer, device_id_type=MESH)
    pl.semaphore_wait(barrier, sum(len(group) for group in groups))

    stat_local = pltpu.make_async_copy(stat_in, stat, own_s.at[0])
    stat_remote = remote(stat_in, stat, st_s, st_r, owner)

    @pl.when(stays)
    def _():
        stat_local.start()

    @pl.when(moves)
    def _():
        stat_remote.start()

    def columns(slot, half):
        xt = (x + RELATIVE[slot % 4]) % 4
        zt = (1 - zh) if slot < 4 else zh
        block = blocks[0, (xt % 2) * 4 + zt * 2 + xt // 2]
        return act[:, pl.ds(block * BLOCK + half * HALF, HALF)]

    def partial(slot, half):
        return lax.dot_general(
            columns(slot, half), og[...], (((0,), (0,)), ((), ())), preferred_element_type=f32
        )

    def ring_copy(phase, d, step, q):
        index = ((phase * 2 + d) * 3 + step) * QS + q
        source = acc.at[phase * 4 + SEQUENCE[d][step], rows_of(d * QS + q)]
        return remote(source, ring.at[index], ring_s.at[index], ring_r.at[index], side[d])

    started = []

    def ring_start(phase, d, step, q):
        copy = ring_copy(phase, d, step, q)
        copy.start()
        started.append(copy)

    def ring_take(phase, d, step, q):
        index = ((phase * 2 + d) * 3 + step) * QS + q
        ring_copy(phase, d, step, q).wait_recv()
        slot = phase * 4 + SEQUENCE[d][step + 1]
        rows = rows_of(d * QS + q)
        acc[slot, rows] = acc[slot, rows] + ring[index]

    def pair_take(slot):
        pair[slot].wait_recv()
        acc[slot] = acc[slot] + precv[slot]

    pair = []
    for slot in range(8):
        psend[slot] = partial(slot, 1 - c)
        copy = remote(psend.at[slot], precv.at[slot], ps_s.at[slot], ps_r.at[slot], sibling)
        copy.start()
        pair.append(copy)
        acc[slot] = partial(slot, c)
        if slot > 0:
            pair_take(slot - 1)
        if slot == 2:
            for q in range(QS):
                for d in range(2):
                    ring_start(0, d, 0, q)
    pair_take(7)

    def advance(phase, step):
        for q in range(QS):
            for d in range(2):
                ring_take(phase, d, step, q)
                ring_start(phase, d, step + 1, q)

    zcopies = [
        remote(acc.at[3, rows_of(i)], zbuf.at[i], z_s.at[i], z_r.at[i], zmate) for i in range(PIECES)
    ]
    advance(0, 0)
    for d in range(2):
        ring_start(1, d, 0, 0)
    advance(0, 1)
    for q in range(1, QS):
        for d in range(2):
            ring_start(1, d, 0, q)
    for q in range(QS):
        for d in range(2):
            ring_take(0, d, 2, q)
            zcopies[d * QS + q].start()
    advance(1, 0)
    advance(1, 1)

    gcopies = []
    for q in range(QS):
        for d in range(2):
            i = d * QS + q
            ring_take(1, d, 2, q)
            zcopies[i].wait_recv()
            here = pl.ds(c * HALF + i * ROWS, ROWS)
            grad[here, :] = acc[7, rows_of(i)] + zbuf[i]
            copy = remote(grad.at[here, :], grad.at[here, :], g_s.at[i], g_r.at[i], sibling)
            copy.start()
            gcopies.append(copy)

    @pl.when(stays)
    def _():
        stat_local.wait()

    @pl.when(moves)
    def _():
        stat_remote.wait()

    lane = lax.broadcasted_iota(jnp.int32, (8, 128), 1)
    sum_copies = []

    def stage_copy(which, stage, o, peer, slot_of):
        base = which * 20 + (0, 8, 12)[stage]
        mine = base + places[stage]
        theirs = base + (places[stage] + o) % sizes[stage]
        send = sum_s.at[base + o]
        return remote(sums.at[mine], sums.at[mine], send, sum_r.at[mine if slot_of == "send" else theirs], peer)

    def stage_start(which, stage, value):
        base = which * 20 + (0, 8, 12)[stage]
        sums[base + places[stage]] = value
        for o, peer in groups[stage]:
            copy = stage_copy(which, stage, o, peer, "send")
            copy.start()
            sum_copies.append(copy)

    def stage_take(which, stage):
        base = which * 20 + (0, 8, 12)[stage]
        for o, peer in groups[stage]:
            stage_copy(which, stage, o, peer, "recv").wait_recv()
        value = sums[base]
        for i in range(1, sizes[stage]):
            value = value + sums[base + i]
        return value

    mask = eye_mask(BLOCK)
    stat_trace = total(jnp.where(mask, stat[...], 0.0))
    half = grad[pl.ds(c * HALF, HALF), :]
    square = total(half * half)
    stage_start(0, 0, jnp.where(lane == 0, stat_trace, 0.0) + jnp.where(lane == 1, square, 0.0))

    for copy in gcopies:
        copy.wait_recv()
    gsplit = split(grad[...])

    @pl.when(c == 0)
    def _():
        stat[...] = DECAY * stat[...] + product(gsplit, gsplit, ((1,), (1,)))

    @pl.when(c == 1)
    def _():
        stat[...] = DECAY * stat[...] + product(gsplit, gsplit, ((0,), (0,)))

    back_local = pltpu.make_async_copy(stat, new_stat, own_s.at[1])
    back_remote = remote(stat, new_stat, ns_s, ns_r, owner)
    value = stage_take(0, 0)
    stage_start(0, 1, value)

    now = stat[...]
    square_sum = total(now * now)
    now_trace = total(jnp.where(mask, now, 0.0))
    size = jnp.sqrt(square_sum + EPS)
    first = now * (1.0 / size)
    norm[0] = first
    first_split = split(first)
    second = product(first_split, first_split)
    norm[1] = second
    value = stage_take(0, 1)
    stage_start(0, 2, value)
    third = product(split(second), first_split)
    norm[2] = third

    @pl.when(stays)
    def _():
        back_local.start()

    @pl.when(moves)
    def _():
        back_remote.start()

    value = stage_take(0, 2)
    top = lax.broadcasted_iota(jnp.int32, (8, 128), 0) == 0
    trace_all = total(jnp.where(top & (lane == 0), value, 0.0))
    grad_sq = total(jnp.where(top & (lane == 1), value, 0.0))
    shift = DAMPING * ((DECAY * trace_all + 2.0 * grad_sq) / COUNT)
    frob = jnp.sqrt(square_sum + (2.0 * shift * now_trace + BLOCK * shift * shift) + EPS)
    ratio = size / frob
    e = shift / frob
    gain = 1.0 / jnp.sqrt(jnp.sqrt(frob))
    a = (
        25.0 / 16.0, -5.0 / 16.0 - 3125.0 / 4096.0, 3125.0 / 4096.0, -1250.0 / 4096.0,
        250.0 / 4096.0, -25.0 / 4096.0, 1.0 / 4096.0,
    )
    binomial = (
        (1,), (1, 1), (1, 2, 1), (1, 3, 3, 1), (1, 4, 6, 4, 1), (1, 5, 10, 10, 5, 1), (1, 6, 15, 20, 15, 6, 1),
    )
    coefs = []
    scale = gain
    for j in range(7):
        coef = jnp.full_like(e, a[6] * binomial[6][j])
        for i in range(5, j - 1, -1):
            coef = coef * e + a[i] * binomial[i][j]
        coefs.append(coef * scale)
        scale = scale * ratio
    first, second, third = norm[0], norm[1], norm[2]
    upper = coefs[4] * first + coefs[5] * second + coefs[6] * third
    root = coefs[1] * first + coefs[2] * second + coefs[3] * third + jnp.where(mask, coefs[0], 0.0)
    root = root + product(split(third), split(upper))
    roots[c] = root
    root_copy = remote(roots.at[c], roots.at[c], rt_s, rt_r, sibling)
    root_copy.start()
    root_copy.wait_recv()

    mine = roots[0, pl.ds(c * HALF, HALF), :]
    left = product(split(mine), gsplit)
    result = product(split(left), split(roots[1]))
    for i in range(PIECES):
        precond[i] = result[i * ROWS : (i + 1) * ROWS]
    stage_start(1, 0, jnp.where(lane == 0, total(result * result), 0.0))

    def place(xt, zt):
        return (xt * 2 + zt) * 2 + c

    gathers = []

    def spread(i, d2d, source, xt, zt):
        where = gath.at[place(xt, zt), rows_of(i)]
        copy = remote(source, where, gd_s.at[d2d], gd_r.at[d2d], sibling)
        copy.start()
        gathers.append(copy)

    def gather_copy(phase, d, step, q):
        index = ((phase * 2 + d) * 3 + step) * QS + q
        xt = (x + 4 - step) % 4 if d == 0 else (x + step) % 4
        zt = zh if phase == 0 else 1 - zh
        where = gath.at[place(xt, zt), rows_of(d * QS + q)]
        source = precond.at[d * QS + q] if phase == 0 and step == 0 else where
        return remote(source, where, gr_s.at[index], gr_r.at[index], side[d])

    def gather_start(phase, d, step, q):
        copy = gather_copy(phase, d, step, q)
        copy.start()
        gathers.append(copy)

    def gather_take(phase, d, step, q):
        gather_copy(phase, d, step, q).wait_recv()
        if step < 2:
            gather_start(phase, d, step + 1, q)
        xt = (x + 3 - step) % 4 if d == 0 else (x + 1 + step) % 4
        zt = zh if phase == 0 else 1 - zh
        spread(d * QS + q, (phase * 4 + step + 1) * PIECES + d * QS + q, gath.at[place(xt, zt), rows_of(d * QS + q)], xt, zt)

    mates = [
        remote(precond.at[i], gath.at[place(x, zh), rows_of(i)], gz_s.at[i], gz_r.at[i], zmate)
        for i in range(PIECES)
    ]
    kept = [
        pltpu.make_async_copy(precond.at[i], gath.at[place(x, zh), rows_of(i)], own_s.at[2 + i])
        for i in range(PIECES)
    ]
    order = [(d, q) for q in range(QS) for d in range(2)]
    for d, q in order:
        mates[d * QS + q].start()
        gather_start(0, d, 0, q)
    for i in range(PIECES):
        spread(i, i, precond.at[i], x, zh)
        kept[i].start()

    def mate_take(d, q):
        i = d * QS + q
        mates[i].wait_recv()
        gather_start(1, d, 0, q)
        spread(i, 4 * PIECES + i, gath.at[place(x, 1 - zh), rows_of(i)], x, 1 - zh)

    for d, q in order:
        gather_take(0, d, 0, q)
    value = stage_take(1, 0)
    stage_start(1, 1, value)
    mate_take(0, 0)
    for d, q in order:
        gather_take(0, d, 1, q)
    value = stage_take(1, 1)
    stage_start(1, 2, value)
    mate_take(1, 0)
    for d, q in order:
        gather_take(0, d, 2, q)
    for q in range(1, QS):
        for d in range(2):
            mate_take(d, q)
    for step in range(3):
        for d, q in order:
            gather_take(1, d, step, q)
    value = stage_take(1, 2)
    prec_sq = total(jnp.where(top & (lane == 0), value, 0.0))
    scale_out[...] = jnp.broadcast_to(jnp.sqrt(grad_sq / (prec_sq + EPS)), (8, 128))

    for i in range(8 * PIECES):
        where = gath.at[0, rows_of(i % PIECES)]
        remote(where, where, gd_s.at[i], gd_r.at[i], sibling).wait_recv()
    for copy in pair + started + zcopies + gcopies + sum_copies + [root_copy] + gathers + mates:
        copy.wait_send()
    for copy in kept:
        copy.wait()

    @pl.when(stays)
    def _():
        back_local.wait()

    @pl.when(moves)
    def _():
        back_remote.wait()


def run_main(blocks, act, og, stat):
    dma = pltpu.SemaphoreType.DMA
    ring_count = 12 * QS
    space = pl.BlockSpec
    return pl.pallas_call(
        main_kernel,
        out_shape=(
            jax.ShapeDtypeStruct((16, HALF, BLOCK), f32),
            jax.ShapeDtypeStruct((BLOCK, BLOCK), f32),
            jax.ShapeDtypeStruct((8, 128), f32),
        ),
        in_specs=[
            space(memory_space=pltpu.SMEM), space(memory_space=pltpu.VMEM),
            space(memory_space=pltpu.VMEM), space(memory_space=pl.ANY),
        ],
        out_specs=(space(memory_space=pl.ANY), space(memory_space=pl.ANY), space(memory_space=pltpu.VMEM)),
        scratch_shapes=[
            pltpu.VMEM((8, HALF, BLOCK), f32),
            pltpu.VMEM((8, HALF, BLOCK), f32),
            pltpu.VMEM((8, HALF, BLOCK), f32),
            pltpu.VMEM((ring_count, ROWS, BLOCK), f32),
            pltpu.VMEM((PIECES, ROWS, BLOCK), f32),
            pltpu.VMEM((BLOCK, BLOCK), f32),
            pltpu.VMEM((BLOCK, BLOCK), f32),
            pltpu.VMEM((3, BLOCK, BLOCK), f32),
            pltpu.VMEM((2, BLOCK, BLOCK), f32),
            pltpu.VMEM((PIECES, ROWS, BLOCK), f32),
            pltpu.VMEM((40, 8, 128), f32),
            dma((8,)), dma((8,)), dma((ring_count,)), dma((ring_count,)), dma((PIECES,)), dma((PIECES,)),
            dma((PIECES,)), dma((PIECES,)), dma(()), dma(()), dma(()), dma(()), dma(()), dma(()),
            dma((ring_count,)), dma((ring_count,)), dma((PIECES,)), dma((PIECES,)),
            dma((8 * PIECES,)), dma((8 * PIECES,)), dma((2 + PIECES,)), dma((40,)), dma((40,)),
        ],
        compiler_params=pltpu.CompilerParams(
            collective_id=0, has_side_effects=True, vmem_limit_bytes=48 * 1024 * 1024
        ),
        name="shampoo",
    )(blocks, act, og, stat)


def place_kernel(order, gath, scale, out):
    out[...] = gath[0] * scale[0:1, 0:1]


def run_place(order, gath, scale):
    return pl.pallas_call(
        place_kernel,
        grid_spec=pltpu.PrefetchScalarGridSpec(
            num_scalar_prefetch=1,
            grid=(16,),
            in_specs=[
                pl.BlockSpec((1, HALF, BLOCK), lambda i, order: (order[i], 0, 0)),
                pl.BlockSpec((8, 128), lambda i, order: (0, 0)),
            ],
            out_specs=pl.BlockSpec((HALF, BLOCK), lambda i, order: (i, 0)),
        ),
        out_shape=jax.ShapeDtypeStruct((16 * HALF, BLOCK), f32),
        name="place",
    )(order, gath, scale)


def per_device(activations, out_grads, statistics, owner_blocks):
    gath, new_stat, scale = run_main(owner_blocks, activations, out_grads, statistics[0, 0])
    pairs = jnp.arange(8, dtype=jnp.int32)
    pair = jnp.sum(pairs[:, None] * (owner_blocks[0][:, None] == pairs[None, :]).astype(jnp.int32), axis=0)
    slot = (pair // 4 + 2 * (pair % 2)) * 2 + (pair // 2) % 2
    order = jnp.stack([slot * 2, slot * 2 + 1], axis=1).reshape(-1)
    return run_place(order, gath, scale), new_stat[None, None]


def solution(mesh):
    return jax.shard_map(
        per_device,
        mesh=mesh,
        in_specs=(P("rep", None), P("rep", "stripe"), P("rep", "stripe", None, None), P("stripe", None)),
        out_specs=(P(None, "stripe"), P("rep", "stripe", None, None)),
        check_vma=False,
    )
```

```python
import functools

import jax
import jax.numpy as jnp
from jax import lax
from jax.experimental import pallas as pl
from jax.experimental.pallas import tpu as pltpu
from jax.sharding import PartitionSpec as P

MESH = pl.DeviceIdType.MESH
f32 = jnp.float32
bf16 = jnp.bfloat16

BLOCK = 512
HALF = 256
DECAY = 0.95
DAMPING = 0.25
EPS = 1e-06
COUNT = 131072.0

RELATIVE = (3, 1, 2, 0)
SEQUENCE = ((0, 2, 1, 3), (1, 2, 0, 3))
QS = 2
ROWS = HALF // 2 // QS
PIECES = 2 * QS


def position():
    rep = lax.axis_index("rep")
    stripe = lax.axis_index("stripe")
    return rep // 4, stripe // 4, (rep // 2) % 2, stripe % 4, rep % 2


def device(x, y, z, c):
    return (x * 4 + (z // 4) * 2 + c, y * 4 + z % 4)


def split(a):
    high = a.astype(bf16)
    low = (a - high.astype(f32)).astype(bf16)
    return high, low


def product(a, b, dims=((1,), (0,))):
    (ah, al), (bh, bl) = a, b

    def dot(u, v):
        return lax.dot_general(u, v, (dims, ((), ())), preferred_element_type=f32)

    return dot(ah, bh) + (dot(ah, bl) + dot(al, bh))


def total(a):
    return jnp.sum(jnp.sum(a, axis=0, keepdims=True), axis=1, keepdims=True)


def eye_mask(n):
    return lax.broadcasted_iota(jnp.int32, (n, n), 0) == lax.broadcasted_iota(jnp.int32, (n, n), 1)


def rows_of(piece):
    return pl.ds(piece * ROWS, ROWS)


def main_kernel(
    blocks, act_in, og_in, stat_in,
    gath, new_stat, scale_out,
    act, og, acc, psend, precv, ring, zbuf, grad, stat, norm, roots, precond, sums,
    ps_s, ps_r, ring_s, ring_r, z_s, z_r, g_s, g_r, st_s, st_r, ns_s, ns_r, rt_s, rt_r,
    gr_s, gr_r, gz_s, gz_r, gd_s, gd_r, own_s, sum_s, sum_r, in_s,
):
    x, y, zh, zl, c = position()
    z = zh * 4 + zl
    sibling = device(x, y, z, 1 - c)
    side = (device((x + 1) % 4, y, z, c), device((x + 3) % 4, y, z, c))
    zmate = device(x, y, (z + 4) % 8, c)
    owner = device((x + 2) % 4, y, z, 1 - c)
    stays = c == x // 2
    moves = c != x // 2

    def remote(src, dst, send, recv, to):
        return pltpu.make_async_remote_copy(
            src_ref=src, dst_ref=dst, send_sem=send, recv_sem=recv, device_id=to, device_id_type=MESH
        )

    groups = (
        [(o, device(((x * 2 + c + o) % 8) // 2, y, z, (x * 2 + c + o) % 2)) for o in range(1, 8)],
        [(o, device(x, (y + o) % 4, z, c)) for o in range(1, 4)],
        [(o, device(x, y, (z + o) % 8, c)) for o in range(1, 8)],
    )
    places = (x * 2 + c, y, z)
    sizes = (8, 4, 8)

    inputs = [pltpu.make_async_copy(act_in, act, in_s.at[0]), pltpu.make_async_copy(og_in, og, in_s.at[1])]
    for copy in inputs:
        copy.start()
    barrier = pltpu.get_barrier_semaphore()
    for group in groups:
        for _, peer in group:
            pl.semaphore_signal(barrier, inc=1, device_id=peer, device_id_type=MESH)
    pl.semaphore_wait(barrier, sum(len(group) for group in groups))

    stat_local = pltpu.make_async_copy(stat_in, stat, own_s.at[0])
    stat_remote = remote(stat_in, stat, st_s, st_r, owner)

    @pl.when(stays)
    def _():
        stat_local.start()

    @pl.when(moves)
    def _():
        stat_remote.start()

    def columns(slot, half):
        xt = (x + RELATIVE[slot % 4]) % 4
        zt = (1 - zh) if slot < 4 else zh
        block = blocks[0, (xt % 2) * 4 + zt * 2 + xt // 2]
        return act[:, pl.ds(block * BLOCK + half * HALF, HALF)]

    def partial(slot, half):
        return lax.dot_general(
            columns(slot, half), og[...], (((0,), (0,)), ((), ())), preferred_element_type=f32
        )

    def ring_copy(phase, d, step, q):
        index = ((phase * 2 + d) * 3 + step) * QS + q
        source = acc.at[phase * 4 + SEQUENCE[d][step], rows_of(d * QS + q)]
        return remote(source, ring.at[index], ring_s.at[index], ring_r.at[index], side[d])

    started = []

    def ring_start(phase, d, step, q):
        copy = ring_copy(phase, d, step, q)
        copy.start()
        started.append(copy)

    def ring_take(phase, d, step, q):
        index = ((phase * 2 + d) * 3 + step) * QS + q
        ring_copy(phase, d, step, q).wait_recv()
        slot = phase * 4 + SEQUENCE[d][step + 1]
        rows = rows_of(d * QS + q)
        acc[slot, rows] = acc[slot, rows] + ring[index]

    def pair_take(slot):
        pair[slot].wait_recv()
        acc[slot] = acc[slot] + precv[slot]

    for copy in inputs:
        copy.wait()
    pair = []
    for slot in range(8):
        psend[slot] = partial(slot, 1 - c)
        copy = remote(psend.at[slot], precv.at[slot], ps_s.at[slot], ps_r.at[slot], sibling)
        copy.start()
        pair.append(copy)
        acc[slot] = partial(slot, c)
        if slot > 0:
            pair_take(slot - 1)
        if slot == 2:
            for q in range(QS):
                for d in range(2):
                    ring_start(0, d, 0, q)
    pair_take(7)

    def advance(phase, step):
        for q in range(QS):
            for d in range(2):
                ring_take(phase, d, step, q)
                ring_start(phase, d, step + 1, q)

    zcopies = [
        remote(acc.at[3, rows_of(i)], zbuf.at[i], z_s.at[i], z_r.at[i], zmate) for i in range(PIECES)
    ]
    advance(0, 0)
    for d in range(2):
        ring_start(1, d, 0, 0)
    advance(0, 1)
    for q in range(1, QS):
        for d in range(2):
            ring_start(1, d, 0, q)
    for q in range(QS):
        for d in range(2):
            ring_take(0, d, 2, q)
            zcopies[d * QS + q].start()
    advance(1, 0)
    advance(1, 1)

    gcopies = []
    for q in range(QS):
        for d in range(2):
            i = d * QS + q
            ring_take(1, d, 2, q)
            zcopies[i].wait_recv()
            here = pl.ds(c * HALF + i * ROWS, ROWS)
            grad[here, :] = acc[7, rows_of(i)] + zbuf[i]
            copy = remote(grad.at[here, :], grad.at[here, :], g_s.at[i], g_r.at[i], sibling)
            copy.start()
            gcopies.append(copy)

    @pl.when(stays)
    def _():
        stat_local.wait()

    @pl.when(moves)
    def _():
        stat_remote.wait()

    lane = lax.broadcasted_iota(jnp.int32, (8, 128), 1)
    sum_copies = []

    def stage_copy(which, stage, o, peer, slot_of):
        base = which * 20 + (0, 8, 12)[stage]
        mine = base + places[stage]
        theirs = base + (places[stage] + o) % sizes[stage]
        send = sum_s.at[base + o]
        return remote(sums.at[mine], sums.at[mine], send, sum_r.at[mine if slot_of == "send" else theirs], peer)

    def stage_start(which, stage, value):
        base = which * 20 + (0, 8, 12)[stage]
        sums[base + places[stage]] = value
        for o, peer in groups[stage]:
            copy = stage_copy(which, stage, o, peer, "send")
            copy.start()
            sum_copies.append(copy)

    def stage_take(which, stage):
        base = which * 20 + (0, 8, 12)[stage]
        for o, peer in groups[stage]:
            stage_copy(which, stage, o, peer, "recv").wait_recv()
        value = sums[base]
        for i in range(1, sizes[stage]):
            value = value + sums[base + i]
        return value

    mask = eye_mask(BLOCK)
    stat_trace = total(jnp.where(mask, stat[...], 0.0))
    half = grad[pl.ds(c * HALF, HALF), :]
    square = total(half * half)
    stage_start(0, 0, jnp.where(lane == 0, stat_trace, 0.0) + jnp.where(lane == 1, square, 0.0))

    for copy in gcopies:
        copy.wait_recv()
    gsplit = split(grad[...])

    @pl.when(c == 0)
    def _():
        stat[...] = DECAY * stat[...] + product(gsplit, gsplit, ((1,), (1,)))

    @pl.when(c == 1)
    def _():
        stat[...] = DECAY * stat[...] + product(gsplit, gsplit, ((0,), (0,)))

    back_remote = remote(stat, new_stat, ns_s, ns_r, owner)
    value = stage_take(0, 0)
    stage_start(0, 1, value)

    now = stat[...]
    square_sum = total(now * now)
    now_trace = total(jnp.where(mask, now, 0.0))
    size = jnp.sqrt(square_sum + EPS)
    first = now * (1.0 / size)
    norm[0] = first
    first_split = split(first)
    second = product(first_split, first_split)
    norm[1] = second
    value = stage_take(0, 1)
    stage_start(0, 2, value)
    third = product(split(second), first_split)
    norm[2] = third

    @pl.when(stays)
    def _():
        new_stat[...] = stat[...]

    @pl.when(moves)
    def _():
        back_remote.start()

    value = stage_take(0, 2)
    top = lax.broadcasted_iota(jnp.int32, (8, 128), 0) == 0
    trace_all = total(jnp.where(top & (lane == 0), value, 0.0))
    grad_sq = total(jnp.where(top & (lane == 1), value, 0.0))
    shift = DAMPING * ((DECAY * trace_all + 2.0 * grad_sq) / COUNT)
    frob = jnp.sqrt(square_sum + (2.0 * shift * now_trace + BLOCK * shift * shift) + EPS)
    ratio = size / frob
    e = shift / frob
    gain = 1.0 / jnp.sqrt(jnp.sqrt(frob))
    a = (
        25.0 / 16.0, -5.0 / 16.0 - 3125.0 / 4096.0, 3125.0 / 4096.0, -1250.0 / 4096.0,
        250.0 / 4096.0, -25.0 / 4096.0, 1.0 / 4096.0,
    )
    binomial = (
        (1,), (1, 1), (1, 2, 1), (1, 3, 3, 1), (1, 4, 6, 4, 1), (1, 5, 10, 10, 5, 1), (1, 6, 15, 20, 15, 6, 1),
    )
    coefs = []
    scale = gain
    for j in range(7):
        coef = jnp.full_like(e, a[6] * binomial[6][j])
        for i in range(5, j - 1, -1):
            coef = coef * e + a[i] * binomial[i][j]
        coefs.append(coef * scale)
        scale = scale * ratio
    first, second, third = norm[0], norm[1], norm[2]
    upper = coefs[4] * first + coefs[5] * second + coefs[6] * third
    root = coefs[1] * first + coefs[2] * second + coefs[3] * third + jnp.where(mask, coefs[0], 0.0)
    root = root + product(split(third), split(upper))
    roots[c] = root
    root_copy = remote(roots.at[c], roots.at[c], rt_s, rt_r, sibling)
    root_copy.start()
    root_copy.wait_recv()

    mine = roots[0, pl.ds(c * HALF, HALF), :]
    left = product(split(mine), gsplit)
    result = product(split(left), split(roots[1]))
    for i in range(PIECES):
        precond[i] = result[i * ROWS : (i + 1) * ROWS]
    stage_start(1, 0, jnp.where(lane == 0, total(result * result), 0.0))

    def place(xt, zt):
        return (xt * 2 + zt) * 2 + c

    gathers = []

    def spread(i, d2d, source, xt, zt):
        where = gath.at[place(xt, zt), rows_of(i)]
        copy = remote(source, where, gd_s.at[d2d], gd_r.at[d2d], sibling)
        copy.start()
        gathers.append(copy)

    def gather_copy(phase, d, step, q):
        index = ((phase * 2 + d) * 3 + step) * QS + q
        xt = (x + 4 - step) % 4 if d == 0 else (x + step) % 4
        zt = zh if phase == 0 else 1 - zh
        where = gath.at[place(xt, zt), rows_of(d * QS + q)]
        source = precond.at[d * QS + q] if phase == 0 and step == 0 else where
        return remote(source, where, gr_s.at[index], gr_r.at[index], side[d])

    def gather_start(phase, d, step, q):
        copy = gather_copy(phase, d, step, q)
        copy.start()
        gathers.append(copy)

    def gather_take(phase, d, step, q):
        gather_copy(phase, d, step, q).wait_recv()
        if step < 2:
            gather_start(phase, d, step + 1, q)
        xt = (x + 3 - step) % 4 if d == 0 else (x + 1 + step) % 4
        zt = zh if phase == 0 else 1 - zh
        spread(d * QS + q, (phase * 4 + step + 1) * PIECES + d * QS + q, gath.at[place(xt, zt), rows_of(d * QS + q)], xt, zt)

    mates = [
        remote(precond.at[i], gath.at[place(x, zh), rows_of(i)], gz_s.at[i], gz_r.at[i], zmate)
        for i in range(PIECES)
    ]
    order = [(d, q) for q in range(QS) for d in range(2)]
    for d, q in order:
        mates[d * QS + q].start()
        gather_start(0, d, 0, q)
    for i in range(PIECES):
        spread(i, i, precond.at[i], x, zh)
        gath[place(x, zh), rows_of(i)] = precond[i]

    def mate_take(d, q):
        i = d * QS + q
        mates[i].wait_recv()
        gather_start(1, d, 0, q)
        spread(i, 4 * PIECES + i, gath.at[place(x, 1 - zh), rows_of(i)], x, 1 - zh)

    for d, q in order:
        gather_take(0, d, 0, q)
    value = stage_take(1, 0)
    stage_start(1, 1, value)
    mate_take(0, 0)
    for d, q in order:
        gather_take(0, d, 1, q)
    value = stage_take(1, 1)
    stage_start(1, 2, value)
    mate_take(1, 0)
    for d, q in order:
        gather_take(0, d, 2, q)
    for q in range(1, QS):
        for d in range(2):
            mate_take(d, q)
    for step in range(3):
        for d, q in order:
            gather_take(1, d, step, q)
    value = stage_take(1, 2)
    prec_sq = total(jnp.where(top & (lane == 0), value, 0.0))
    scale_out[...] = jnp.broadcast_to(jnp.sqrt(grad_sq / (prec_sq + EPS)), (8, 128))

    for i in range(8 * PIECES):
        where = gath.at[0, rows_of(i % PIECES)]
        remote(where, where, gd_s.at[i], gd_r.at[i], sibling).wait_recv()
    for copy in pair + started + zcopies + gcopies + sum_copies + [root_copy] + gathers + mates:
        copy.wait_send()

    @pl.when(moves)
    def _():
        back_remote.wait()


def run_main(blocks, act, og, stat):
    dma = pltpu.SemaphoreType.DMA
    ring_count = 12 * QS
    space = pl.BlockSpec
    return pl.pallas_call(
        main_kernel,
        out_shape=(
            jax.ShapeDtypeStruct((16, HALF, BLOCK), f32),
            jax.ShapeDtypeStruct((BLOCK, BLOCK), f32),
            jax.ShapeDtypeStruct((8, 128), f32),
        ),
        in_specs=[
            space(memory_space=pltpu.SMEM), space(memory_space=pltpu.HBM),
            space(memory_space=pltpu.HBM), space(memory_space=pltpu.HBM),
        ],
        out_specs=(space(memory_space=pltpu.VMEM), space(memory_space=pltpu.VMEM), space(memory_space=pltpu.VMEM)),
        scratch_shapes=[
            pltpu.VMEM((HALF, 4096), bf16),
            pltpu.VMEM((HALF, BLOCK), bf16),
            pltpu.VMEM((8, HALF, BLOCK), f32),
            pltpu.VMEM((8, HALF, BLOCK), f32),
            pltpu.VMEM((8, HALF, BLOCK), f32),
            pltpu.VMEM((ring_count, ROWS, BLOCK), f32),
            pltpu.VMEM((PIECES, ROWS, BLOCK), f32),
            pltpu.VMEM((BLOCK, BLOCK), f32),
            pltpu.VMEM((BLOCK, BLOCK), f32),
            pltpu.VMEM((3, BLOCK, BLOCK), f32),
            pltpu.VMEM((2, BLOCK, BLOCK), f32),
            pltpu.VMEM((PIECES, ROWS, BLOCK), f32),
            pltpu.VMEM((40, 8, 128), f32),
            dma((8,)), dma((8,)), dma((ring_count,)), dma((ring_count,)), dma((PIECES,)), dma((PIECES,)),
            dma((PIECES,)), dma((PIECES,)), dma(()), dma(()), dma(()), dma(()), dma(()), dma(()),
            dma((ring_count,)), dma((ring_count,)), dma((PIECES,)), dma((PIECES,)),
            dma((8 * PIECES,)), dma((8 * PIECES,)), dma((2 + PIECES,)), dma((40,)), dma((40,)), dma((2,)),
        ],
        compiler_params=pltpu.CompilerParams(
            collective_id=0, has_side_effects=True, vmem_limit_bytes=40 * 1024 * 1024
        ),
        name="shampoo",
    )(blocks, act, og, stat)


def place_kernel(blocks, gath, stat_in, scale, out, stat_out, stage, sem):
    stat_copy = pltpu.make_async_copy(stat_in, stat_out, sem.at[8])
    stat_copy.start()
    copies = []
    for block in range(8):
        pair = jnp.int32(0)
        for p in range(1, 8):
            pair = jnp.where(blocks[0, p] == block, p, pair)
        slot = (pair // 4 + 2 * (pair % 2)) * 2 + (pair // 2) % 2
        for half in range(2):
            stage[block, half * HALF : (half + 1) * HALF] = gath[slot * 2 + half] * scale[0:1, 0:1]
        copy = pltpu.make_async_copy(stage.at[block], out.at[pl.ds(block * BLOCK, BLOCK)], sem.at[block])
        copy.start()
        copies.append(copy)
    for copy in copies:
        copy.wait()
    stat_copy.wait()


def run_place(blocks, gath, stat, scale):
    vmem = pl.BlockSpec(memory_space=pltpu.VMEM)
    hbm = pl.BlockSpec(memory_space=pltpu.HBM)
    return pl.pallas_call(
        place_kernel,
        in_specs=[pl.BlockSpec(memory_space=pltpu.SMEM), vmem, vmem, vmem],
        out_specs=(hbm, hbm),
        out_shape=(
            jax.ShapeDtypeStruct((8 * BLOCK, BLOCK), f32),
            jax.ShapeDtypeStruct((BLOCK, BLOCK), f32),
        ),
        scratch_shapes=[pltpu.VMEM((8, BLOCK, BLOCK), f32), pltpu.SemaphoreType.DMA((9,))],
        compiler_params=pltpu.CompilerParams(vmem_limit_bytes=24 * 1024 * 1024),
        name="place",
    )(blocks, gath, stat, scale)


def per_device(activations, out_grads, statistics, owner_blocks):
    held = [pltpu.with_memory_space_constraint(a, pltpu.HBM) for a in (owner_blocks, activations, out_grads, statistics[0, 0])]
    gath, new_stat, scale = run_main(*held)
    rows, new_stat = run_place(held[0], gath, new_stat, scale)
    return rows, new_stat[None, None]


def solution(mesh):
    return jax.shard_map(
        per_device,
        mesh=mesh,
        in_specs=(P("rep", None), P("rep", "stripe"), P("rep", "stripe", None, None), P("stripe", None)),
        out_specs=(P(None, "stripe"), P("rep", "stripe", None, None)),
        check_vma=False,
    )
```

```python
import functools

import jax
import jax.numpy as jnp
from jax import lax
from jax.experimental import pallas as pl
from jax.experimental.pallas import tpu as pltpu
from jax.sharding import PartitionSpec as P

MESH = pl.DeviceIdType.MESH
f32 = jnp.float32
bf16 = jnp.bfloat16

BLOCK = 512
HALF = 256
TILE = 128
DECAY = 0.95
DAMPING = 0.25
EPS = 1e-06
COUNT = 131072.0

RELATIVE = (3, 1, 2, 0)
SEQUENCE = ((0, 2, 1, 3), (1, 2, 0, 3))
QS = 2
ROWS = HALF // 2 // QS
PIECES = 2 * QS


def position():
    rep = lax.axis_index("rep")
    stripe = lax.axis_index("stripe")
    return rep // 4, stripe // 4, (rep // 2) % 2, stripe % 4, rep % 2


def device(x, y, z, c):
    return (x * 4 + (z // 4) * 2 + c, y * 4 + z % 4)


def split(a):
    high = a.astype(bf16)
    low = (a - high.astype(f32)).astype(bf16)
    return high, low


def product(a, b, dims=((1,), (0,))):
    (ah, al), (bh, bl) = a, b

    def dot(u, v):
        return lax.dot_general(u, v, (dims, ((), ())), preferred_element_type=f32)

    return dot(ah, bh) + (dot(ah, bl) + dot(al, bh))


def total(a):
    return jnp.sum(jnp.sum(a, axis=0, keepdims=True), axis=1, keepdims=True)


def eye_mask(n):
    return lax.broadcasted_iota(jnp.int32, (n, n), 0) == lax.broadcasted_iota(jnp.int32, (n, n), 1)


def rows_of(piece):
    return pl.ds(piece * ROWS, ROWS)


def main_kernel(
    blocks, act_in, og_in, stat_in,
    gath, new_stat, scale_out,
    act, og, diag, acc, psend, precv, ring, zbuf, grad, stat, norm, roots, precond, sums,
    ps_s, ps_r, ring_s, ring_r, z_s, z_r, g_s, g_r, st_s, st_r, ns_s, ns_r, rt_s, rt_r,
    gr_s, gr_r, gz_s, gz_r, gd_s, gd_r, own_s, sum_s, sum_r, in_s,
):
    x, y, zh, zl, c = position()
    z = zh * 4 + zl
    sibling = device(x, y, z, 1 - c)
    side = (device((x + 1) % 4, y, z, c), device((x + 3) % 4, y, z, c))
    zmate = device(x, y, (z + 4) % 8, c)
    owner = device((x + 2) % 4, y, z, 1 - c)
    stays = c == x // 2
    moves = c != x // 2

    def remote(src, dst, send, recv, to):
        return pltpu.make_async_remote_copy(
            src_ref=src, dst_ref=dst, send_sem=send, recv_sem=recv, device_id=to, device_id_type=MESH
        )

    groups = (
        [(o, device(x, y, (z + o) % 8, c)) for o in range(1, 8)],
        [(o, device(x, (y + o) % 4, z, c)) for o in range(1, 4)],
        [(o, device(((x * 2 + c + o) % 8) // 2, y, z, (x * 2 + c + o) % 2)) for o in range(1, 8)],
    )
    places = (z, y, x * 2 + c)
    sizes = (8, 4, 8)

    inputs = [pltpu.make_async_copy(act_in, act, in_s.at[0]), pltpu.make_async_copy(og_in, og, in_s.at[1])]
    for i in range(4):
        tile = pl.ds(i * TILE, TILE)
        inputs.append(pltpu.make_async_copy(stat_in.at[tile, tile], diag.at[i], in_s.at[2 + i]))
    for copy in inputs:
        copy.start()
    barrier = pltpu.get_barrier_semaphore()
    for group in groups:
        for _, peer in group:
            pl.semaphore_signal(barrier, inc=1, device_id=peer, device_id_type=MESH)
    pl.semaphore_wait(barrier, sum(len(group) for group in groups))

    stat_local = pltpu.make_async_copy(stat_in, stat, own_s)
    stat_remote = []
    back_remote = []
    for i in range(4):
        rows, cols = pl.ds(i * TILE, TILE), pl.ds(i * TILE, BLOCK - i * TILE)
        stat_remote.append(remote(stat_in.at[rows, cols], stat.at[rows, cols], st_s.at[i], st_r.at[i], owner))
        back_remote.append(remote(stat.at[rows, cols], new_stat.at[rows, cols], ns_s.at[i], ns_r.at[i], owner))

    def mirror(ref):
        for i in range(4):
            for j in range(i + 1, 4):
                a, b = slice(i * TILE, (i + 1) * TILE), slice(j * TILE, (j + 1) * TILE)
                ref[b, a] = ref[a, b].T

    @pl.when(stays)
    def _():
        stat_local.start()

    def columns(slot, half):
        xt = (x + RELATIVE[slot % 4]) % 4
        zt = (1 - zh) if slot < 4 else zh
        block = blocks[0, (xt % 2) * 4 + zt * 2 + xt // 2]
        return act[:, pl.ds(block * BLOCK + half * HALF, HALF)]

    def partial(slot, half):
        return lax.dot_general(
            columns(slot, half), og[...], (((0,), (0,)), ((), ())), preferred_element_type=f32
        )

    def ring_copy(phase, d, step, q):
        index = ((phase * 2 + d) * 3 + step) * QS + q
        source = acc.at[phase * 4 + SEQUENCE[d][step], rows_of(d * QS + q)]
        return remote(source, ring.at[index], ring_s.at[index], ring_r.at[index], side[d])

    started = []

    def ring_start(phase, d, step, q):
        copy = ring_copy(phase, d, step, q)
        copy.start()
        started.append(copy)

    def ring_take(phase, d, step, q):
        index = ((phase * 2 + d) * 3 + step) * QS + q
        ring_copy(phase, d, step, q).wait_recv()
        slot = phase * 4 + SEQUENCE[d][step + 1]
        rows = rows_of(d * QS + q)
        acc[slot, rows] = acc[slot, rows] + ring[index]

    def pair_take(slot):
        pair[slot].wait_recv()
        acc[slot] = acc[slot] + precv[slot]

    for copy in inputs:
        copy.wait()
    pair = []
    for slot in range(8):
        psend[slot] = partial(slot, 1 - c)
        copy = remote(psend.at[slot], precv.at[slot], ps_s.at[slot], ps_r.at[slot], sibling)
        copy.start()
        pair.append(copy)
        acc[slot] = partial(slot, c)
        if slot > 0:
            pair_take(slot - 1)
        if slot == 2:
            for q in range(QS):
                for d in range(2):
                    ring_start(0, d, 0, q)
    pair_take(7)

    def advance(phase, step):
        for q in range(QS):
            for d in range(2):
                ring_take(phase, d, step, q)
                ring_start(phase, d, step + 1, q)

    zcopies = [
        remote(acc.at[3, rows_of(i)], zbuf.at[i], z_s.at[i], z_r.at[i], zmate) for i in range(PIECES)
    ]
    advance(0, 0)
    for d in range(2):
        ring_start(1, d, 0, 0)
    advance(0, 1)
    for q in range(1, QS):
        for d in range(2):
            ring_start(1, d, 0, q)
    for q in range(QS):
        for d in range(2):
            ring_take(0, d, 2, q)
            zcopies[d * QS + q].start()
    advance(1, 0)
    advance(1, 1)

    @pl.when(moves)
    def _():
        for copy in stat_remote:
            copy.start()

    gcopies = []
    for q in range(QS):
        for d in range(2):
            i = d * QS + q
            ring_take(1, d, 2, q)
            zcopies[i].wait_recv()
            here = pl.ds(c * HALF + i * ROWS, ROWS)
            grad[here, :] = acc[7, rows_of(i)] + zbuf[i]
            copy = remote(grad.at[here, :], grad.at[here, :], g_s.at[i], g_r.at[i], sibling)
            copy.start()
            gcopies.append(copy)

    lane = lax.broadcasted_iota(jnp.int32, (8, 128), 1)
    sum_copies = []

    def stage_copy(which, stage, o, peer, slot_of):
        base = which * 20 + (0, 8, 12)[stage]
        mine = base + places[stage]
        theirs = base + (places[stage] + o) % sizes[stage]
        send = sum_s.at[base + o]
        return remote(sums.at[mine], sums.at[mine], send, sum_r.at[mine if slot_of == "send" else theirs], peer)

    def stage_start(which, stage, value):
        base = which * 20 + (0, 8, 12)[stage]
        sums[base + places[stage]] = value
        for o, peer in groups[stage]:
            copy = stage_copy(which, stage, o, peer, "send")
            copy.start()
            sum_copies.append(copy)

    def stage_take(which, stage):
        base = which * 20 + (0, 8, 12)[stage]
        for o, peer in groups[stage]:
            stage_copy(which, stage, o, peer, "recv").wait_recv()
        value = sums[base]
        for i in range(1, sizes[stage]):
            value = value + sums[base + i]
        return value

    mask = eye_mask(BLOCK)
    diagonal = diag[0] + diag[1] + diag[2] + diag[3]
    stat_trace = total(jnp.where(eye_mask(TILE), diagonal, 0.0))
    half = grad[pl.ds(c * HALF, HALF), :]
    square = total(half * half)
    stage_start(0, 0, jnp.where(lane == 0, stat_trace, 0.0) + jnp.where(lane == 1, square, 0.0))

    for copy in gcopies:
        copy.wait_recv()
    gsplit = split(grad[...])

    @pl.when(c == 0)
    def _():
        norm[0] = product(gsplit, gsplit, ((1,), (1,)))

    @pl.when(c == 1)
    def _():
        norm[0] = product(gsplit, gsplit, ((0,), (0,)))

    value = stage_take(0, 0)
    stage_start(0, 1, value)

    @pl.when(stays)
    def _():
        stat_local.wait()

    @pl.when(moves)
    def _():
        for copy in stat_remote:
            copy.wait()
        mirror(stat)

    now = DECAY * stat[...] + norm[0]
    stat[...] = now
    value = stage_take(0, 1)
    stage_start(0, 2, value)
    square_sum = total(now * now)
    now_trace = total(jnp.where(mask, now, 0.0))
    size = jnp.sqrt(square_sum + EPS)
    first = now * (1.0 / size)
    norm[0] = first
    first_split = split(first)
    second = product(first_split, first_split)
    norm[1] = second
    third = product(split(second), first_split)
    norm[2] = third

    value = stage_take(0, 2)

    @pl.when(stays)
    def _():
        new_stat[...] = stat[...]

    @pl.when(moves)
    def _():
        for copy in back_remote:
            copy.start()

    top = lax.broadcasted_iota(jnp.int32, (8, 128), 0) == 0
    trace_all = total(jnp.where(top & (lane == 0), value, 0.0))
    grad_sq = total(jnp.where(top & (lane == 1), value, 0.0))
    shift = DAMPING * ((DECAY * trace_all + 2.0 * grad_sq) / COUNT)
    frob = jnp.sqrt(square_sum + (2.0 * shift * now_trace + BLOCK * shift * shift) + EPS)
    ratio = size / frob
    e = shift / frob
    gain = 1.0 / jnp.sqrt(jnp.sqrt(frob))
    a = (
        25.0 / 16.0, -5.0 / 16.0 - 3125.0 / 4096.0, 3125.0 / 4096.0, -1250.0 / 4096.0,
        250.0 / 4096.0, -25.0 / 4096.0, 1.0 / 4096.0,
    )
    binomial = (
        (1,), (1, 1), (1, 2, 1), (1, 3, 3, 1), (1, 4, 6, 4, 1), (1, 5, 10, 10, 5, 1), (1, 6, 15, 20, 15, 6, 1),
    )
    coefs = []
    scale = gain
    for j in range(7):
        coef = jnp.full_like(e, a[6] * binomial[6][j])
        for i in range(5, j - 1, -1):
            coef = coef * e + a[i] * binomial[i][j]
        coefs.append(coef * scale)
        scale = scale * ratio
    first, second, third = norm[0], norm[1], norm[2]
    upper = coefs[4] * first + coefs[5] * second + coefs[6] * third
    root = coefs[1] * first + coefs[2] * second + coefs[3] * third + jnp.where(mask, coefs[0], 0.0)
    root = root + product(split(third), split(upper))
    roots[c] = root
    root_copy = remote(roots.at[c], roots.at[c], rt_s, rt_r, sibling)
    root_copy.start()
    root_copy.wait_recv()

    mine = roots[0, pl.ds(c * HALF, HALF), :]
    left = product(split(mine), gsplit)
    result = product(split(left), split(roots[1]))
    for i in range(PIECES):
        precond[i] = result[i * ROWS : (i + 1) * ROWS]
    stage_start(1, 0, jnp.where(lane == 0, total(result * result), 0.0))

    def place(xt, zt):
        return (xt * 2 + zt) * 2 + c

    gathers = []

    def spread(i, d2d, source, xt, zt):
        where = gath.at[place(xt, zt), rows_of(i)]
        copy = remote(source, where, gd_s.at[d2d], gd_r.at[d2d], sibling)
        copy.start()
        gathers.append(copy)

    def gather_copy(phase, d, step, q):
        index = ((phase * 2 + d) * 3 + step) * QS + q
        xt = (x + 4 - step) % 4 if d == 0 else (x + step) % 4
        zt = zh if phase == 0 else 1 - zh
        where = gath.at[place(xt, zt), rows_of(d * QS + q)]
        source = precond.at[d * QS + q] if phase == 0 and step == 0 else where
        return remote(source, where, gr_s.at[index], gr_r.at[index], side[d])

    def gather_start(phase, d, step, q):
        copy = gather_copy(phase, d, step, q)
        copy.start()
        gathers.append(copy)

    def gather_take(phase, d, step, q):
        gather_copy(phase, d, step, q).wait_recv()
        if step < 2:
            gather_start(phase, d, step + 1, q)
        xt = (x + 3 - step) % 4 if d == 0 else (x + 1 + step) % 4
        zt = zh if phase == 0 else 1 - zh
        spread(d * QS + q, (phase * 4 + step + 1) * PIECES + d * QS + q, gath.at[place(xt, zt), rows_of(d * QS + q)], xt, zt)

    mates = [
        remote(precond.at[i], gath.at[place(x, zh), rows_of(i)], gz_s.at[i], gz_r.at[i], zmate)
        for i in range(PIECES)
    ]
    order = [(d, q) for q in range(QS) for d in range(2)]
    for d, q in order:
        mates[d * QS + q].start()
        gather_start(0, d, 0, q)
    for i in range(PIECES):
        spread(i, i, precond.at[i], x, zh)
        gath[place(x, zh), rows_of(i)] = precond[i]

    def mate_take(d, q):
        i = d * QS + q
        mates[i].wait_recv()
        gather_start(1, d, 0, q)
        spread(i, 4 * PIECES + i, gath.at[place(x, 1 - zh), rows_of(i)], x, 1 - zh)

    for d, q in order:
        gather_take(0, d, 0, q)
    value = stage_take(1, 0)
    stage_start(1, 1, value)
    mate_take(0, 0)
    for d, q in order:
        gather_take(0, d, 1, q)
    value = stage_take(1, 1)
    stage_start(1, 2, value)
    mate_take(1, 0)
    for d, q in order:
        gather_take(0, d, 2, q)
    for q in range(1, QS):
        for d in range(2):
            mate_take(d, q)

    @pl.when(moves)
    def _():
        for copy in back_remote:
            copy.wait()
        mirror(new_stat)

    for step in range(3):
        for d, q in order:
            gather_take(1, d, step, q)
    value = stage_take(1, 2)
    prec_sq = total(jnp.where(top & (lane == 0), value, 0.0))
    scale_out[...] = jnp.broadcast_to(jnp.sqrt(grad_sq / (prec_sq + EPS)), (8, 128))

    for i in range(8 * PIECES):
        where = gath.at[0, rows_of(i % PIECES)]
        remote(where, where, gd_s.at[i], gd_r.at[i], sibling).wait_recv()
    for copy in pair + started + zcopies + gcopies + sum_copies + [root_copy] + gathers + mates:
        copy.wait_send()


def run_main(blocks, act, og, stat):
    dma = pltpu.SemaphoreType.DMA
    ring_count = 12 * QS
    space = pl.BlockSpec
    return pl.pallas_call(
        main_kernel,
        out_shape=(
            jax.ShapeDtypeStruct((16, HALF, BLOCK), f32),
            jax.ShapeDtypeStruct((BLOCK, BLOCK), f32),
            jax.ShapeDtypeStruct((8, 128), f32),
        ),
        in_specs=[
            space(memory_space=pltpu.SMEM), space(memory_space=pltpu.HBM),
            space(memory_space=pltpu.HBM), space(memory_space=pltpu.HBM),
        ],
        out_specs=(space(memory_space=pltpu.VMEM), space(memory_space=pltpu.VMEM), space(memory_space=pltpu.VMEM)),
        scratch_shapes=[
            pltpu.VMEM((HALF, 4096), bf16),
            pltpu.VMEM((HALF, BLOCK), bf16),
            pltpu.VMEM((4, TILE, TILE), f32),
            pltpu.VMEM((8, HALF, BLOCK), f32),
            pltpu.VMEM((8, HALF, BLOCK), f32),
            pltpu.VMEM((8, HALF, BLOCK), f32),
            pltpu.VMEM((ring_count, ROWS, BLOCK), f32),
            pltpu.VMEM((PIECES, ROWS, BLOCK), f32),
            pltpu.VMEM((BLOCK, BLOCK), f32),
            pltpu.VMEM((BLOCK, BLOCK), f32),
            pltpu.VMEM((3, BLOCK, BLOCK), f32),
            pltpu.VMEM((2, BLOCK, BLOCK), f32),
            pltpu.VMEM((PIECES, ROWS, BLOCK), f32),
            pltpu.VMEM((40, 8, 128), f32),
            dma((8,)), dma((8,)), dma((ring_count,)), dma((ring_count,)), dma((PIECES,)), dma((PIECES,)),
            dma((PIECES,)), dma((PIECES,)), dma((4,)), dma((4,)), dma((4,)), dma((4,)), dma(()), dma(()),
            dma((ring_count,)), dma((ring_count,)), dma((PIECES,)), dma((PIECES,)),
            dma((8 * PIECES,)), dma((8 * PIECES,)), dma(()), dma((40,)), dma((40,)), dma((6,)),
        ],
        compiler_params=pltpu.CompilerParams(
            collective_id=0, has_side_effects=True, vmem_limit_bytes=40 * 1024 * 1024
        ),
        name="shampoo",
    )(blocks, act, og, stat)


def place_kernel(blocks, gath, stat_in, scale, out, stat_out, stage, sem):
    stat_copy = pltpu.make_async_copy(stat_in, stat_out, sem.at[8])
    stat_copy.start()
    copies = []
    for block in range(8):
        pair = jnp.int32(0)
        for p in range(1, 8):
            pair = jnp.where(blocks[0, p] == block, p, pair)
        slot = (pair // 4 + 2 * (pair % 2)) * 2 + (pair // 2) % 2
        for half in range(2):
            stage[block, half * HALF : (half + 1) * HALF] = gath[slot * 2 + half] * scale[0:1, 0:1]
        copy = pltpu.make_async_copy(stage.at[block], out.at[pl.ds(block * BLOCK, BLOCK)], sem.at[block])
        copy.start()
        copies.append(copy)
    for copy in copies:
        copy.wait()
    stat_copy.wait()


def run_place(blocks, gath, stat, scale):
    vmem = pl.BlockSpec(memory_space=pltpu.VMEM)
    hbm = pl.BlockSpec(memory_space=pltpu.HBM)
    return pl.pallas_call(
        place_kernel,
        in_specs=[pl.BlockSpec(memory_space=pltpu.SMEM), vmem, vmem, vmem],
        out_specs=(hbm, hbm),
        out_shape=(
            jax.ShapeDtypeStruct((8 * BLOCK, BLOCK), f32),
            jax.ShapeDtypeStruct((BLOCK, BLOCK), f32),
        ),
        scratch_shapes=[pltpu.VMEM((8, BLOCK, BLOCK), f32), pltpu.SemaphoreType.DMA((9,))],
        compiler_params=pltpu.CompilerParams(vmem_limit_bytes=24 * 1024 * 1024),
        name="place",
    )(blocks, gath, stat, scale)


def per_device(activations, out_grads, statistics, owner_blocks):
    held = [pltpu.with_memory_space_constraint(a, pltpu.HBM) for a in (owner_blocks, activations, out_grads, statistics[0, 0])]
    gath, new_stat, scale = run_main(*held)
    rows, new_stat = run_place(held[0], gath, new_stat, scale)
    return rows, new_stat[None, None]


def solution(mesh):
    return jax.shard_map(
        per_device,
        mesh=mesh,
        in_specs=(P("rep", None), P("rep", "stripe"), P("rep", "stripe", None, None), P("stripe", None)),
        out_specs=(P(None, "stripe"), P("rep", "stripe", None, None)),
        check_vma=False,
    )
```

```python
import functools

import jax
import jax.numpy as jnp
from jax import lax
from jax.experimental import pallas as pl
from jax.experimental.pallas import tpu as pltpu
from jax.sharding import PartitionSpec as P

MESH = pl.DeviceIdType.MESH
f32 = jnp.float32
bf16 = jnp.bfloat16

BLOCK = 512
HALF = 256
TILE = 128
DECAY = 0.95
DAMPING = 0.25
EPS = 1e-06
COUNT = 131072.0

RELATIVE = (3, 1, 2, 0)
SEQUENCE = ((0, 2, 1, 3), (1, 2, 0, 3))
QS = 4
ROWS = HALF // 2 // QS
PIECES = 2 * QS
PAIR, RING, ZX, GRAD, ST, NS, SUMS, ROOT, GRING, GZ, SPREAD = range(11)


def position():
    rep = lax.axis_index("rep")
    stripe = lax.axis_index("stripe")
    return rep // 4, stripe // 4, (rep // 2) % 2, stripe % 4, rep % 2


def device(x, y, z, c):
    return (x * 4 + (z // 4) * 2 + c, y * 4 + z % 4)


def split(a):
    high = a.astype(bf16)
    low = (a - high.astype(f32)).astype(bf16)
    return high, low


def product(a, b, dims=((1,), (0,))):
    (ah, al), (bh, bl) = a, b

    def dot(u, v):
        return lax.dot_general(u, v, (dims, ((), ())), preferred_element_type=f32)

    return dot(ah, bh) + (dot(ah, bl) + dot(al, bh))


def total(a):
    return jnp.sum(jnp.sum(a, axis=0, keepdims=True), axis=1, keepdims=True)


def eye_mask(n):
    return lax.broadcasted_iota(jnp.int32, (n, n), 0) == lax.broadcasted_iota(jnp.int32, (n, n), 1)


def rows_of(piece):
    return pl.ds(piece * ROWS, ROWS)


def main_kernel(
    blocks, act_in, og_in, stat_in,
    gath, new_stat, scale_out,
    act, og, diag, acc, psend, precv, ring, zbuf, grad, stat, norm, roots, precond, sums,
    send, pair_r, ring_r, z_r, one_r, sum_r, own_s, in_s,
):
    x, y, zh, zl, c = position()
    z = zh * 4 + zl
    sibling = device(x, y, z, 1 - c)
    side = (device((x + 1) % 4, y, z, c), device((x + 3) % 4, y, z, c))
    zmate = device(x, y, (z + 4) % 8, c)
    owner = device((x + 2) % 4, y, z, 1 - c)
    stays = c == x // 2
    moves = c != x // 2

    def remote(src, dst, kind, recv, to):
        return pltpu.make_async_remote_copy(
            src_ref=src, dst_ref=dst, send_sem=send.at[kind], recv_sem=recv, device_id=to, device_id_type=MESH
        )

    def sent(kind, size):
        remote(size, size, kind, one_r.at[0], sibling).wait_send()

    def received(recv, size):
        remote(size, size, 0, recv, sibling).wait_recv()

    groups = (
        [(o, device(x, y, (z + o) % 8, c)) for o in range(1, 8)],
        [(o, device(x, (y + o) % 4, z, c)) for o in range(1, 4)],
        [(o, device(((x * 2 + c + o) % 8) // 2, y, z, (x * 2 + c + o) % 2)) for o in range(1, 8)],
    )
    places = (z, y, x * 2 + c)
    sizes = (8, 4, 8)

    inputs = [pltpu.make_async_copy(act_in, act, in_s.at[0]), pltpu.make_async_copy(og_in, og, in_s.at[1])]
    for i in range(4):
        tile = pl.ds(i * TILE, TILE)
        inputs.append(pltpu.make_async_copy(stat_in.at[tile, tile], diag.at[i], in_s.at[2 + i]))
    for copy in inputs:
        copy.start()
    barrier = pltpu.get_barrier_semaphore()
    for group in groups:
        for _, peer in group:
            pl.semaphore_signal(barrier, inc=1, device_id=peer, device_id_type=MESH)
    pl.semaphore_wait(barrier, sum(len(group) for group in groups))

    stat_local = pltpu.make_async_copy(stat_in, stat, own_s)
    stat_remote = []
    back_remote = []
    for i in range(4):
        rows, cols = pl.ds(i * TILE, TILE), pl.ds(i * TILE, BLOCK - i * TILE)
        stat_remote.append(remote(stat_in.at[rows, cols], stat.at[rows, cols], ST, one_r.at[0], owner))
        back_remote.append(remote(stat.at[rows, cols], new_stat.at[rows, cols], NS, one_r.at[1], owner))

    triangle = ring.at[pl.ds(0, (BLOCK + 3 * TILE + 2 * TILE + TILE) * TILE // (ROWS * BLOCK))]

    def mirror(ref):
        for i in range(4):
            for j in range(i + 1, 4):
                a, b = slice(i * TILE, (i + 1) * TILE), slice(j * TILE, (j + 1) * TILE)
                ref[b, a] = ref[a, b].T

    @pl.when(stays)
    def _():
        stat_local.start()

    def columns(slot, half):
        xt = (x + RELATIVE[slot % 4]) % 4
        zt = (1 - zh) if slot < 4 else zh
        block = blocks[0, (xt % 2) * 4 + zt * 2 + xt // 2]
        return act[:, pl.ds(block * BLOCK + half * HALF, HALF)]

    def partial(slot, half):
        return lax.dot_general(
            columns(slot, half), og[...], (((0,), (0,)), ((), ())), preferred_element_type=f32
        )

    def ring_copy(phase, d, step, q):
        index = ((phase * 2 + d) * 3 + step) * QS + q
        source = acc.at[phase * 4 + SEQUENCE[d][step], rows_of(d * QS + q)]
        return remote(source, ring.at[index], RING, ring_r.at[index], side[d])

    def ring_start(phase, d, step, q):
        ring_copy(phase, d, step, q).start()

    def ring_take(phase, d, step, q):
        index = ((phase * 2 + d) * 3 + step) * QS + q
        ring_copy(phase, d, step, q).wait_recv()
        slot = phase * 4 + SEQUENCE[d][step + 1]
        rows = rows_of(d * QS + q)
        acc[slot, rows] = acc[slot, rows] + ring[index]

    def pair_take(slot):
        pair[slot].wait_recv()
        acc[slot] = acc[slot] + precv[slot]

    for copy in inputs:
        copy.wait()
    pair = []

    def pair_start(slot):
        psend[slot] = partial(slot, 1 - c)
        copy = remote(psend.at[slot], precv.at[slot], PAIR, pair_r.at[slot], sibling)
        copy.start()
        pair.append(copy)

    def make(slot):
        pair_start(slot)
        acc[slot] = partial(slot, c)

    def advance(phase, step, qs):
        for q in qs:
            for d in range(2):
                ring_take(phase, d, step, q)
                ring_start(phase, d, step + 1, q)

    zcopies = [remote(acc.at[3, rows_of(i)], zbuf.at[i], ZX, z_r.at[i], zmate) for i in range(PIECES)]
    pair_start(0)
    pair_start(1)
    for slot in range(2):
        acc[slot] = partial(slot, c)
        pair_take(slot)
        for q in range(QS):
            ring_start(0, slot, 0, q)
    make(2)
    make(3)
    pair_take(2)
    advance(0, 0, (0, 1))
    make(4)
    pair_take(3)
    advance(0, 0, (2, 3))
    make(5)
    pair_take(4)
    advance(0, 1, (0, 1))
    make(6)
    pair_take(5)
    advance(0, 1, (2, 3))
    for q in range(QS):
        for d in range(2):
            ring_start(1, d, 0, q)
    make(7)
    pair_take(6)
    for q in range(QS):
        for d in range(2):
            ring_take(0, d, 2, q)
            zcopies[d * QS + q].start()
    pair_take(7)
    advance(1, 0, range(4))
    advance(1, 1, range(4))

    @pl.when(moves)
    def _():
        for copy in stat_remote:
            copy.start()

    for q in range(QS):
        for d in range(2):
            i = d * QS + q
            ring_take(1, d, 2, q)
            zcopies[i].wait_recv()
            here = pl.ds(c * HALF + i * ROWS, ROWS)
            grad[here, :] = acc[7, rows_of(i)] + zbuf[i]
            remote(grad.at[here, :], grad.at[here, :], GRAD, one_r.at[2], sibling).start()

    lane = lax.broadcasted_iota(jnp.int32, (8, 128), 1)

    def stage_start(which, stage, value):
        base = which * 20 + (0, 8, 12)[stage]
        mine = base + places[stage]
        sums[mine] = value
        for _, peer in groups[stage]:
            remote(sums.at[mine], sums.at[mine], SUMS, sum_r.at[which * 3 + stage], peer).start()

    def stage_take(which, stage):
        base = which * 20 + (0, 8, 12)[stage]
        received(sum_r.at[which * 3 + stage], sums.at[pl.ds(base, sizes[stage] - 1)])
        value = sums[base]
        for i in range(1, sizes[stage]):
            value = value + sums[base + i]
        return value

    mask = eye_mask(BLOCK)
    diagonal = diag[0] + diag[1] + diag[2] + diag[3]
    stat_trace = total(jnp.where(eye_mask(TILE), diagonal, 0.0))
    half = grad[pl.ds(c * HALF, HALF), :]
    square = total(half * half)
    stage_start(0, 0, jnp.where(lane == 0, stat_trace, 0.0) + jnp.where(lane == 1, square, 0.0))

    received(one_r.at[2], grad.at[pl.ds(0, HALF), :])
    gsplit = split(grad[...])

    @pl.when(c == 0)
    def _():
        norm[0] = product(gsplit, gsplit, ((1,), (1,)))

    @pl.when(c == 1)
    def _():
        norm[0] = product(gsplit, gsplit, ((0,), (0,)))

    value = stage_take(0, 0)
    stage_start(0, 1, value)

    @pl.when(stays)
    def _():
        stat_local.wait()

    @pl.when(moves)
    def _():
        received(one_r.at[0], triangle)
        mirror(stat)

    now = DECAY * stat[...] + norm[0]
    stat[...] = now
    value = stage_take(0, 1)
    stage_start(0, 2, value)
    square_sum = total(now * now)
    now_trace = total(jnp.where(mask, now, 0.0))
    size = jnp.sqrt(square_sum + EPS)
    first = now * (1.0 / size)
    norm[0] = first
    first_split = split(first)
    second = product(first_split, first_split)
    norm[1] = second
    third = product(split(second), first_split)
    norm[2] = third

    value = stage_take(0, 2)

    @pl.when(stays)
    def _():
        new_stat[...] = stat[...]

    @pl.when(moves)
    def _():
        for copy in back_remote:
            copy.start()

    top = lax.broadcasted_iota(jnp.int32, (8, 128), 0) == 0
    trace_all = total(jnp.where(top & (lane == 0), value, 0.0))
    grad_sq = total(jnp.where(top & (lane == 1), value, 0.0))
    shift = DAMPING * ((DECAY * trace_all + 2.0 * grad_sq) / COUNT)
    frob = jnp.sqrt(square_sum + (2.0 * shift * now_trace + BLOCK * shift * shift) + EPS)
    ratio = size / frob
    e = shift / frob
    gain = 1.0 / jnp.sqrt(jnp.sqrt(frob))
    a = (
        25.0 / 16.0, -5.0 / 16.0 - 3125.0 / 4096.0, 3125.0 / 4096.0, -1250.0 / 4096.0,
        250.0 / 4096.0, -25.0 / 4096.0, 1.0 / 4096.0,
    )
    binomial = (
        (1,), (1, 1), (1, 2, 1), (1, 3, 3, 1), (1, 4, 6, 4, 1), (1, 5, 10, 10, 5, 1), (1, 6, 15, 20, 15, 6, 1),
    )
    coefs = []
    scale = gain
    for j in range(7):
        coef = jnp.full_like(e, a[6] * binomial[6][j])
        for i in range(5, j - 1, -1):
            coef = coef * e + a[i] * binomial[i][j]
        coefs.append(coef * scale)
        scale = scale * ratio
    first, second, third = norm[0], norm[1], norm[2]
    upper = coefs[4] * first + coefs[5] * second + coefs[6] * third
    upper = split(upper)
    low = coefs[1] * first + coefs[2] * second + coefs[3] * third + jnp.where(mask, coefs[0], 0.0)
    for half in (1, 0):
        rows = slice(half * HALF, (half + 1) * HALF)
        roots[c, rows] = low[rows] + product(split(third[rows]), upper)
        part = roots.at[c, pl.ds(half * HALF, HALF)]
        remote(part, part, ROOT, one_r.at[3 + half], sibling).start()
    received(one_r.at[4], grad.at[pl.ds(0, HALF), :])
    left = product(split(roots[0, pl.ds(c * HALF, HALF), :]), gsplit)
    received(one_r.at[3], grad.at[pl.ds(0, HALF), :])
    result = product(split(left), split(roots[1]))
    for i in range(PIECES):
        precond[i] = result[i * ROWS : (i + 1) * ROWS]
    stage_start(1, 0, jnp.where(lane == 0, total(result * result), 0.0))

    def place(xt, zt):
        return (xt * 2 + zt) * 2 + c

    def spread(i, source, xt, zt):
        remote(source, gath.at[place(xt, zt), rows_of(i)], SPREAD, one_r.at[5], sibling).start()

    def gather_copy(phase, d, step, q):
        index = ((phase * 2 + d) * 3 + step) * QS + q
        xt = (x + 4 - step) % 4 if d == 0 else (x + step) % 4
        zt = zh if phase == 0 else 1 - zh
        where = gath.at[place(xt, zt), rows_of(d * QS + q)]
        source = precond.at[d * QS + q] if phase == 0 and step == 0 else where
        return remote(source, where, GRING, ring_r.at[index], side[d])

    def gather_start(phase, d, step, q):
        gather_copy(phase, d, step, q).start()

    def gather_take(phase, d, step, q):
        gather_copy(phase, d, step, q).wait_recv()
        if step < 2:
            gather_start(phase, d, step + 1, q)
        xt = (x + 3 - step) % 4 if d == 0 else (x + 1 + step) % 4
        zt = zh if phase == 0 else 1 - zh
        spread(d * QS + q, gath.at[place(xt, zt), rows_of(d * QS + q)], xt, zt)

    mates = [
        remote(precond.at[i], gath.at[place(x, zh), rows_of(i)], GZ, z_r.at[i], zmate) for i in range(PIECES)
    ]
    order = [(d, q) for q in range(QS) for d in range(2)]
    for d, q in order:
        mates[d * QS + q].start()
        gather_start(0, d, 0, q)
    for i in range(PIECES):
        spread(i, precond.at[i], x, zh)
        gath[place(x, zh), rows_of(i)] = precond[i]

    def mate_take(d, q):
        i = d * QS + q
        mates[i].wait_recv()
        gather_start(1, d, 0, q)
        spread(i, gath.at[place(x, 1 - zh), rows_of(i)], x, 1 - zh)

    def takes(phase, step, qs):
        for q in qs:
            for d in range(2):
                gather_take(phase, d, step, q)

    def mate_takes(q):
        for d in range(2):
            mate_take(d, q)

    takes(0, 0, range(4))
    value = stage_take(1, 0)
    stage_start(1, 1, value)
    mate_takes(0)
    takes(0, 1, range(4))
    value = stage_take(1, 1)
    stage_start(1, 2, value)
    mate_takes(1)

    @pl.when(moves)
    def _():
        received(one_r.at[1], triangle)
        mirror(new_stat)

    takes(1, 0, (0,))
    mate_takes(2)
    takes(1, 0, (1,))
    takes(1, 1, (0,))
    takes(0, 2, range(4))
    mate_takes(3)
    takes(1, 0, (2,))
    takes(1, 1, (1,))
    takes(1, 2, (0,))
    takes(1, 0, (3,))
    takes(1, 1, (2,))
    takes(1, 2, (1,))
    takes(1, 1, (3,))
    takes(1, 2, (2, 3))
    value = stage_take(1, 2)
    prec_sq = total(jnp.where(top & (lane == 0), value, 0.0))
    scale_out[...] = jnp.broadcast_to(jnp.sqrt(grad_sq / (prec_sq + EPS)), (8, 128))

    received(one_r.at[5], acc)
    for kind, size in (
        (PAIR, psend), (RING, psend.at[pl.ds(0, 6)]), (ZX, psend.at[0]), (GRAD, psend.at[0]),
        (SUMS, sums.at[pl.ds(0, 34)]), (ROOT, psend.at[pl.ds(0, 2)]), (GRING, psend.at[pl.ds(0, 6)]),
        (GZ, psend.at[0]), (SPREAD, psend),
    ):
        sent(kind, size)

    @pl.when(moves)
    def _():
        sent(ST, triangle)
        sent(NS, triangle)


def run_main(blocks, act, og, stat):
    dma = pltpu.SemaphoreType.DMA
    ring_count = 12 * QS
    space = pl.BlockSpec
    return pl.pallas_call(
        main_kernel,
        out_shape=(
            jax.ShapeDtypeStruct((16, HALF, BLOCK), f32),
            jax.ShapeDtypeStruct((BLOCK, BLOCK), f32),
            jax.ShapeDtypeStruct((8, 128), f32),
        ),
        in_specs=[
            space(memory_space=pltpu.SMEM), space(memory_space=pltpu.HBM),
            space(memory_space=pltpu.HBM), space(memory_space=pltpu.HBM),
        ],
        out_specs=(space(memory_space=pltpu.VMEM), space(memory_space=pltpu.VMEM), space(memory_space=pltpu.VMEM)),
        scratch_shapes=[
            pltpu.VMEM((HALF, 4096), bf16),
            pltpu.VMEM((HALF, BLOCK), bf16),
            pltpu.VMEM((4, TILE, TILE), f32),
            pltpu.VMEM((8, HALF, BLOCK), f32),
            pltpu.VMEM((8, HALF, BLOCK), f32),
            pltpu.VMEM((8, HALF, BLOCK), f32),
            pltpu.VMEM((ring_count, ROWS, BLOCK), f32),
            pltpu.VMEM((PIECES, ROWS, BLOCK), f32),
            pltpu.VMEM((BLOCK, BLOCK), f32),
            pltpu.VMEM((BLOCK, BLOCK), f32),
            pltpu.VMEM((3, BLOCK, BLOCK), f32),
            pltpu.VMEM((2, BLOCK, BLOCK), f32),
            pltpu.VMEM((PIECES, ROWS, BLOCK), f32),
            pltpu.VMEM((40, 8, 128), f32),
            dma((11,)), dma((8,)), dma((ring_count,)), dma((PIECES,)), dma((6,)), dma((6,)), dma(()), dma((6,)),
        ],
        compiler_params=pltpu.CompilerParams(
            collective_id=0, has_side_effects=True, vmem_limit_bytes=40 * 1024 * 1024
        ),
        name="shampoo",
    )(blocks, act, og, stat)


def place_kernel(blocks, gath, stat_in, scale, out, stat_out, stage, sem):
    stat_copy = pltpu.make_async_copy(stat_in, stat_out, sem.at[8])
    stat_copy.start()
    copies = []
    for block in range(8):
        pair = jnp.int32(0)
        for p in range(1, 8):
            pair = jnp.where(blocks[0, p] == block, p, pair)
        slot = (pair // 4 + 2 * (pair % 2)) * 2 + (pair // 2) % 2
        for half in range(2):
            stage[block, half * HALF : (half + 1) * HALF] = gath[slot * 2 + half] * scale[0:1, 0:1]
        copy = pltpu.make_async_copy(stage.at[block], out.at[pl.ds(block * BLOCK, BLOCK)], sem.at[block])
        copy.start()
        copies.append(copy)
    for copy in copies:
        copy.wait()
    stat_copy.wait()


def run_place(blocks, gath, stat, scale):
    vmem = pl.BlockSpec(memory_space=pltpu.VMEM)
    hbm = pl.BlockSpec(memory_space=pltpu.HBM)
    return pl.pallas_call(
        place_kernel,
        in_specs=[pl.BlockSpec(memory_space=pltpu.SMEM), vmem, vmem, vmem],
        out_specs=(hbm, hbm),
        out_shape=(
            jax.ShapeDtypeStruct((8 * BLOCK, BLOCK), f32),
            jax.ShapeDtypeStruct((BLOCK, BLOCK), f32),
        ),
        scratch_shapes=[pltpu.VMEM((8, BLOCK, BLOCK), f32), pltpu.SemaphoreType.DMA((9,))],
        compiler_params=pltpu.CompilerParams(vmem_limit_bytes=24 * 1024 * 1024),
        name="place",
    )(blocks, gath, stat, scale)


def per_device(activations, out_grads, statistics, owner_blocks):
    held = [pltpu.with_memory_space_constraint(a, pltpu.HBM) for a in (owner_blocks, activations, out_grads, statistics[0, 0])]
    gath, new_stat, scale = run_main(*held)
    rows, new_stat = run_place(held[0], gath, new_stat, scale)
    return rows, new_stat[None, None]


def solution(mesh):
    return jax.shard_map(
        per_device,
        mesh=mesh,
        in_specs=(P("rep", None), P("rep", "stripe"), P("rep", "stripe", None, None), P("stripe", None)),
        out_specs=(P(None, "stripe"), P("rep", "stripe", None, None)),
        check_vma=False,
    )
```

```python
import functools

import jax
import jax.numpy as jnp
from jax import lax
from jax.experimental import pallas as pl
from jax.experimental.pallas import tpu as pltpu
from jax.sharding import PartitionSpec as P

MESH = pl.DeviceIdType.MESH
f32 = jnp.float32
bf16 = jnp.bfloat16

BLOCK = 512
HALF = 256
TILE = 128
DECAY = 0.95
DAMPING = 0.25
EPS = 1e-06
COUNT = 131072.0

RELATIVE = (2, 3, 1, 0)
SOURCES = ((0, 2, 1), (0, 1, 2))
QS = 4
ROWS = HALF // 2 // QS
PIECES = 2 * QS
PAIR, RING, ZX, GRAD, ST, NS, SUMS, ROOT, GRING, GZ, SPREAD = range(11)


def position():
    rep = lax.axis_index("rep")
    stripe = lax.axis_index("stripe")
    return rep // 4, stripe // 4, (rep // 2) % 2, stripe % 4, rep % 2


def device(x, y, z, c):
    return (x * 4 + (z // 4) * 2 + c, y * 4 + z % 4)


def split(a):
    high = a.astype(bf16)
    low = (a - high.astype(f32)).astype(bf16)
    return high, low


def product(a, b, dims=((1,), (0,))):
    (ah, al), (bh, bl) = a, b

    def dot(u, v):
        return lax.dot_general(u, v, (dims, ((), ())), preferred_element_type=f32)

    return dot(ah, bh) + (dot(ah, bl) + dot(al, bh))


def total(a):
    return jnp.sum(jnp.sum(a, axis=0, keepdims=True), axis=1, keepdims=True)


def eye_mask(n):
    return lax.broadcasted_iota(jnp.int32, (n, n), 0) == lax.broadcasted_iota(jnp.int32, (n, n), 1)


def rows_of(piece):
    return pl.ds(piece * ROWS, ROWS)


def main_kernel(
    blocks, act_in, og_in, stat_in,
    gath, new_stat, scale_out,
    act, og, diag, acc, psend, precv, ring, zbuf, grad, stat, norm, roots, precond, sums,
    send, pair_r, ring_r, z_r, one_r, sum_r, own_s, in_s,
):
    x, y, zh, zl, c = position()
    z = zh * 4 + zl
    sibling = device(x, y, z, 1 - c)
    side = (device((x + 1) % 4, y, z, c), device((x + 3) % 4, y, z, c))
    zmate = device(x, y, (z + 4) % 8, c)
    owner = device((x + 2) % 4, y, z, 1 - c)
    stays = c == x // 2
    moves = c != x // 2

    def remote(src, dst, kind, recv, to):
        return pltpu.make_async_remote_copy(
            src_ref=src, dst_ref=dst, send_sem=send.at[kind], recv_sem=recv, device_id=to, device_id_type=MESH
        )

    def sent(kind, size):
        remote(size, size, kind, one_r.at[0], sibling).wait_send()

    def received(recv, size):
        remote(size, size, 0, recv, sibling).wait_recv()

    groups = (
        [(o, device(x, y, (z + o) % 8, c)) for o in range(1, 8)],
        [(o, device(x, (y + o) % 4, z, c)) for o in range(1, 4)],
        [(o, device(((x * 2 + c + o) % 8) // 2, y, z, (x * 2 + c + o) % 2)) for o in range(1, 8)],
    )
    places = (z, y, x * 2 + c)
    sizes = (8, 4, 8)

    inputs = [pltpu.make_async_copy(act_in, act, in_s.at[0]), pltpu.make_async_copy(og_in, og, in_s.at[1])]
    for i in range(4):
        tile = pl.ds(i * TILE, TILE)
        inputs.append(pltpu.make_async_copy(stat_in.at[tile, tile], diag.at[i], in_s.at[2 + i]))
    for copy in inputs:
        copy.start()
    barrier = pltpu.get_barrier_semaphore()
    for group in groups:
        for _, peer in group:
            pl.semaphore_signal(barrier, inc=1, device_id=peer, device_id_type=MESH)
    pl.semaphore_wait(barrier, sum(len(group) for group in groups))

    stat_local = pltpu.make_async_copy(stat_in, stat, own_s)
    stat_remote = []
    back_remote = []
    for i in range(4):
        rows, cols = pl.ds(i * TILE, TILE), pl.ds(i * TILE, BLOCK - i * TILE)
        stat_remote.append(remote(stat_in.at[rows, cols], stat.at[rows, cols], ST, one_r.at[0], owner))
        back_remote.append(remote(stat.at[rows, cols], new_stat.at[rows, cols], NS, one_r.at[1], owner))

    triangle = ring.at[pl.ds(0, (BLOCK + 3 * TILE + 2 * TILE + TILE) * TILE // (ROWS * BLOCK))]

    def mirror(ref):
        for i in range(4):
            for j in range(i + 1, 4):
                a, b = slice(i * TILE, (i + 1) * TILE), slice(j * TILE, (j + 1) * TILE)
                ref[b, a] = ref[a, b].T

    @pl.when(stays)
    def _():
        stat_local.start()

    def columns(slot, half):
        xt = (x + RELATIVE[slot % 4]) % 4
        zt = (1 - zh) if slot < 4 else zh
        block = blocks[0, (xt % 2) * 4 + zt * 2 + xt // 2]
        return act[:, pl.ds(block * BLOCK + half * HALF, HALF)]

    def partial(slot, half):
        return lax.dot_general(
            columns(slot, half), og[...], (((0,), (0,)), ((), ())), preferred_element_type=f32
        )

    def to_side(d, kind):
        return side[1 - d if kind == 2 else d]

    def ring_copy(phase, d, kind, q):
        index = ((phase * 2 + d) * 3 + kind) * QS + q
        source = acc.at[phase * 4 + SOURCES[d][kind], rows_of(d * QS + q)]
        return remote(source, ring.at[index], RING, ring_r.at[index], to_side(d, kind))

    def ring_start(phase, kind, q):
        for d in range(2):
            ring_copy(phase, d, kind, q).start()

    def ring_take(phase, d, kind, q):
        index = ((phase * 2 + d) * 3 + kind) * QS + q
        ring_copy(phase, d, kind, q).wait_recv()
        slot = phase * 4 + (SOURCES[d][1] if kind == 0 else 3)
        rows = rows_of(d * QS + q)
        acc[slot, rows] = acc[slot, rows] + ring[index]

    def pair_take(slot):
        pair[slot].wait_recv()
        acc[slot] = acc[slot] + precv[slot]

    for copy in inputs:
        copy.wait()
    pair = []

    def pair_start(slot):
        psend[slot] = partial(slot, 1 - c)
        copy = remote(psend.at[slot], precv.at[slot], PAIR, pair_r.at[slot], sibling)
        copy.start()
        pair.append(copy)

    def make(slot):
        pair_start(slot)
        acc[slot] = partial(slot, c)

    def advance(phase, qs):
        for q in qs:
            ring_start(phase, 2, q)
            for d in range(2):
                ring_take(phase, d, 0, q)
            ring_start(phase, 1, q)

    zcopies = [remote(acc.at[3, rows_of(i)], zbuf.at[i], ZX, z_r.at[i], zmate) for i in range(PIECES)]
    pair_start(0)
    pair_start(1)
    pair_start(2)
    acc[0] = partial(0, c)
    pair_take(0)
    for q in range(QS):
        ring_start(0, 0, q)
    for slot in range(1, 3):
        acc[slot] = partial(slot, c)
        pair_take(slot)
    advance(0, (0, 1))
    make(3)
    make(4)
    pair_take(3)
    advance(0, (2, 3))
    pair_take(4)
    for q in range(QS):
        ring_start(1, 0, q)
    for slot in range(5, 8):
        make(slot)
        if slot > 5:
            pair_take(slot - 1)
    pair_take(7)
    for q in range(QS):
        for d in range(2):
            for kind in (2, 1):
                ring_take(0, d, kind, q)
            zcopies[d * QS + q].start()
    advance(1, range(4))

    @pl.when(moves)
    def _():
        for copy in stat_remote:
            copy.start()

    for q in range(QS):
        for d in range(2):
            i = d * QS + q
            for kind in (2, 1):
                ring_take(1, d, kind, q)
            zcopies[i].wait_recv()
            here = pl.ds(c * HALF + i * ROWS, ROWS)
            grad[here, :] = acc[7, rows_of(i)] + zbuf[i]
            remote(grad.at[here, :], grad.at[here, :], GRAD, one_r.at[2], sibling).start()

    lane = lax.broadcasted_iota(jnp.int32, (8, 128), 1)

    def stage_start(which, stage, value):
        base = which * 20 + (0, 8, 12)[stage]
        mine = base + places[stage]
        sums[mine] = value
        for _, peer in groups[stage]:
            remote(sums.at[mine], sums.at[mine], SUMS, sum_r.at[which * 3 + stage], peer).start()

    def stage_take(which, stage):
        base = which * 20 + (0, 8, 12)[stage]
        received(sum_r.at[which * 3 + stage], sums.at[pl.ds(base, sizes[stage] - 1)])
        value = sums[base]
        for i in range(1, sizes[stage]):
            value = value + sums[base + i]
        return value

    mask = eye_mask(BLOCK)
    diagonal = diag[0] + diag[1] + diag[2] + diag[3]
    stat_trace = total(jnp.where(eye_mask(TILE), diagonal, 0.0))
    half = grad[pl.ds(c * HALF, HALF), :]
    square = total(half * half)
    stage_start(0, 0, jnp.where(lane == 0, stat_trace, 0.0) + jnp.where(lane == 1, square, 0.0))

    received(one_r.at[2], grad.at[pl.ds(0, HALF), :])
    gsplit = split(grad[...])

    @pl.when(c == 0)
    def _():
        norm[0] = product(gsplit, gsplit, ((1,), (1,)))

    @pl.when(c == 1)
    def _():
        norm[0] = product(gsplit, gsplit, ((0,), (0,)))

    value = stage_take(0, 0)
    stage_start(0, 1, value)
    value = stage_take(0, 1)
    stage_start(0, 2, value)

    @pl.when(stays)
    def _():
        stat_local.wait()

    @pl.when(moves)
    def _():
        received(one_r.at[0], triangle)
        mirror(stat)

    now = DECAY * stat[...] + norm[0]
    stat[...] = now

    @pl.when(stays)
    def _():
        new_stat[...] = now

    @pl.when(moves)
    def _():
        for copy in back_remote:
            copy.start()

    square_sum = total(now * now)
    now_trace = total(jnp.where(mask, now, 0.0))
    size = jnp.sqrt(square_sum + EPS)
    first = now * (1.0 / size)
    norm[0] = first
    first_split = split(first)
    second = product(first_split, first_split)
    norm[1] = second
    third = product(split(second), first_split)
    norm[2] = third

    value = stage_take(0, 2)
    top = lax.broadcasted_iota(jnp.int32, (8, 128), 0) == 0
    trace_all = total(jnp.where(top & (lane == 0), value, 0.0))
    grad_sq = total(jnp.where(top & (lane == 1), value, 0.0))
    shift = DAMPING * ((DECAY * trace_all + 2.0 * grad_sq) / COUNT)
    frob = jnp.sqrt(square_sum + (2.0 * shift * now_trace + BLOCK * shift * shift) + EPS)
    ratio = size / frob
    e = shift / frob
    gain = 1.0 / jnp.sqrt(jnp.sqrt(frob))
    a = (
        25.0 / 16.0, -5.0 / 16.0 - 3125.0 / 4096.0, 3125.0 / 4096.0, -1250.0 / 4096.0,
        250.0 / 4096.0, -25.0 / 4096.0, 1.0 / 4096.0,
    )
    binomial = (
        (1,), (1, 1), (1, 2, 1), (1, 3, 3, 1), (1, 4, 6, 4, 1), (1, 5, 10, 10, 5, 1), (1, 6, 15, 20, 15, 6, 1),
    )
    coefs = []
    scale = gain
    for j in range(7):
        coef = jnp.full_like(e, a[6] * binomial[6][j])
        for i in range(5, j - 1, -1):
            coef = coef * e + a[i] * binomial[i][j]
        coefs.append(coef * scale)
        scale = scale * ratio
    first, second, third = norm[0], norm[1], norm[2]
    upper = coefs[4] * first + coefs[5] * second + coefs[6] * third
    upper = split(upper)
    low = coefs[1] * first + coefs[2] * second + coefs[3] * third + jnp.where(mask, coefs[0], 0.0)
    for half in (1, 0):
        rows = slice(half * HALF, (half + 1) * HALF)
        roots[c, rows] = low[rows] + product(split(third[rows]), upper)
        part = roots.at[c, pl.ds(half * HALF, HALF)]
        remote(part, part, ROOT, one_r.at[3 + half], sibling).start()
    received(one_r.at[4], grad.at[pl.ds(0, HALF), :])
    left = product(split(roots[0, pl.ds(c * HALF, HALF), :]), gsplit)
    received(one_r.at[3], grad.at[pl.ds(0, HALF), :])
    result = product(split(left), split(roots[1]))
    for i in range(PIECES):
        precond[i] = result[i * ROWS : (i + 1) * ROWS]
    stage_start(1, 0, jnp.where(lane == 0, total(result * result), 0.0))

    def place(xt, zt):
        return (xt * 2 + zt) * 2 + c

    def spread(i, source, xt, zt):
        remote(source, gath.at[place(xt, zt), rows_of(i)], SPREAD, one_r.at[5], sibling).start()

    def gather_copy(phase, d, kind, q):
        index = ((phase * 2 + d) * 3 + kind) * QS + q
        xt = x if kind != 1 else (x + 3 + 2 * d) % 4
        zt = zh if phase == 0 else 1 - zh
        where = gath.at[place(xt, zt), rows_of(d * QS + q)]
        source = precond.at[d * QS + q] if phase == 0 and kind != 1 else where
        return remote(source, where, GRING, ring_r.at[index], to_side(d, kind))

    def gather_take(phase, d, kind, q):
        gather_copy(phase, d, kind, q).wait_recv()
        if kind == 0:
            gather_copy(phase, d, 1, q).start()
        xt = (x + (3 + 2 * d, 2, 1 + 2 * d)[kind]) % 4
        zt = zh if phase == 0 else 1 - zh
        spread(d * QS + q, gath.at[place(xt, zt), rows_of(d * QS + q)], xt, zt)

    mates = [
        remote(precond.at[i], gath.at[place(x, zh), rows_of(i)], GZ, z_r.at[i], zmate) for i in range(PIECES)
    ]
    for kind in (0, 2):
        for q in range(QS):
            for d in range(2):
                if kind == 0:
                    mates[d * QS + q].start()
                gather_copy(0, d, kind, q).start()
    for i in range(PIECES):
        spread(i, precond.at[i], x, zh)
        gath[place(x, zh), rows_of(i)] = precond[i]

    def mate_takes(q):
        for d in range(2):
            i = d * QS + q
            mates[i].wait_recv()
            gather_copy(1, d, 0, q).start()
            gather_copy(1, d, 2, q).start()
            spread(i, gath.at[place(x, 1 - zh), rows_of(i)], x, 1 - zh)

    def takes(phase, kind, qs):
        for q in qs:
            for d in range(2):
                gather_take(phase, d, kind, q)

    takes(0, 0, range(4))
    value = stage_take(1, 0)
    stage_start(1, 1, value)
    mate_takes(0)
    takes(0, 2, range(4))
    value = stage_take(1, 1)
    stage_start(1, 2, value)
    mate_takes(1)

    @pl.when(moves)
    def _():
        received(one_r.at[1], triangle)
        mirror(new_stat)

    takes(0, 1, range(4))
    mate_takes(2)
    takes(1, 0, (0, 1))
    takes(1, 2, (0, 1))
    mate_takes(3)
    takes(1, 0, (2,))
    takes(1, 2, (2,))
    takes(1, 1, (0, 1))
    takes(1, 0, (3,))
    takes(1, 2, (3,))
    takes(1, 1, (2, 3))
    value = stage_take(1, 2)
    prec_sq = total(jnp.where(top & (lane == 0), value, 0.0))
    scale_out[...] = jnp.broadcast_to(jnp.sqrt(grad_sq / (prec_sq + EPS)), (8, 128))

    received(one_r.at[5], acc)
    for kind, size in (
        (PAIR, psend), (RING, psend.at[pl.ds(0, 6)]), (ZX, psend.at[0]), (GRAD, psend.at[0]),
        (SUMS, sums.at[pl.ds(0, 34)]), (ROOT, psend.at[pl.ds(0, 2)]), (GRING, psend.at[pl.ds(0, 6)]),
        (GZ, psend.at[0]), (SPREAD, psend),
    ):
        sent(kind, size)

    @pl.when(moves)
    def _():
        sent(ST, triangle)
        sent(NS, triangle)


def run_main(blocks, act, og, stat):
    dma = pltpu.SemaphoreType.DMA
    ring_count = 12 * QS
    space = pl.BlockSpec
    return pl.pallas_call(
        main_kernel,
        out_shape=(
            jax.ShapeDtypeStruct((16, HALF, BLOCK), f32),
            jax.ShapeDtypeStruct((BLOCK, BLOCK), f32),
            jax.ShapeDtypeStruct((8, 128), f32),
        ),
        in_specs=[
            space(memory_space=pltpu.SMEM), space(memory_space=pltpu.HBM),
            space(memory_space=pltpu.HBM), space(memory_space=pltpu.HBM),
        ],
        out_specs=(space(memory_space=pltpu.VMEM), space(memory_space=pltpu.VMEM), space(memory_space=pltpu.VMEM)),
        scratch_shapes=[
            pltpu.VMEM((HALF, 4096), bf16),
            pltpu.VMEM((HALF, BLOCK), bf16),
            pltpu.VMEM((4, TILE, TILE), f32),
            pltpu.VMEM((8, HALF, BLOCK), f32),
            pltpu.VMEM((8, HALF, BLOCK), f32),
            pltpu.VMEM((8, HALF, BLOCK), f32),
            pltpu.VMEM((ring_count, ROWS, BLOCK), f32),
            pltpu.VMEM((PIECES, ROWS, BLOCK), f32),
            pltpu.VMEM((BLOCK, BLOCK), f32),
            pltpu.VMEM((BLOCK, BLOCK), f32),
            pltpu.VMEM((3, BLOCK, BLOCK), f32),
            pltpu.VMEM((2, BLOCK, BLOCK), f32),
            pltpu.VMEM((PIECES, ROWS, BLOCK), f32),
            pltpu.VMEM((40, 8, 128), f32),
            dma((11,)), dma((8,)), dma((ring_count,)), dma((PIECES,)), dma((6,)), dma((6,)), dma(()), dma((6,)),
        ],
        compiler_params=pltpu.CompilerParams(
            collective_id=0, has_side_effects=True, vmem_limit_bytes=40 * 1024 * 1024
        ),
        name="shampoo",
    )(blocks, act, og, stat)


def place_kernel(blocks, gath, stat_in, scale, out, stat_out, stage, sem):
    stat_copy = pltpu.make_async_copy(stat_in, stat_out, sem.at[8])
    stat_copy.start()
    copies = []
    for block in range(8):
        pair = jnp.int32(0)
        for p in range(1, 8):
            pair = jnp.where(blocks[0, p] == block, p, pair)
        slot = (pair // 4 + 2 * (pair % 2)) * 2 + (pair // 2) % 2
        for half in range(2):
            stage[block, half * HALF : (half + 1) * HALF] = gath[slot * 2 + half] * scale[0:1, 0:1]
        copy = pltpu.make_async_copy(stage.at[block], out.at[pl.ds(block * BLOCK, BLOCK)], sem.at[block])
        copy.start()
        copies.append(copy)
    for copy in copies:
        copy.wait()
    stat_copy.wait()


def run_place(blocks, gath, stat, scale):
    vmem = pl.BlockSpec(memory_space=pltpu.VMEM)
    hbm = pl.BlockSpec(memory_space=pltpu.HBM)
    return pl.pallas_call(
        place_kernel,
        in_specs=[pl.BlockSpec(memory_space=pltpu.SMEM), vmem, vmem, vmem],
        out_specs=(hbm, hbm),
        out_shape=(
            jax.ShapeDtypeStruct((8 * BLOCK, BLOCK), f32),
            jax.ShapeDtypeStruct((BLOCK, BLOCK), f32),
        ),
        scratch_shapes=[pltpu.VMEM((8, BLOCK, BLOCK), f32), pltpu.SemaphoreType.DMA((9,))],
        compiler_params=pltpu.CompilerParams(vmem_limit_bytes=24 * 1024 * 1024),
        name="place",
    )(blocks, gath, stat, scale)


def per_device(activations, out_grads, statistics, owner_blocks):
    held = [pltpu.with_memory_space_constraint(a, pltpu.HBM) for a in (owner_blocks, activations, out_grads, statistics[0, 0])]
    gath, new_stat, scale = run_main(*held)
    rows, new_stat = run_place(held[0], gath, new_stat, scale)
    return rows, new_stat[None, None]


def solution(mesh):
    return jax.shard_map(
        per_device,
        mesh=mesh,
        in_specs=(P("rep", None), P("rep", "stripe"), P("rep", "stripe", None, None), P("stripe", None)),
        out_specs=(P(None, "stripe"), P("rep", "stripe", None, None)),
        check_vma=False,
    )
```

```python
import functools

import jax
import jax.numpy as jnp
from jax import lax
from jax.experimental import pallas as pl
from jax.experimental.pallas import tpu as pltpu
from jax.sharding import PartitionSpec as P

MESH = pl.DeviceIdType.MESH
f32 = jnp.float32
bf16 = jnp.bfloat16

BLOCK = 512
HALF = 256
TILE = 128
DECAY = 0.95
DAMPING = 0.25
EPS = 1e-06
COUNT = 131072.0

RELATIVE = (2, 3, 1, 0)
SOURCES = ((0, 2, 1), (0, 1, 2))
QS = 4
ROWS = HALF // 2 // QS
PIECES = 2 * QS
PAIR, RING, ZX, GRAD, ST, NS, SUMS, ROOT, GRING, GZ, SPREAD = range(11)


def position():
    rep = lax.axis_index("rep")
    stripe = lax.axis_index("stripe")
    return rep // 4, stripe // 4, (rep // 2) % 2, stripe % 4, rep % 2


def device(x, y, z, c):
    return (x * 4 + (z // 4) * 2 + c, y * 4 + z % 4)


def split(a):
    high = a.astype(bf16)
    low = (a - high.astype(f32)).astype(bf16)
    return high, low


def product(a, b, dims=((1,), (0,))):
    (ah, al), (bh, bl) = a, b

    def dot(u, v):
        return lax.dot_general(u, v, (dims, ((), ())), preferred_element_type=f32)

    return dot(ah, bh) + (dot(ah, bl) + dot(al, bh))


def total(a):
    return jnp.sum(jnp.sum(a, axis=0, keepdims=True), axis=1, keepdims=True)


def eye_mask(n):
    return lax.broadcasted_iota(jnp.int32, (n, n), 0) == lax.broadcasted_iota(jnp.int32, (n, n), 1)


def rows_of(piece):
    return pl.ds(piece * ROWS, ROWS)


def main_kernel(
    blocks, act_in, og_in, stat_in,
    gath, new_stat, scale_out,
    act, og, diag, acc, psend, precv, ring, zbuf, grad, stat, norm, roots, precond, sums,
    send, pair_r, ring_r, z_r, one_r, sum_r, own_s, in_s,
):
    x, y, zh, zl, c = position()
    z = zh * 4 + zl
    sibling = device(x, y, z, 1 - c)
    side = (device((x + 1) % 4, y, z, c), device((x + 3) % 4, y, z, c))
    zmate = device(x, y, (z + 4) % 8, c)
    owner = device((x + 2) % 4, y, z, 1 - c)
    stays = c == x // 2
    moves = c != x // 2

    def remote(src, dst, kind, recv, to):
        return pltpu.make_async_remote_copy(
            src_ref=src, dst_ref=dst, send_sem=send.at[kind], recv_sem=recv, device_id=to, device_id_type=MESH
        )

    def sent(kind, size):
        remote(size, size, kind, one_r.at[0], sibling).wait_send()

    def received(recv, size):
        remote(size, size, 0, recv, sibling).wait_recv()

    groups = (
        [(o, device(x, y, (z + o) % 8, c)) for o in range(1, 8)],
        [(o, device(x, (y + o) % 4, z, c)) for o in range(1, 4)],
        [(o, device(((x * 2 + c + o) % 8) // 2, y, z, (x * 2 + c + o) % 2)) for o in range(1, 8)],
    )
    places = (z, y, x * 2 + c)
    sizes = (8, 4, 8)

    inputs = [pltpu.make_async_copy(act_in, act, in_s.at[0]), pltpu.make_async_copy(og_in, og, in_s.at[1])]
    for i in range(4):
        tile = pl.ds(i * TILE, TILE)
        inputs.append(pltpu.make_async_copy(stat_in.at[tile, tile], diag.at[i], in_s.at[2 + i]))
    for copy in inputs:
        copy.start()
    barrier = pltpu.get_barrier_semaphore()
    for group in groups:
        for _, peer in group:
            pl.semaphore_signal(barrier, inc=1, device_id=peer, device_id_type=MESH)
    pl.semaphore_wait(barrier, sum(len(group) for group in groups))

    stat_local = pltpu.make_async_copy(stat_in, stat, own_s)
    stat_remote = []
    back_remote = []
    for i in range(4):
        rows, cols = pl.ds(i * TILE, TILE), pl.ds(i * TILE, BLOCK - i * TILE)
        stat_remote.append(remote(stat_in.at[rows, cols], stat.at[rows, cols], ST, one_r.at[0], owner))
        back_remote.append(remote(stat.at[rows, cols], new_stat.at[rows, cols], NS, one_r.at[1], owner))

    triangle = ring.at[pl.ds(0, (BLOCK + 3 * TILE + 2 * TILE + TILE) * TILE // (ROWS * BLOCK))]

    def mirror(ref):
        for i in range(4):
            for j in range(i + 1, 4):
                a, b = slice(i * TILE, (i + 1) * TILE), slice(j * TILE, (j + 1) * TILE)
                ref[b, a] = ref[a, b].T

    @pl.when(stays)
    def _():
        stat_local.start()

    def columns(slot, half):
        xt = (x + RELATIVE[slot % 4]) % 4
        zt = (1 - zh) if slot < 4 else zh
        block = blocks[0, (xt % 2) * 4 + zt * 2 + xt // 2]
        return act[:, pl.ds(block * BLOCK + half * HALF, HALF)]

    def partial(slot, half):
        return lax.dot_general(
            columns(slot, half), og[...], (((0,), (0,)), ((), ())), preferred_element_type=f32
        )

    def to_side(d, kind):
        return side[1 - d if kind == 2 else d]

    def ring_copy(phase, d, kind, q):
        index = ((phase * 2 + d) * 3 + kind) * QS + q
        source = acc.at[phase * 4 + SOURCES[d][kind], rows_of(d * QS + q)]
        return remote(source, ring.at[index], RING, ring_r.at[index], to_side(d, kind))

    def ring_start(phase, kind, q):
        for d in range(2):
            ring_copy(phase, d, kind, q).start()

    def ring_take(phase, d, kind, q):
        index = ((phase * 2 + d) * 3 + kind) * QS + q
        ring_copy(phase, d, kind, q).wait_recv()
        slot = phase * 4 + (SOURCES[d][1] if kind == 0 else 3)
        rows = rows_of(d * QS + q)
        acc[slot, rows] = acc[slot, rows] + ring[index]

    def pair_take(slot):
        pair[slot].wait_recv()
        acc[slot] = acc[slot] + precv[slot]

    for copy in inputs:
        copy.wait()
    pair = []

    def pair_start(slot):
        psend[slot] = partial(slot, 1 - c)
        copy = remote(psend.at[slot], precv.at[slot], PAIR, pair_r.at[slot], sibling)
        copy.start()
        pair.append(copy)

    def make(slot):
        pair_start(slot)
        acc[slot] = partial(slot, c)

    def advance(phase, qs):
        for q in qs:
            ring_start(phase, 2, q)
            for d in range(2):
                ring_take(phase, d, 0, q)
            ring_start(phase, 1, q)

    zcopies = [remote(acc.at[3, rows_of(i)], zbuf.at[i], ZX, z_r.at[i], zmate) for i in range(PIECES)]
    pair_start(0)
    pair_start(1)
    pair_start(2)
    acc[0] = partial(0, c)
    pair_take(0)
    for q in range(QS):
        ring_start(0, 0, q)
    for slot in range(1, 3):
        acc[slot] = partial(slot, c)
        pair_take(slot)
    advance(0, (0, 1))
    make(3)
    make(4)
    pair_take(3)
    advance(0, (2, 3))
    pair_take(4)
    for q in range(QS):
        ring_start(1, 0, q)
    for slot in range(5, 8):
        make(slot)
        if slot > 5:
            pair_take(slot - 1)
    pair_take(7)
    for q in range(QS):
        for d in range(2):
            for kind in (2, 1):
                ring_take(0, d, kind, q)
            zcopies[d * QS + q].start()
    advance(1, range(4))

    @pl.when(moves)
    def _():
        for copy in stat_remote:
            copy.start()

    for q in range(QS):
        for d in range(2):
            i = d * QS + q
            for kind in (2, 1):
                ring_take(1, d, kind, q)
            zcopies[i].wait_recv()
            here = pl.ds(c * HALF + i * ROWS, ROWS)
            grad[here, :] = acc[7, rows_of(i)] + zbuf[i]
            remote(grad.at[here, :], grad.at[here, :], GRAD, one_r.at[2], sibling).start()

    lane = lax.broadcasted_iota(jnp.int32, (8, 128), 1)

    def stage_start(which, stage, value):
        base = which * 20 + (0, 8, 12)[stage]
        mine = base + places[stage]
        sums[mine] = value
        for _, peer in groups[stage]:
            remote(sums.at[mine], sums.at[mine], SUMS, sum_r.at[which * 3 + stage], peer).start()

    def stage_take(which, stage):
        base = which * 20 + (0, 8, 12)[stage]
        received(sum_r.at[which * 3 + stage], sums.at[pl.ds(base, sizes[stage] - 1)])
        value = sums[base]
        for i in range(1, sizes[stage]):
            value = value + sums[base + i]
        return value

    mask = eye_mask(BLOCK)
    diagonal = diag[0] + diag[1] + diag[2] + diag[3]
    stat_trace = total(jnp.where(eye_mask(TILE), diagonal, 0.0))
    half = grad[pl.ds(c * HALF, HALF), :]
    square = total(half * half)
    stage_start(0, 0, jnp.where(lane == 0, stat_trace, 0.0) + jnp.where(lane == 1, square, 0.0))

    received(one_r.at[2], grad.at[pl.ds(0, HALF), :])
    gsplit = split(grad[...])

    @pl.when(c == 0)
    def _():
        norm[0] = product(gsplit, gsplit, ((1,), (1,)))

    @pl.when(c == 1)
    def _():
        norm[0] = product(gsplit, gsplit, ((0,), (0,)))

    value = stage_take(0, 0)
    stage_start(0, 1, value)
    value = stage_take(0, 1)
    stage_start(0, 2, value)

    @pl.when(stays)
    def _():
        stat_local.wait()

    @pl.when(moves)
    def _():
        received(one_r.at[0], triangle)
        mirror(stat)

    now = DECAY * stat[...] + norm[0]
    stat[...] = now

    @pl.when(stays)
    def _():
        new_stat[...] = now

    @pl.when(moves)
    def _():
        for copy in back_remote:
            copy.start()

    square_sum = total(now * now)
    now_trace = total(jnp.where(mask, now, 0.0))
    size = jnp.sqrt(square_sum + EPS)
    first = now * (1.0 / size)
    norm[0] = first
    first_split = split(first)
    second = product(first_split, first_split)
    norm[1] = second
    third = product(split(second), first_split)
    norm[2] = third

    value = stage_take(0, 2)
    top = lax.broadcasted_iota(jnp.int32, (8, 128), 0) == 0
    trace_all = total(jnp.where(top & (lane == 0), value, 0.0))
    grad_sq = total(jnp.where(top & (lane == 1), value, 0.0))
    shift = DAMPING * ((DECAY * trace_all + 2.0 * grad_sq) / COUNT)
    frob = jnp.sqrt(square_sum + (2.0 * shift * now_trace + BLOCK * shift * shift) + EPS)
    ratio = size / frob
    e = shift / frob
    gain = 1.0 / jnp.sqrt(jnp.sqrt(frob))
    a = (
        25.0 / 16.0, -5.0 / 16.0 - 3125.0 / 4096.0, 3125.0 / 4096.0, -1250.0 / 4096.0,
        250.0 / 4096.0, -25.0 / 4096.0, 1.0 / 4096.0,
    )
    binomial = (
        (1,), (1, 1), (1, 2, 1), (1, 3, 3, 1), (1, 4, 6, 4, 1), (1, 5, 10, 10, 5, 1), (1, 6, 15, 20, 15, 6, 1),
    )
    coefs = []
    scale = gain
    for j in range(7):
        coef = jnp.full_like(e, a[6] * binomial[6][j])
        for i in range(5, j - 1, -1):
            coef = coef * e + a[i] * binomial[i][j]
        coefs.append(coef * scale)
        scale = scale * ratio
    first, second, third = norm[0], norm[1], norm[2]
    upper = coefs[4] * first + coefs[5] * second + coefs[6] * third
    upper = split(upper)
    low = coefs[1] * first + coefs[2] * second + coefs[3] * third + jnp.where(mask, coefs[0], 0.0)
    for half in (1, 0):
        rows = slice(half * HALF, (half + 1) * HALF)
        roots[c, rows] = low[rows] + product(split(third[rows]), upper)
        part = roots.at[c, pl.ds(half * HALF, HALF)]
        remote(part, part, ROOT, one_r.at[3 + half], sibling).start()
    received(one_r.at[4], grad.at[pl.ds(0, HALF), :])
    left = product(split(roots[0, pl.ds(c * HALF, HALF), :]), gsplit)
    received(one_r.at[3], grad.at[pl.ds(0, HALF), :])
    result = product(split(left), split(roots[1]))
    for i in range(PIECES):
        precond[i] = result[i * ROWS : (i + 1) * ROWS]
    stage_start(1, 0, jnp.where(lane == 0, total(result * result), 0.0))

    def place(xt, zt):
        return (xt * 2 + zt) * 2 + c

    def spread(i, source, xt, zt):
        remote(source, gath.at[place(xt, zt), rows_of(i)], SPREAD, one_r.at[5], sibling).start()

    def gather_copy(phase, d, step, q):
        index = ((phase * 2 + d) * 3 + step) * QS + q
        xt = (x + 4 - step) % 4 if d == 0 else (x + step) % 4
        zt = zh if phase == 0 else 1 - zh
        where = gath.at[place(xt, zt), rows_of(d * QS + q)]
        source = precond.at[d * QS + q] if phase == 0 and step == 0 else where
        return remote(source, where, GRING, ring_r.at[index], side[d])

    def gather_start(phase, d, step, q):
        gather_copy(phase, d, step, q).start()

    def gather_take(phase, d, step, q):
        gather_copy(phase, d, step, q).wait_recv()
        if step < 2:
            gather_start(phase, d, step + 1, q)
        xt = (x + 3 - step) % 4 if d == 0 else (x + 1 + step) % 4
        zt = zh if phase == 0 else 1 - zh
        spread(d * QS + q, gath.at[place(xt, zt), rows_of(d * QS + q)], xt, zt)

    mates = [
        remote(precond.at[i], gath.at[place(x, zh), rows_of(i)], GZ, z_r.at[i], zmate) for i in range(PIECES)
    ]
    order = [(d, q) for q in range(QS) for d in range(2)]
    for d, q in order:
        mates[d * QS + q].start()
        gather_start(0, d, 0, q)
    for i in range(PIECES):
        spread(i, precond.at[i], x, zh)
        gath[place(x, zh), rows_of(i)] = precond[i]

    def mate_take(d, q):
        i = d * QS + q
        mates[i].wait_recv()
        gather_start(1, d, 0, q)
        spread(i, gath.at[place(x, 1 - zh), rows_of(i)], x, 1 - zh)

    def takes(phase, step, qs):
        for q in qs:
            for d in range(2):
                gather_take(phase, d, step, q)

    def mate_takes(q):
        for d in range(2):
            mate_take(d, q)

    takes(0, 0, range(4))
    value = stage_take(1, 0)
    stage_start(1, 1, value)
    mate_takes(0)
    takes(0, 1, range(4))
    value = stage_take(1, 1)
    stage_start(1, 2, value)
    mate_takes(1)

    @pl.when(moves)
    def _():
        received(one_r.at[1], triangle)
        mirror(new_stat)

    takes(1, 0, (0,))
    mate_takes(2)
    takes(1, 0, (1,))
    takes(1, 1, (0,))
    takes(0, 2, range(4))
    mate_takes(3)
    takes(1, 0, (2,))
    takes(1, 1, (1,))
    takes(1, 2, (0,))
    takes(1, 0, (3,))
    takes(1, 1, (2,))
    takes(1, 2, (1,))
    takes(1, 1, (3,))
    takes(1, 2, (2, 3))
    value = stage_take(1, 2)
    prec_sq = total(jnp.where(top & (lane == 0), value, 0.0))
    scale_out[...] = jnp.broadcast_to(jnp.sqrt(grad_sq / (prec_sq + EPS)), (8, 128))

    received(one_r.at[5], acc)
    for kind, size in (
        (PAIR, psend), (RING, psend.at[pl.ds(0, 6)]), (ZX, psend.at[0]), (GRAD, psend.at[0]),
        (SUMS, sums.at[pl.ds(0, 34)]), (ROOT, psend.at[pl.ds(0, 2)]), (GRING, psend.at[pl.ds(0, 6)]),
        (GZ, psend.at[0]), (SPREAD, psend),
    ):
        sent(kind, size)

    @pl.when(moves)
    def _():
        sent(ST, triangle)
        sent(NS, triangle)


def run_main(blocks, act, og, stat):
    dma = pltpu.SemaphoreType.DMA
    ring_count = 12 * QS
    space = pl.BlockSpec
    return pl.pallas_call(
        main_kernel,
        out_shape=(
            jax.ShapeDtypeStruct((16, HALF, BLOCK), f32),
            jax.ShapeDtypeStruct((BLOCK, BLOCK), f32),
            jax.ShapeDtypeStruct((8, 128), f32),
        ),
        in_specs=[
            space(memory_space=pltpu.SMEM), space(memory_space=pltpu.HBM),
            space(memory_space=pltpu.HBM), space(memory_space=pltpu.HBM),
        ],
        out_specs=(space(memory_space=pltpu.VMEM), space(memory_space=pltpu.VMEM), space(memory_space=pltpu.VMEM)),
        scratch_shapes=[
            pltpu.VMEM((HALF, 4096), bf16),
            pltpu.VMEM((HALF, BLOCK), bf16),
            pltpu.VMEM((4, TILE, TILE), f32),
            pltpu.VMEM((8, HALF, BLOCK), f32),
            pltpu.VMEM((8, HALF, BLOCK), f32),
            pltpu.VMEM((8, HALF, BLOCK), f32),
            pltpu.VMEM((ring_count, ROWS, BLOCK), f32),
            pltpu.VMEM((PIECES, ROWS, BLOCK), f32),
            pltpu.VMEM((BLOCK, BLOCK), f32),
            pltpu.VMEM((BLOCK, BLOCK), f32),
            pltpu.VMEM((3, BLOCK, BLOCK), f32),
            pltpu.VMEM((2, BLOCK, BLOCK), f32),
            pltpu.VMEM((PIECES, ROWS, BLOCK), f32),
            pltpu.VMEM((40, 8, 128), f32),
            dma((11,)), dma((8,)), dma((ring_count,)), dma((PIECES,)), dma((6,)), dma((6,)), dma(()), dma((6,)),
        ],
        compiler_params=pltpu.CompilerParams(
            collective_id=0, has_side_effects=True, vmem_limit_bytes=40 * 1024 * 1024
        ),
        name="shampoo",
    )(blocks, act, og, stat)


def place_kernel(blocks, gath, stat_in, scale, out, stat_out, stage, sem):
    stat_copy = pltpu.make_async_copy(stat_in, stat_out, sem.at[8])
    stat_copy.start()
    copies = []
    for block in range(8):
        pair = jnp.int32(0)
        for p in range(1, 8):
            pair = jnp.where(blocks[0, p] == block, p, pair)
        slot = (pair // 4 + 2 * (pair % 2)) * 2 + (pair // 2) % 2
        for half in range(2):
            stage[block, half * HALF : (half + 1) * HALF] = gath[slot * 2 + half] * scale[0:1, 0:1]
        copy = pltpu.make_async_copy(stage.at[block], out.at[pl.ds(block * BLOCK, BLOCK)], sem.at[block])
        copy.start()
        copies.append(copy)
    for copy in copies:
        copy.wait()
    stat_copy.wait()


def run_place(blocks, gath, stat, scale):
    vmem = pl.BlockSpec(memory_space=pltpu.VMEM)
    hbm = pl.BlockSpec(memory_space=pltpu.HBM)
    return pl.pallas_call(
        place_kernel,
        in_specs=[pl.BlockSpec(memory_space=pltpu.SMEM), vmem, vmem, vmem],
        out_specs=(hbm, hbm),
        out_shape=(
            jax.ShapeDtypeStruct((8 * BLOCK, BLOCK), f32),
            jax.ShapeDtypeStruct((BLOCK, BLOCK), f32),
        ),
        scratch_shapes=[pltpu.VMEM((8, BLOCK, BLOCK), f32), pltpu.SemaphoreType.DMA((9,))],
        compiler_params=pltpu.CompilerParams(vmem_limit_bytes=24 * 1024 * 1024),
        name="place",
    )(blocks, gath, stat, scale)


def per_device(activations, out_grads, statistics, owner_blocks):
    held = [pltpu.with_memory_space_constraint(a, pltpu.HBM) for a in (owner_blocks, activations, out_grads, statistics[0, 0])]
    gath, new_stat, scale = run_main(*held)
    rows, new_stat = run_place(held[0], gath, new_stat, scale)
    return rows, new_stat[None, None]


def solution(mesh):
    return jax.shard_map(
        per_device,
        mesh=mesh,
        in_specs=(P("rep", None), P("rep", "stripe"), P("rep", "stripe", None, None), P("stripe", None)),
        out_specs=(P(None, "stripe"), P("rep", "stripe", None, None)),
        check_vma=False,
    )
```

```python
import functools

import jax
import jax.numpy as jnp
from jax import lax
from jax.experimental import pallas as pl
from jax.experimental.pallas import tpu as pltpu
from jax.sharding import PartitionSpec as P

MESH = pl.DeviceIdType.MESH
f32 = jnp.float32
bf16 = jnp.bfloat16

BLOCK = 512
HALF = 256
TILE = 128
DECAY = 0.95
DAMPING = 0.25
EPS = 1e-06
COUNT = 131072.0

RELATIVE = (2, 3, 1, 0)
SOURCES = ((0, 2, 1), (0, 1, 2))
QS = 4
ROWS = HALF // 2 // QS
PIECES = 2 * QS
PAIR, RING, ZX, GRAD, ST, NS, SUMS, ROOT, GRING, GZ, SPREAD = range(11)


def position():
    rep = lax.axis_index("rep")
    stripe = lax.axis_index("stripe")
    return rep // 4, stripe // 4, (rep // 2) % 2, stripe % 4, rep % 2


def device(x, y, z, c):
    return (x * 4 + (z // 4) * 2 + c, y * 4 + z % 4)


def split(a):
    high = a.astype(bf16)
    low = (a - high.astype(f32)).astype(bf16)
    return high, low


def product(a, b, dims=((1,), (0,))):
    (ah, al), (bh, bl) = a, b

    def dot(u, v):
        return lax.dot_general(u, v, (dims, ((), ())), preferred_element_type=f32)

    return dot(ah, bh) + (dot(ah, bl) + dot(al, bh))


def total(a):
    return jnp.sum(jnp.sum(a, axis=0, keepdims=True), axis=1, keepdims=True)


def eye_mask(n):
    return lax.broadcasted_iota(jnp.int32, (n, n), 0) == lax.broadcasted_iota(jnp.int32, (n, n), 1)


def rows_of(piece):
    return pl.ds(piece * ROWS, ROWS)


def main_kernel(
    blocks, act_in, og_in, stat_in,
    gath, new_stat, scale_out,
    act, og, diag, acc, psend, precv, ring, zbuf, grad, stat, norm, roots, precond, sums,
    send, pair_r, ring_r, z_r, one_r, sum_r, own_s, in_s,
):
    x, y, zh, zl, c = position()
    z = zh * 4 + zl
    sibling = device(x, y, z, 1 - c)
    side = (device((x + 1) % 4, y, z, c), device((x + 3) % 4, y, z, c))
    zmate = device(x, y, (z + 4) % 8, c)
    owner = device((x + 2) % 4, y, z, 1 - c)
    stays = c == x // 2
    moves = c != x // 2

    def remote(src, dst, kind, recv, to):
        return pltpu.make_async_remote_copy(
            src_ref=src, dst_ref=dst, send_sem=send.at[kind], recv_sem=recv, device_id=to, device_id_type=MESH
        )

    def sent(kind, size):
        remote(size, size, kind, one_r.at[0], sibling).wait_send()

    def received(recv, size):
        remote(size, size, 0, recv, sibling).wait_recv()

    groups = (
        [(o, device(x, y, (z + o) % 8, c)) for o in range(1, 8)],
        [(o, device(x, (y + o) % 4, z, c)) for o in range(1, 4)],
        [(o, device(((x * 2 + c + o) % 8) // 2, y, z, (x * 2 + c + o) % 2)) for o in range(1, 8)],
    )
    places = (z, y, x * 2 + c)
    sizes = (8, 4, 8)

    inputs = [pltpu.make_async_copy(act_in, act, in_s.at[0]), pltpu.make_async_copy(og_in, og, in_s.at[1])]
    for i in range(4):
        tile = pl.ds(i * TILE, TILE)
        inputs.append(pltpu.make_async_copy(stat_in.at[tile, tile], diag.at[i], in_s.at[2 + i]))
    for copy in inputs:
        copy.start()
    barrier = pltpu.get_barrier_semaphore()
    for group in groups:
        for _, peer in group:
            pl.semaphore_signal(barrier, inc=1, device_id=peer, device_id_type=MESH)
    pl.semaphore_wait(barrier, sum(len(group) for group in groups))

    stat_local = pltpu.make_async_copy(stat_in, stat, own_s)
    stat_remote = []
    back_remote = []
    for i in range(4):
        rows, cols = pl.ds(i * TILE, TILE), pl.ds(i * TILE, BLOCK - i * TILE)
        stat_remote.append(remote(stat_in.at[rows, cols], stat.at[rows, cols], ST, one_r.at[0], owner))
        back_remote.append(remote(stat.at[rows, cols], new_stat.at[rows, cols], NS, one_r.at[1], owner))

    triangle = ring.at[pl.ds(0, (BLOCK + 3 * TILE + 2 * TILE + TILE) * TILE // (ROWS * BLOCK))]

    def mirror(ref):
        for i in range(4):
            for j in range(i + 1, 4):
                a, b = slice(i * TILE, (i + 1) * TILE), slice(j * TILE, (j + 1) * TILE)
                ref[b, a] = ref[a, b].T

    @pl.when(stays)
    def _():
        stat_local.start()

    def columns(slot, half):
        xt = (x + RELATIVE[slot % 4]) % 4
        zt = (1 - zh) if slot < 4 else zh
        block = blocks[0, (xt % 2) * 4 + zt * 2 + xt // 2]
        return act[:, pl.ds(block * BLOCK + half * HALF, HALF)]

    def partial(slot, half):
        return lax.dot_general(
            columns(slot, half), og[...], (((0,), (0,)), ((), ())), preferred_element_type=f32
        )

    def to_side(d, kind):
        return side[1 - d if kind == 2 else d]

    def ring_copy(phase, d, kind, q):
        index = ((phase * 2 + d) * 3 + kind) * QS + q
        source = acc.at[phase * 4 + SOURCES[d][kind], rows_of(d * QS + q)]
        return remote(source, ring.at[index], RING, ring_r.at[index], to_side(d, kind))

    def ring_start(phase, kind, q):
        for d in range(2):
            ring_copy(phase, d, kind, q).start()

    def ring_take(phase, d, kind, q):
        index = ((phase * 2 + d) * 3 + kind) * QS + q
        ring_copy(phase, d, kind, q).wait_recv()
        slot = phase * 4 + (SOURCES[d][1] if kind == 0 else 3)
        rows = rows_of(d * QS + q)
        acc[slot, rows] = acc[slot, rows] + ring[index]

    def pair_take(slot):
        pair[slot].wait_recv()
        acc[slot] = acc[slot] + precv[slot]

    for copy in inputs:
        copy.wait()
    pair = []

    def pair_start(slot):
        psend[slot] = partial(slot, 1 - c)
        copy = remote(psend.at[slot], precv.at[slot], PAIR, pair_r.at[slot], sibling)
        copy.start()
        pair.append(copy)

    def make(slot):
        pair_start(slot)
        acc[slot] = partial(slot, c)

    def advance(phase, qs):
        for q in qs:
            ring_start(phase, 2, q)
            for d in range(2):
                ring_take(phase, d, 0, q)
            ring_start(phase, 1, q)

    zcopies = [remote(acc.at[3, rows_of(i)], zbuf.at[i], ZX, z_r.at[i], zmate) for i in range(PIECES)]
    pair_start(0)
    pair_start(1)
    pair_start(2)
    acc[0] = partial(0, c)
    pair_take(0)
    for q in range(QS):
        ring_start(0, 0, q)
    for slot in range(1, 3):
        acc[slot] = partial(slot, c)
        pair_take(slot)
    advance(0, (0, 1))
    make(3)
    make(4)
    pair_take(3)
    advance(0, (2, 3))
    pair_take(4)
    for q in range(QS):
        ring_start(1, 0, q)
    for slot in range(5, 8):
        make(slot)
        if slot > 5:
            pair_take(slot - 1)
    pair_take(7)
    for q in range(QS):
        for d in range(2):
            for kind in (2, 1):
                ring_take(0, d, kind, q)
            zcopies[d * QS + q].start()
    advance(1, range(4))

    @pl.when(moves)
    def _():
        for copy in stat_remote:
            copy.start()

    for q in range(QS):
        for d in range(2):
            i = d * QS + q
            for kind in (2, 1):
                ring_take(1, d, kind, q)
            zcopies[i].wait_recv()
            here = pl.ds(c * HALF + i * ROWS, ROWS)
            grad[here, :] = acc[7, rows_of(i)] + zbuf[i]
            remote(grad.at[here, :], grad.at[here, :], GRAD, one_r.at[2], sibling).start()

    lane = lax.broadcasted_iota(jnp.int32, (8, 128), 1)

    def stage_start(which, stage, value):
        base = which * 20 + (0, 8, 12)[stage]
        mine = base + places[stage]
        sums[mine] = value
        for _, peer in groups[stage]:
            remote(sums.at[mine], sums.at[mine], SUMS, sum_r.at[which * 3 + stage], peer).start()

    def stage_take(which, stage):
        base = which * 20 + (0, 8, 12)[stage]
        received(sum_r.at[which * 3 + stage], sums.at[pl.ds(base, sizes[stage] - 1)])
        value = sums[base]
        for i in range(1, sizes[stage]):
            value = value + sums[base + i]
        return value

    mask = eye_mask(BLOCK)
    diagonal = diag[0] + diag[1] + diag[2] + diag[3]
    stat_trace = total(jnp.where(eye_mask(TILE), diagonal, 0.0))
    half = grad[pl.ds(c * HALF, HALF), :]
    square = total(half * half)
    stage_start(0, 0, jnp.where(lane == 0, stat_trace, 0.0) + jnp.where(lane == 1, square, 0.0))

    received(one_r.at[2], grad.at[pl.ds(0, HALF), :])
    gsplit = split(grad[...])

    @pl.when(c == 0)
    def _():
        norm[0] = product(gsplit, gsplit, ((1,), (1,)))

    @pl.when(c == 1)
    def _():
        norm[0] = product(gsplit, gsplit, ((0,), (0,)))

    value = stage_take(0, 0)
    stage_start(0, 1, value)
    value = stage_take(0, 1)
    stage_start(0, 2, value)

    @pl.when(stays)
    def _():
        stat_local.wait()

    @pl.when(moves)
    def _():
        received(one_r.at[0], triangle)
        mirror(stat)

    now = DECAY * stat[...] + norm[0]
    stat[...] = now

    square_sum = total(now * now)
    now_trace = total(jnp.where(mask, now, 0.0))
    size = jnp.sqrt(square_sum + EPS)
    first = now * (1.0 / size)
    norm[0] = first
    first_split = split(first)
    second = product(first_split, first_split)
    norm[1] = second
    third = product(split(second), first_split)
    norm[2] = third

    value = stage_take(0, 2)

    @pl.when(stays)
    def _():
        new_stat[...] = stat[...]

    @pl.when(moves)
    def _():
        for copy in back_remote:
            copy.start()

    top = lax.broadcasted_iota(jnp.int32, (8, 128), 0) == 0
    trace_all = total(jnp.where(top & (lane == 0), value, 0.0))
    grad_sq = total(jnp.where(top & (lane == 1), value, 0.0))
    shift = DAMPING * ((DECAY * trace_all + 2.0 * grad_sq) / COUNT)
    frob = jnp.sqrt(square_sum + (2.0 * shift * now_trace + BLOCK * shift * shift) + EPS)
    ratio = size / frob
    e = shift / frob
    gain = 1.0 / jnp.sqrt(jnp.sqrt(frob))
    a = (
        25.0 / 16.0, -5.0 / 16.0 - 3125.0 / 4096.0, 3125.0 / 4096.0, -1250.0 / 4096.0,
        250.0 / 4096.0, -25.0 / 4096.0, 1.0 / 4096.0,
    )
    binomial = (
        (1,), (1, 1), (1, 2, 1), (1, 3, 3, 1), (1, 4, 6, 4, 1), (1, 5, 10, 10, 5, 1), (1, 6, 15, 20, 15, 6, 1),
    )
    coefs = []
    scale = gain
    for j in range(7):
        coef = jnp.full_like(e, a[6] * binomial[6][j])
        for i in range(5, j - 1, -1):
            coef = coef * e + a[i] * binomial[i][j]
        coefs.append(coef * scale)
        scale = scale * ratio
    first, second, third = norm[0], norm[1], norm[2]
    upper = coefs[4] * first + coefs[5] * second + coefs[6] * third
    upper = split(upper)
    low = coefs[1] * first + coefs[2] * second + coefs[3] * third + jnp.where(mask, coefs[0], 0.0)
    for half in (1, 0):
        rows = slice(half * HALF, (half + 1) * HALF)
        roots[c, rows] = low[rows] + product(split(third[rows]), upper)
        part = roots.at[c, pl.ds(half * HALF, HALF)]
        remote(part, part, ROOT, one_r.at[3 + half], sibling).start()
    received(one_r.at[4], grad.at[pl.ds(0, HALF), :])
    left = product(split(roots[0, pl.ds(c * HALF, HALF), :]), gsplit)
    received(one_r.at[3], grad.at[pl.ds(0, HALF), :])
    result = product(split(left), split(roots[1]))
    for i in range(PIECES):
        precond[i] = result[i * ROWS : (i + 1) * ROWS]
    stage_start(1, 0, jnp.where(lane == 0, total(result * result), 0.0))

    def place(xt, zt):
        return (xt * 2 + zt) * 2 + c

    def spread(i, source, xt, zt):
        remote(source, gath.at[place(xt, zt), rows_of(i)], SPREAD, one_r.at[5], sibling).start()

    def gather_copy(phase, d, kind, q):
        index = ((phase * 2 + d) * 3 + kind) * QS + q
        xt = x if kind != 1 else (x + 3 + 2 * d) % 4
        zt = zh if phase == 0 else 1 - zh
        where = gath.at[place(xt, zt), rows_of(d * QS + q)]
        source = precond.at[d * QS + q] if phase == 0 and kind != 1 else where
        return remote(source, where, GRING, ring_r.at[index], to_side(d, kind))

    def gather_take(phase, d, kind, q):
        gather_copy(phase, d, kind, q).wait_recv()
        if kind == 0:
            gather_copy(phase, d, 1, q).start()
        xt = (x + (3 + 2 * d, 2, 1 + 2 * d)[kind]) % 4
        zt = zh if phase == 0 else 1 - zh
        spread(d * QS + q, gath.at[place(xt, zt), rows_of(d * QS + q)], xt, zt)

    mates = [
        remote(precond.at[i], gath.at[place(x, zh), rows_of(i)], GZ, z_r.at[i], zmate) for i in range(PIECES)
    ]
    for kind in (0, 2):
        for q in range(QS):
            for d in range(2):
                if kind == 0:
                    mates[d * QS + q].start()
                gather_copy(0, d, kind, q).start()
    for i in range(PIECES):
        spread(i, precond.at[i], x, zh)
        gath[place(x, zh), rows_of(i)] = precond[i]

    def mate_takes(q):
        for d in range(2):
            i = d * QS + q
            mates[i].wait_recv()
            gather_copy(1, d, 0, q).start()
            gather_copy(1, d, 2, q).start()
            spread(i, gath.at[place(x, 1 - zh), rows_of(i)], x, 1 - zh)

    def takes(phase, kind, qs):
        for q in qs:
            for d in range(2):
                gather_take(phase, d, kind, q)

    takes(0, 0, range(4))
    value = stage_take(1, 0)
    stage_start(1, 1, value)
    mate_takes(0)
    takes(0, 2, range(4))
    value = stage_take(1, 1)
    stage_start(1, 2, value)
    mate_takes(1)

    @pl.when(moves)
    def _():
        received(one_r.at[1], triangle)
        mirror(new_stat)

    takes(0, 1, range(4))
    mate_takes(2)
    takes(1, 0, (0, 1))
    takes(1, 2, (0, 1))
    mate_takes(3)
    takes(1, 0, (2,))
    takes(1, 2, (2,))
    takes(1, 1, (0, 1))
    takes(1, 0, (3,))
    takes(1, 2, (3,))
    takes(1, 1, (2, 3))
    value = stage_take(1, 2)
    prec_sq = total(jnp.where(top & (lane == 0), value, 0.0))
    scale_out[...] = jnp.broadcast_to(jnp.sqrt(grad_sq / (prec_sq + EPS)), (8, 128))

    received(one_r.at[5], acc)
    for kind, size in (
        (PAIR, psend), (RING, psend.at[pl.ds(0, 6)]), (ZX, psend.at[0]), (GRAD, psend.at[0]),
        (SUMS, sums.at[pl.ds(0, 34)]), (ROOT, psend.at[pl.ds(0, 2)]), (GRING, psend.at[pl.ds(0, 6)]),
        (GZ, psend.at[0]), (SPREAD, psend),
    ):
        sent(kind, size)

    @pl.when(moves)
    def _():
        sent(ST, triangle)
        sent(NS, triangle)


def run_main(blocks, act, og, stat):
    dma = pltpu.SemaphoreType.DMA
    ring_count = 12 * QS
    space = pl.BlockSpec
    return pl.pallas_call(
        main_kernel,
        out_shape=(
            jax.ShapeDtypeStruct((16, HALF, BLOCK), f32),
            jax.ShapeDtypeStruct((BLOCK, BLOCK), f32),
            jax.ShapeDtypeStruct((8, 128), f32),
        ),
        in_specs=[
            space(memory_space=pltpu.SMEM), space(memory_space=pltpu.HBM),
            space(memory_space=pltpu.HBM), space(memory_space=pltpu.HBM),
        ],
        out_specs=(space(memory_space=pltpu.VMEM), space(memory_space=pltpu.VMEM), space(memory_space=pltpu.VMEM)),
        scratch_shapes=[
            pltpu.VMEM((HALF, 4096), bf16),
            pltpu.VMEM((HALF, BLOCK), bf16),
            pltpu.VMEM((4, TILE, TILE), f32),
            pltpu.VMEM((8, HALF, BLOCK), f32),
            pltpu.VMEM((8, HALF, BLOCK), f32),
            pltpu.VMEM((8, HALF, BLOCK), f32),
            pltpu.VMEM((ring_count, ROWS, BLOCK), f32),
            pltpu.VMEM((PIECES, ROWS, BLOCK), f32),
            pltpu.VMEM((BLOCK, BLOCK), f32),
            pltpu.VMEM((BLOCK, BLOCK), f32),
            pltpu.VMEM((3, BLOCK, BLOCK), f32),
            pltpu.VMEM((2, BLOCK, BLOCK), f32),
            pltpu.VMEM((PIECES, ROWS, BLOCK), f32),
            pltpu.VMEM((40, 8, 128), f32),
            dma((11,)), dma((8,)), dma((ring_count,)), dma((PIECES,)), dma((6,)), dma((6,)), dma(()), dma((6,)),
        ],
        compiler_params=pltpu.CompilerParams(
            collective_id=0, has_side_effects=True, vmem_limit_bytes=40 * 1024 * 1024
        ),
        name="shampoo",
    )(blocks, act, og, stat)


def place_kernel(blocks, gath, stat_in, scale, out, stat_out, stage, sem):
    stat_copy = pltpu.make_async_copy(stat_in, stat_out, sem.at[8])
    stat_copy.start()
    copies = []
    for block in range(8):
        pair = jnp.int32(0)
        for p in range(1, 8):
            pair = jnp.where(blocks[0, p] == block, p, pair)
        slot = (pair // 4 + 2 * (pair % 2)) * 2 + (pair // 2) % 2
        for half in range(2):
            stage[block, half * HALF : (half + 1) * HALF] = gath[slot * 2 + half] * scale[0:1, 0:1]
        copy = pltpu.make_async_copy(stage.at[block], out.at[pl.ds(block * BLOCK, BLOCK)], sem.at[block])
        copy.start()
        copies.append(copy)
    for copy in copies:
        copy.wait()
    stat_copy.wait()


def run_place(blocks, gath, stat, scale):
    vmem = pl.BlockSpec(memory_space=pltpu.VMEM)
    hbm = pl.BlockSpec(memory_space=pltpu.HBM)
    return pl.pallas_call(
        place_kernel,
        in_specs=[pl.BlockSpec(memory_space=pltpu.SMEM), vmem, vmem, vmem],
        out_specs=(hbm, hbm),
        out_shape=(
            jax.ShapeDtypeStruct((8 * BLOCK, BLOCK), f32),
            jax.ShapeDtypeStruct((BLOCK, BLOCK), f32),
        ),
        scratch_shapes=[pltpu.VMEM((8, BLOCK, BLOCK), f32), pltpu.SemaphoreType.DMA((9,))],
        compiler_params=pltpu.CompilerParams(vmem_limit_bytes=24 * 1024 * 1024),
        name="place",
    )(blocks, gath, stat, scale)


def per_device(activations, out_grads, statistics, owner_blocks):
    held = [pltpu.with_memory_space_constraint(a, pltpu.HBM) for a in (owner_blocks, activations, out_grads, statistics[0, 0])]
    gath, new_stat, scale = run_main(*held)
    rows, new_stat = run_place(held[0], gath, new_stat, scale)
    return rows, new_stat[None, None]


def solution(mesh):
    return jax.shard_map(
        per_device,
        mesh=mesh,
        in_specs=(P("rep", None), P("rep", "stripe"), P("rep", "stripe", None, None), P("stripe", None)),
        out_specs=(P(None, "stripe"), P("rep", "stripe", None, None)),
        check_vma=False,
    )
```

```python
import functools

import jax
import jax.numpy as jnp
from jax import lax
from jax.experimental import pallas as pl
from jax.experimental.pallas import tpu as pltpu
from jax.sharding import PartitionSpec as P

MESH = pl.DeviceIdType.MESH
f32 = jnp.float32
bf16 = jnp.bfloat16

BLOCK = 512
HALF = 256
TILE = 128
DECAY = 0.95
DAMPING = 0.25
EPS = 1e-06
COUNT = 131072.0

RELATIVE = (2, 3, 1, 0)
SOURCES = ((0, 2, 1), (0, 1, 2))
QS = 4
ROWS = HALF // 2 // QS
PIECES = 2 * QS
LAST = PIECES - 1
PAIR, RING, ZX, GRAD, ST, NS, SUMS, ROOT, GRING, GZ, SPREAD = range(11)


def position():
    rep = lax.axis_index("rep")
    stripe = lax.axis_index("stripe")
    return rep // 4, stripe // 4, (rep // 2) % 2, stripe % 4, rep % 2


def device(x, y, z, c):
    return (x * 4 + (z // 4) * 2 + c, y * 4 + z % 4)


def split(a):
    high = a.astype(bf16)
    low = (a - high.astype(f32)).astype(bf16)
    return high, low


def product(a, b, dims=((1,), (0,))):
    (ah, al), (bh, bl) = a, b

    def dot(u, v):
        return lax.dot_general(u, v, (dims, ((), ())), preferred_element_type=f32)

    return dot(ah, bh) + (dot(ah, bl) + dot(al, bh))


def total(a):
    return jnp.sum(jnp.sum(a, axis=0, keepdims=True), axis=1, keepdims=True)


def eye_mask(n):
    return lax.broadcasted_iota(jnp.int32, (n, n), 0) == lax.broadcasted_iota(jnp.int32, (n, n), 1)


def rows_of(piece):
    return pl.ds(piece * ROWS, ROWS)


def main_kernel(
    blocks, act_in, og_in, stat_in,
    gath, new_stat, scale_out,
    act, og, diag, acc, psend, precv, ring, zbuf, grad, stat, norm, roots, precond, sums,
    send, pair_r, ring_r, z_r, one_r, sum_r, own_s, in_s,
):
    x, y, zh, zl, c = position()
    z = zh * 4 + zl
    sibling = device(x, y, z, 1 - c)
    side = (device((x + 1) % 4, y, z, c), device((x + 3) % 4, y, z, c))
    zmate = device(x, y, (z + 4) % 8, c)
    owner = device((x + 2) % 4, y, z, 1 - c)
    stays = c == x // 2
    moves = c != x // 2

    def remote(src, dst, kind, recv, to):
        return pltpu.make_async_remote_copy(
            src_ref=src, dst_ref=dst, send_sem=send.at[kind], recv_sem=recv, device_id=to, device_id_type=MESH
        )

    def sent(kind, size):
        remote(size, size, kind, one_r.at[0], sibling).wait_send()

    def received(recv, size):
        remote(size, size, 0, recv, sibling).wait_recv()

    groups = (
        [(o, device(x, y, (z + o) % 8, c)) for o in range(1, 8)],
        [(o, device(x, (y + o) % 4, z, c)) for o in range(1, 4)],
        [(o, device(((x * 2 + c + o) % 8) // 2, y, z, (x * 2 + c + o) % 2)) for o in range(1, 8)],
    )
    places = (z, y, x * 2 + c)
    sizes = (8, 4, 8)

    inputs = [pltpu.make_async_copy(act_in, act, in_s.at[0]), pltpu.make_async_copy(og_in, og, in_s.at[1])]
    for i in range(4):
        tile = pl.ds(i * TILE, TILE)
        inputs.append(pltpu.make_async_copy(stat_in.at[tile, tile], diag.at[i], in_s.at[2 + i]))
    for copy in inputs:
        copy.start()
    barrier = pltpu.get_barrier_semaphore()
    for group in groups:
        for _, peer in group:
            pl.semaphore_signal(barrier, inc=1, device_id=peer, device_id_type=MESH)
    pl.semaphore_wait(barrier, sum(len(group) for group in groups))

    stat_local = pltpu.make_async_copy(stat_in, stat, own_s)
    stat_remote = []
    back_remote = []
    for i in range(4):
        rows, cols = pl.ds(i * TILE, TILE), pl.ds(i * TILE, BLOCK - i * TILE)
        stat_remote.append(remote(stat_in.at[rows, cols], stat.at[rows, cols], ST, one_r.at[0], owner))
        back_remote.append(remote(stat.at[rows, cols], new_stat.at[rows, cols], NS, one_r.at[1], owner))

    triangle = ring.at[pl.ds(0, (BLOCK + 3 * TILE + 2 * TILE + TILE) * TILE // (ROWS * BLOCK))]

    def mirror(ref):
        for i in range(4):
            for j in range(i + 1, 4):
                a, b = slice(i * TILE, (i + 1) * TILE), slice(j * TILE, (j + 1) * TILE)
                ref[b, a] = ref[a, b].T

    @pl.when(stays)
    def _():
        stat_local.start()

    def columns(slot, half):
        xt = (x + RELATIVE[slot % 4]) % 4
        zt = (1 - zh) if slot < 4 else zh
        block = blocks[0, (xt % 2) * 4 + zt * 2 + xt // 2]
        return act[:, pl.ds(block * BLOCK + half * HALF, HALF)]

    def partial(slot, half):
        return lax.dot_general(
            columns(slot, half), og[...], (((0,), (0,)), ((), ())), preferred_element_type=f32
        )

    def to_side(d, kind):
        return side[1 - d if kind == 2 else d]

    def ring_copy(phase, d, kind, q):
        index = ((phase * 2 + d) * 3 + kind) * QS + q
        source = acc.at[phase * 4 + SOURCES[d][kind], rows_of(d * QS + q)]
        return remote(source, ring.at[index], RING, ring_r.at[index], to_side(d, kind))

    def halves(phase, q):
        return [d for d in range(2) if phase == 1 or d * QS + q != LAST]

    def ring_start(phase, kind, q):
        for d in halves(phase, q):
            ring_copy(phase, d, kind, q).start()

    def ring_take(phase, d, kind, q):
        index = ((phase * 2 + d) * 3 + kind) * QS + q
        ring_copy(phase, d, kind, q).wait_recv()
        slot = phase * 4 + (SOURCES[d][1] if kind == 0 else 3)
        rows = rows_of(d * QS + q)
        acc[slot, rows] = acc[slot, rows] + ring[index]

    def pair_take(slot):
        pair[slot].wait_recv()
        acc[slot] = acc[slot] + precv[slot]

    for copy in inputs:
        copy.wait()
    pair = []

    def pair_start(slot):
        psend[slot] = partial(slot, 1 - c)
        copy = remote(psend.at[slot], precv.at[slot], PAIR, pair_r.at[slot], sibling)
        copy.start()
        pair.append(copy)

    def make(slot):
        pair_start(slot)
        acc[slot] = partial(slot, c)

    def advance(phase, qs):
        for q in qs:
            ring_start(phase, 2, q)
            for d in halves(phase, q):
                ring_take(phase, d, 0, q)
            ring_start(phase, 1, q)

    zcopies = [remote(acc.at[3, rows_of(i)], zbuf.at[i], ZX, z_r.at[i], zmate) for i in range(LAST)]
    zfirst = [
        remote(acc.at[k, rows_of(LAST)], zbuf.at[LAST + k], ZX, z_r.at[LAST + k], zmate) for k in range(4)
    ]

    def zfirst_take(k):
        zfirst[k].wait_recv()
        acc[4 + k, rows_of(LAST)] = acc[4 + k, rows_of(LAST)] + zbuf[LAST + k]

    pair_start(0)
    pair_start(1)
    pair_start(2)
    acc[0] = partial(0, c)
    pair_take(0)
    for q in range(QS):
        ring_start(0, 0, q)
    zfirst[0].start()
    for slot in range(1, 3):
        acc[slot] = partial(slot, c)
        pair_take(slot)
        zfirst[slot].start()
    advance(0, (0, 1))
    make(3)
    make(4)
    pair_take(3)
    zfirst[3].start()
    advance(0, (2, 3))
    pair_take(4)
    for q in range(QS - 1):
        ring_start(1, 0, q)
    zfirst_take(0)
    ring_start(1, 0, QS - 1)
    for slot in range(5, 8):
        make(slot)
        if slot > 5:
            pair_take(slot - 1)
    pair_take(7)
    for q in range(QS):
        for d in halves(0, q):
            for kind in (2, 1):
                ring_take(0, d, kind, q)
            zcopies[d * QS + q].start()
    for k in range(1, 4):
        zfirst_take(k)
    advance(1, range(4))

    @pl.when(moves)
    def _():
        for copy in stat_remote:
            copy.start()

    for q in range(QS):
        for d in range(2):
            i = d * QS + q
            for kind in (2, 1):
                ring_take(1, d, kind, q)
            here = pl.ds(c * HALF + i * ROWS, ROWS)
            if i == LAST:
                grad[here, :] = acc[7, rows_of(i)]
            else:
                zcopies[i].wait_recv()
                grad[here, :] = acc[7, rows_of(i)] + zbuf[i]
            remote(grad.at[here, :], grad.at[here, :], GRAD, one_r.at[2], sibling).start()

    lane = lax.broadcasted_iota(jnp.int32, (8, 128), 1)

    def stage_start(which, stage, value):
        base = which * 20 + (0, 8, 12)[stage]
        mine = base + places[stage]
        sums[mine] = value
        for _, peer in groups[stage]:
            remote(sums.at[mine], sums.at[mine], SUMS, sum_r.at[which * 3 + stage], peer).start()

    def stage_take(which, stage):
        base = which * 20 + (0, 8, 12)[stage]
        received(sum_r.at[which * 3 + stage], sums.at[pl.ds(base, sizes[stage] - 1)])
        value = sums[base]
        for i in range(1, sizes[stage]):
            value = value + sums[base + i]
        return value

    mask = eye_mask(BLOCK)
    diagonal = diag[0] + diag[1] + diag[2] + diag[3]
    stat_trace = total(jnp.where(eye_mask(TILE), diagonal, 0.0))
    half = grad[pl.ds(c * HALF, HALF), :]
    square = total(half * half)
    stage_start(0, 0, jnp.where(lane == 0, stat_trace, 0.0) + jnp.where(lane == 1, square, 0.0))

    received(one_r.at[2], grad.at[pl.ds(0, HALF), :])
    gsplit = split(grad[...])

    @pl.when(c == 0)
    def _():
        norm[0] = product(gsplit, gsplit, ((1,), (1,)))

    @pl.when(c == 1)
    def _():
        norm[0] = product(gsplit, gsplit, ((0,), (0,)))

    value = stage_take(0, 0)
    stage_start(0, 1, value)
    value = stage_take(0, 1)
    stage_start(0, 2, value)

    @pl.when(stays)
    def _():
        stat_local.wait()

    @pl.when(moves)
    def _():
        received(one_r.at[0], triangle)
        mirror(stat)

    now = DECAY * stat[...] + norm[0]
    stat[...] = now

    square_sum = total(now * now)
    now_trace = total(jnp.where(mask, now, 0.0))
    size = jnp.sqrt(square_sum + EPS)
    first = now * (1.0 / size)
    norm[0] = first
    first_split = split(first)
    second = product(first_split, first_split)
    norm[1] = second
    third = product(split(second), first_split)
    norm[2] = third

    value = stage_take(0, 2)

    @pl.when(stays)
    def _():
        new_stat[...] = stat[...]

    @pl.when(moves)
    def _():
        for copy in back_remote:
            copy.start()

    top = lax.broadcasted_iota(jnp.int32, (8, 128), 0) == 0
    trace_all = total(jnp.where(top & (lane == 0), value, 0.0))
    grad_sq = total(jnp.where(top & (lane == 1), value, 0.0))
    shift = DAMPING * ((DECAY * trace_all + 2.0 * grad_sq) / COUNT)
    frob = jnp.sqrt(square_sum + (2.0 * shift * now_trace + BLOCK * shift * shift) + EPS)
    ratio = size / frob
    e = shift / frob
    gain = 1.0 / jnp.sqrt(jnp.sqrt(frob))
    a = (
        25.0 / 16.0, -5.0 / 16.0 - 3125.0 / 4096.0, 3125.0 / 4096.0, -1250.0 / 4096.0,
        250.0 / 4096.0, -25.0 / 4096.0, 1.0 / 4096.0,
    )
    binomial = (
        (1,), (1, 1), (1, 2, 1), (1, 3, 3, 1), (1, 4, 6, 4, 1), (1, 5, 10, 10, 5, 1), (1, 6, 15, 20, 15, 6, 1),
    )
    coefs = []
    scale = gain
    for j in range(7):
        coef = jnp.full_like(e, a[6] * binomial[6][j])
        for i in range(5, j - 1, -1):
            coef = coef * e + a[i] * binomial[i][j]
        coefs.append(coef * scale)
        scale = scale * ratio
    first, second, third = norm[0], norm[1], norm[2]
    upper = coefs[4] * first + coefs[5] * second + coefs[6] * third
    upper = split(upper)
    low = coefs[1] * first + coefs[2] * second + coefs[3] * third + jnp.where(mask, coefs[0], 0.0)
    for half in (1, 0):
        rows = slice(half * HALF, (half + 1) * HALF)
        roots[c, rows] = low[rows] + product(split(third[rows]), upper)
        part = roots.at[c, pl.ds(half * HALF, HALF)]
        remote(part, part, ROOT, one_r.at[3 + half], sibling).start()
    received(one_r.at[4], grad.at[pl.ds(0, HALF), :])
    left = product(split(roots[0, pl.ds(c * HALF, HALF), :]), gsplit)
    received(one_r.at[3], grad.at[pl.ds(0, HALF), :])
    result = product(split(left), split(roots[1]))
    for i in range(PIECES):
        precond[i] = result[i * ROWS : (i + 1) * ROWS]
    stage_start(1, 0, jnp.where(lane == 0, total(result * result), 0.0))

    def place(xt, zt):
        return (xt * 2 + zt) * 2 + c

    def spread(i, source, xt, zt):
        remote(source, gath.at[place(xt, zt), rows_of(i)], SPREAD, one_r.at[5], sibling).start()

    def gather_copy(phase, d, kind, q):
        index = ((phase * 2 + d) * 3 + kind) * QS + q
        xt = x if kind != 1 else (x + 3 + 2 * d) % 4
        zt = zh if phase == 0 else 1 - zh
        where = gath.at[place(xt, zt), rows_of(d * QS + q)]
        source = precond.at[d * QS + q] if phase == 0 and kind != 1 else where
        return remote(source, where, GRING, ring_r.at[index], to_side(d, kind))

    def gather_take(phase, d, kind, q):
        gather_copy(phase, d, kind, q).wait_recv()
        if kind == 0:
            gather_copy(phase, d, 1, q).start()
        xt = (x + (3 + 2 * d, 2, 1 + 2 * d)[kind]) % 4
        zt = zh if phase == 0 else 1 - zh
        if phase == 0 and d * QS + q == LAST:
            last_copy(xt, zt, (kind + 1)).start()
        spread(d * QS + q, gath.at[place(xt, zt), rows_of(d * QS + q)], xt, zt)

    def last_copy(xt, zt, k):
        where = gath.at[place(xt, zt), rows_of(LAST)]
        source = precond.at[LAST] if k == 0 else where
        return remote(source, where, GZ, z_r.at[LAST + k], zmate)

    def last_take(k):
        xt = x if k == 0 else (x + (5, 2, 3)[k - 1]) % 4
        last_copy(xt, 1 - zh, k).wait_recv()
        spread(LAST, gath.at[place(xt, 1 - zh), rows_of(LAST)], xt, 1 - zh)

    mates = [
        remote(precond.at[i], gath.at[place(x, zh), rows_of(i)], GZ, z_r.at[i], zmate) for i in range(LAST)
    ]
    for kind in (0, 2):
        for q in range(QS):
            for d in range(2):
                if kind == 0:
                    (last_copy(x, zh, 0) if d * QS + q == LAST else mates[d * QS + q]).start()
                gather_copy(0, d, kind, q).start()
    for i in range(PIECES):
        spread(i, precond.at[i], x, zh)
        gath[place(x, zh), rows_of(i)] = precond[i]

    def mate_takes(q):
        for d in halves(0, q):
            i = d * QS + q
            mates[i].wait_recv()
            gather_copy(1, d, 0, q).start()
            gather_copy(1, d, 2, q).start()
            spread(i, gath.at[place(x, 1 - zh), rows_of(i)], x, 1 - zh)

    def takes(phase, kind, qs):
        for q in qs:
            for d in halves(1 - phase, q):
                gather_take(phase, d, kind, q)

    takes(0, 0, range(4))
    value = stage_take(1, 0)
    stage_start(1, 1, value)
    mate_takes(0)
    takes(0, 2, range(4))
    value = stage_take(1, 1)
    stage_start(1, 2, value)
    mate_takes(1)

    @pl.when(moves)
    def _():
        received(one_r.at[1], triangle)
        mirror(new_stat)

    takes(0, 1, range(4))
    mate_takes(2)
    takes(1, 0, (0, 1))
    takes(1, 2, (0, 1))
    mate_takes(3)
    takes(1, 0, (2,))
    takes(1, 2, (2,))
    takes(1, 1, (0, 1))
    takes(1, 0, (3,))
    takes(1, 2, (3,))
    last_take(0)
    last_take(1)
    takes(1, 1, (2,))
    last_take(3)
    takes(1, 1, (3,))
    last_take(2)
    value = stage_take(1, 2)
    prec_sq = total(jnp.where(top & (lane == 0), value, 0.0))
    scale_out[...] = jnp.broadcast_to(jnp.sqrt(grad_sq / (prec_sq + EPS)), (8, 128))

    received(one_r.at[5], acc)
    for kind, size in (
        (PAIR, psend), (RING, ring.at[pl.ds(0, 12 * QS - 3)]), (ZX, ring.at[pl.ds(0, LAST + 4)]), (GRAD, psend.at[0]),
        (SUMS, sums.at[pl.ds(0, 34)]), (ROOT, psend.at[pl.ds(0, 2)]), (GRING, ring.at[pl.ds(0, 12 * QS - 3)]),
        (GZ, ring.at[pl.ds(0, LAST + 4)]), (SPREAD, psend),
    ):
        sent(kind, size)

    @pl.when(moves)
    def _():
        sent(ST, triangle)
        sent(NS, triangle)


def run_main(blocks, act, og, stat):
    dma = pltpu.SemaphoreType.DMA
    ring_count = 12 * QS
    space = pl.BlockSpec
    return pl.pallas_call(
        main_kernel,
        out_shape=(
            jax.ShapeDtypeStruct((16, HALF, BLOCK), f32),
            jax.ShapeDtypeStruct((BLOCK, BLOCK), f32),
            jax.ShapeDtypeStruct((8, 128), f32),
        ),
        in_specs=[
            space(memory_space=pltpu.SMEM), space(memory_space=pltpu.HBM),
            space(memory_space=pltpu.HBM), space(memory_space=pltpu.HBM),
        ],
        out_specs=(space(memory_space=pltpu.VMEM), space(memory_space=pltpu.VMEM), space(memory_space=pltpu.VMEM)),
        scratch_shapes=[
            pltpu.VMEM((HALF, 4096), bf16),
            pltpu.VMEM((HALF, BLOCK), bf16),
            pltpu.VMEM((4, TILE, TILE), f32),
            pltpu.VMEM((8, HALF, BLOCK), f32),
            pltpu.VMEM((8, HALF, BLOCK), f32),
            pltpu.VMEM((8, HALF, BLOCK), f32),
            pltpu.VMEM((ring_count, ROWS, BLOCK), f32),
            pltpu.VMEM((LAST + 4, ROWS, BLOCK), f32),
            pltpu.VMEM((BLOCK, BLOCK), f32),
            pltpu.VMEM((BLOCK, BLOCK), f32),
            pltpu.VMEM((3, BLOCK, BLOCK), f32),
            pltpu.VMEM((2, BLOCK, BLOCK), f32),
            pltpu.VMEM((PIECES, ROWS, BLOCK), f32),
            pltpu.VMEM((40, 8, 128), f32),
            dma((11,)), dma((8,)), dma((ring_count,)), dma((LAST + 4,)), dma((6,)), dma((6,)), dma(()), dma((6,)),
        ],
        compiler_params=pltpu.CompilerParams(
            collective_id=0, has_side_effects=True, vmem_limit_bytes=40 * 1024 * 1024
        ),
        name="shampoo",
    )(blocks, act, og, stat)


def place_kernel(blocks, gath, stat_in, scale, out, stat_out, stage, sem):
    stat_copy = pltpu.make_async_copy(stat_in, stat_out, sem.at[8])
    stat_copy.start()
    copies = []
    for block in range(8):
        pair = jnp.int32(0)
        for p in range(1, 8):
            pair = jnp.where(blocks[0, p] == block, p, pair)
        slot = (pair // 4 + 2 * (pair % 2)) * 2 + (pair // 2) % 2
        for half in range(2):
            stage[block, half * HALF : (half + 1) * HALF] = gath[slot * 2 + half] * scale[0:1, 0:1]
        copy = pltpu.make_async_copy(stage.at[block], out.at[pl.ds(block * BLOCK, BLOCK)], sem.at[block])
        copy.start()
        copies.append(copy)
    for copy in copies:
        copy.wait()
    stat_copy.wait()


def run_place(blocks, gath, stat, scale):
    vmem = pl.BlockSpec(memory_space=pltpu.VMEM)
    hbm = pl.BlockSpec(memory_space=pltpu.HBM)
    return pl.pallas_call(
        place_kernel,
        in_specs=[pl.BlockSpec(memory_space=pltpu.SMEM), vmem, vmem, vmem],
        out_specs=(hbm, hbm),
        out_shape=(
            jax.ShapeDtypeStruct((8 * BLOCK, BLOCK), f32),
            jax.ShapeDtypeStruct((BLOCK, BLOCK), f32),
        ),
        scratch_shapes=[pltpu.VMEM((8, BLOCK, BLOCK), f32), pltpu.SemaphoreType.DMA((9,))],
        compiler_params=pltpu.CompilerParams(vmem_limit_bytes=24 * 1024 * 1024),
        name="place",
    )(blocks, gath, stat, scale)


def per_device(activations, out_grads, statistics, owner_blocks):
    held = [pltpu.with_memory_space_constraint(a, pltpu.HBM) for a in (owner_blocks, activations, out_grads, statistics[0, 0])]
    gath, new_stat, scale = run_main(*held)
    rows, new_stat = run_place(held[0], gath, new_stat, scale)
    return rows, new_stat[None, None]


def solution(mesh):
    return jax.shard_map(
        per_device,
        mesh=mesh,
        in_specs=(P("rep", None), P("rep", "stripe"), P("rep", "stripe", None, None), P("stripe", None)),
        out_specs=(P(None, "stripe"), P("rep", "stripe", None, None)),
        check_vma=False,
    )
```

```python
import functools

import jax
import jax.numpy as jnp
from jax import lax
from jax.experimental import pallas as pl
from jax.experimental.pallas import tpu as pltpu
from jax.sharding import PartitionSpec as P

MESH = pl.DeviceIdType.MESH
f32 = jnp.float32
bf16 = jnp.bfloat16

BLOCK = 512
HALF = 256
TILE = 128
DECAY = 0.95
DAMPING = 0.25
EPS = 1e-06
COUNT = 131072.0

RELATIVE = (2, 3, 1, 0)
SOURCES = ((0, 2, 1), (0, 1, 2))
QS = 4
ROWS = HALF // 2 // QS
PIECES = 2 * QS
LAST = PIECES - 1
PAIR, RING, ZX, GRAD, ST, NS, SUMS, ROOT, GRING, GZ, SPREAD = range(11)


def position():
    rep = lax.axis_index("rep")
    stripe = lax.axis_index("stripe")
    return rep // 4, stripe // 4, (rep // 2) % 2, stripe % 4, rep % 2


def device(x, y, z, c):
    return (x * 4 + (z // 4) * 2 + c, y * 4 + z % 4)


def split(a):
    high = a.astype(bf16)
    low = (a - high.astype(f32)).astype(bf16)
    return high, low


def product(a, b, dims=((1,), (0,))):
    (ah, al), (bh, bl) = a, b

    def dot(u, v):
        return lax.dot_general(u, v, (dims, ((), ())), preferred_element_type=f32)

    return dot(ah, bh) + (dot(ah, bl) + dot(al, bh))


def total(a):
    return jnp.sum(jnp.sum(a, axis=0, keepdims=True), axis=1, keepdims=True)


def eye_mask(n):
    return lax.broadcasted_iota(jnp.int32, (n, n), 0) == lax.broadcasted_iota(jnp.int32, (n, n), 1)


def rows_of(piece):
    return pl.ds(piece * ROWS, ROWS)


def main_kernel(
    blocks, act_in, og_in, stat_in,
    gath, new_stat, scale_out,
    act, og, diag, acc, psend, precv, ring, zbuf, grad, stat, norm, roots, precond, sums,
    send, pair_r, ring_r, z_r, one_r, sum_r, own_s, in_s,
):
    x, y, zh, zl, c = position()
    z = zh * 4 + zl
    sibling = device(x, y, z, 1 - c)
    side = (device((x + 1) % 4, y, z, c), device((x + 3) % 4, y, z, c))
    zmate = device(x, y, (z + 4) % 8, c)
    owner = device((x + 2) % 4, y, z, 1 - c)
    stays = c == x // 2
    moves = c != x // 2

    def remote(src, dst, kind, recv, to):
        return pltpu.make_async_remote_copy(
            src_ref=src, dst_ref=dst, send_sem=send.at[kind], recv_sem=recv, device_id=to, device_id_type=MESH
        )

    def sent(kind, size):
        remote(size, size, kind, one_r.at[0], sibling).wait_send()

    def received(recv, size):
        remote(size, size, 0, recv, sibling).wait_recv()

    groups = (
        [(o, device(x, y, (z + o) % 8, c)) for o in range(1, 8)],
        [(o, device(x, (y + o) % 4, z, c)) for o in range(1, 4)],
        [(o, device(((x * 2 + c + o) % 8) // 2, y, z, (x * 2 + c + o) % 2)) for o in range(1, 8)],
    )
    places = (z, y, x * 2 + c)
    sizes = (8, 4, 8)

    inputs = [pltpu.make_async_copy(act_in, act, in_s.at[0]), pltpu.make_async_copy(og_in, og, in_s.at[1])]
    for i in range(4):
        tile = pl.ds(i * TILE, TILE)
        inputs.append(pltpu.make_async_copy(stat_in.at[tile, tile], diag.at[i], in_s.at[2 + i]))
    for copy in inputs:
        copy.start()
    barrier = pltpu.get_barrier_semaphore()
    for group in groups:
        for _, peer in group:
            pl.semaphore_signal(barrier, inc=1, device_id=peer, device_id_type=MESH)
    pl.semaphore_wait(barrier, sum(len(group) for group in groups))

    stat_local = pltpu.make_async_copy(stat_in, stat, own_s)
    stat_remote = []
    back_remote = []
    for i in range(4):
        rows, cols = pl.ds(i * TILE, TILE), pl.ds(i * TILE, BLOCK - i * TILE)
        stat_remote.append(remote(stat_in.at[rows, cols], stat.at[rows, cols], ST, one_r.at[0], owner))
        back_remote.append(remote(stat.at[rows, cols], new_stat.at[rows, cols], NS, one_r.at[1], owner))

    triangle = ring.at[pl.ds(0, (BLOCK + 3 * TILE + 2 * TILE + TILE) * TILE // (ROWS * BLOCK))]

    def mirror(ref):
        for i in range(4):
            for j in range(i + 1, 4):
                a, b = slice(i * TILE, (i + 1) * TILE), slice(j * TILE, (j + 1) * TILE)
                ref[b, a] = ref[a, b].T

    @pl.when(stays)
    def _():
        stat_local.start()

    def columns(slot, half):
        xt = (x + RELATIVE[slot % 4]) % 4
        zt = (1 - zh) if slot < 4 else zh
        block = blocks[0, (xt % 2) * 4 + zt * 2 + xt // 2]
        return act[:, pl.ds(block * BLOCK + half * HALF, HALF)]

    def partial(slot, half):
        return lax.dot_general(
            columns(slot, half), og[...], (((0,), (0,)), ((), ())), preferred_element_type=f32
        )

    def to_side(d, kind):
        return side[1 - d if kind == 2 else d]

    def ring_copy(phase, d, kind, q):
        index = ((phase * 2 + d) * 3 + kind) * QS + q
        source = acc.at[phase * 4 + SOURCES[d][kind], rows_of(d * QS + q)]
        return remote(source, ring.at[index], RING, ring_r.at[index], to_side(d, kind))

    def halves(phase, q):
        return [d for d in range(2) if phase == 1 or d * QS + q != LAST]

    def ring_start(phase, kind, q):
        for d in halves(phase, q):
            ring_copy(phase, d, kind, q).start()

    def ring_take(phase, d, kind, q):
        index = ((phase * 2 + d) * 3 + kind) * QS + q
        ring_copy(phase, d, kind, q).wait_recv()
        slot = phase * 4 + (SOURCES[d][1] if kind == 0 else 3)
        rows = rows_of(d * QS + q)
        acc[slot, rows] = acc[slot, rows] + ring[index]

    def pair_take(slot):
        pair[slot].wait_recv()
        acc[slot] = acc[slot] + precv[slot]

    for copy in inputs:
        copy.wait()
    pair = []

    def pair_start(slot):
        psend[slot] = partial(slot, 1 - c)
        copy = remote(psend.at[slot], precv.at[slot], PAIR, pair_r.at[slot], sibling)
        copy.start()
        pair.append(copy)

    def make(slot):
        pair_start(slot)
        acc[slot] = partial(slot, c)

    def advance(phase, qs):
        for q in qs:
            ring_start(phase, 2, q)
            for d in halves(phase, q):
                ring_take(phase, d, 0, q)
            ring_start(phase, 1, q)

    zcopies = [remote(acc.at[3, rows_of(i)], zbuf.at[i], ZX, z_r.at[i], zmate) for i in range(LAST)]
    zfirst = [
        remote(acc.at[k, rows_of(LAST)], zbuf.at[LAST + k], ZX, z_r.at[LAST + k], zmate) for k in range(4)
    ]

    def zfirst_take(k):
        zfirst[k].wait_recv()
        acc[4 + k, rows_of(LAST)] = acc[4 + k, rows_of(LAST)] + zbuf[LAST + k]

    pair_start(0)
    pair_start(1)
    pair_start(2)
    acc[0] = partial(0, c)
    pair_take(0)
    for q in range(QS):
        ring_start(0, 0, q)
    zfirst[0].start()
    for slot in range(1, 3):
        acc[slot] = partial(slot, c)
        pair_take(slot)
        zfirst[slot].start()
    advance(0, (0, 1))
    make(3)
    make(4)
    pair_take(3)
    zfirst[3].start()
    advance(0, (2, 3))
    pair_take(4)
    for q in range(QS - 1):
        ring_start(1, 0, q)
    zfirst_take(0)
    ring_start(1, 0, QS - 1)
    for slot in range(5, 8):
        make(slot)
        if slot > 5:
            pair_take(slot - 1)
    pair_take(7)
    for q in range(QS):
        for d in halves(0, q):
            for kind in (2, 1):
                ring_take(0, d, kind, q)
            zcopies[d * QS + q].start()
    for k in range(1, 4):
        zfirst_take(k)
    advance(1, range(4))

    @pl.when(moves)
    def _():
        for copy in stat_remote:
            copy.start()

    for q in range(QS):
        for d in range(2):
            i = d * QS + q
            for kind in (2, 1):
                ring_take(1, d, kind, q)
            here = pl.ds(c * HALF + i * ROWS, ROWS)
            if i == LAST:
                grad[here, :] = acc[7, rows_of(i)]
            else:
                zcopies[i].wait_recv()
                grad[here, :] = acc[7, rows_of(i)] + zbuf[i]
            remote(grad.at[here, :], grad.at[here, :], GRAD, one_r.at[2], sibling).start()

    lane = lax.broadcasted_iota(jnp.int32, (8, 128), 1)

    def stage_start(which, stage, value):
        base = which * 20 + (0, 8, 12)[stage]
        mine = base + places[stage]
        sums[mine] = value
        for _, peer in groups[stage]:
            remote(sums.at[mine], sums.at[mine], SUMS, sum_r.at[which * 3 + stage], peer).start()

    def stage_take(which, stage):
        base = which * 20 + (0, 8, 12)[stage]
        received(sum_r.at[which * 3 + stage], sums.at[pl.ds(base, sizes[stage] - 1)])
        value = sums[base]
        for i in range(1, sizes[stage]):
            value = value + sums[base + i]
        return value

    mask = eye_mask(BLOCK)
    diagonal = diag[0] + diag[1] + diag[2] + diag[3]
    stat_trace = total(jnp.where(eye_mask(TILE), diagonal, 0.0))
    half = grad[pl.ds(c * HALF, HALF), :]
    square = total(half * half)
    stage_start(0, 0, jnp.where(lane == 0, stat_trace, 0.0) + jnp.where(lane == 1, square, 0.0))

    received(one_r.at[2], grad.at[pl.ds(0, HALF), :])
    gsplit = split(grad[...])

    @pl.when(c == 0)
    def _():
        norm[0] = product(gsplit, gsplit, ((1,), (1,)))

    @pl.when(c == 1)
    def _():
        norm[0] = product(gsplit, gsplit, ((0,), (0,)))

    value = stage_take(0, 0)
    stage_start(0, 1, value)
    value = stage_take(0, 1)
    stage_start(0, 2, value)

    @pl.when(stays)
    def _():
        stat_local.wait()

    @pl.when(moves)
    def _():
        received(one_r.at[0], triangle)
        mirror(stat)

    now = DECAY * stat[...] + norm[0]
    stat[...] = now

    square_sum = total(now * now)
    now_trace = total(jnp.where(mask, now, 0.0))
    size = jnp.sqrt(square_sum + EPS)
    first = now * (1.0 / size)
    norm[0] = first
    first_split = split(first)
    second = product(first_split, first_split)
    norm[1] = second
    third = product(split(second), first_split)
    norm[2] = third

    value = stage_take(0, 2)

    @pl.when(stays)
    def _():
        new_stat[...] = stat[...]

    @pl.when(moves)
    def _():
        for copy in back_remote:
            copy.start()

    top = lax.broadcasted_iota(jnp.int32, (8, 128), 0) == 0
    trace_all = total(jnp.where(top & (lane == 0), value, 0.0))
    grad_sq = total(jnp.where(top & (lane == 1), value, 0.0))
    shift = DAMPING * ((DECAY * trace_all + 2.0 * grad_sq) / COUNT)
    frob = jnp.sqrt(square_sum + (2.0 * shift * now_trace + BLOCK * shift * shift) + EPS)
    ratio = size / frob
    e = shift / frob
    gain = 1.0 / jnp.sqrt(jnp.sqrt(frob))
    a = (
        25.0 / 16.0, -5.0 / 16.0 - 3125.0 / 4096.0, 3125.0 / 4096.0, -1250.0 / 4096.0,
        250.0 / 4096.0, -25.0 / 4096.0, 1.0 / 4096.0,
    )
    binomial = (
        (1,), (1, 1), (1, 2, 1), (1, 3, 3, 1), (1, 4, 6, 4, 1), (1, 5, 10, 10, 5, 1), (1, 6, 15, 20, 15, 6, 1),
    )
    coefs = []
    scale = gain
    for j in range(7):
        coef = jnp.full_like(e, a[6] * binomial[6][j])
        for i in range(5, j - 1, -1):
            coef = coef * e + a[i] * binomial[i][j]
        coefs.append(coef * scale)
        scale = scale * ratio
    first, second, third = norm[0], norm[1], norm[2]
    upper = coefs[4] * first + coefs[5] * second + coefs[6] * third
    upper = split(upper)
    low = coefs[1] * first + coefs[2] * second + coefs[3] * third + jnp.where(mask, coefs[0], 0.0)
    for half in (1, 0):
        rows = slice(half * HALF, (half + 1) * HALF)
        roots[c, rows] = low[rows] + product(split(third[rows]), upper)
        part = roots.at[c, pl.ds(half * HALF, HALF)]
        remote(part, part, ROOT, one_r.at[3 + half], sibling).start()
    received(one_r.at[4], grad.at[pl.ds(0, HALF), :])
    left = product(split(roots[0, pl.ds(c * HALF, HALF), :]), gsplit)
    received(one_r.at[3], grad.at[pl.ds(0, HALF), :])
    result = product(split(left), split(roots[1]))
    for i in range(PIECES):
        precond[i] = result[i * ROWS : (i + 1) * ROWS]
    stage_start(1, 0, jnp.where(lane == 0, total(result * result), 0.0))

    def place(xt, zt):
        return (xt * 2 + zt) * 2 + c

    def spread(i, source, xt, zt):
        remote(source, gath.at[place(xt, zt), rows_of(i)], SPREAD, one_r.at[5], sibling).start()

    def gather_copy(phase, d, kind, q):
        index = ((phase * 2 + d) * 3 + kind) * QS + q
        xt = x if kind != 1 else (x + 3 + 2 * d) % 4
        zt = zh if phase == 0 else 1 - zh
        where = gath.at[place(xt, zt), rows_of(d * QS + q)]
        source = precond.at[d * QS + q] if phase == 0 and kind != 1 else where
        return remote(source, where, GRING, ring_r.at[index], to_side(d, kind))

    def gather_take(phase, d, kind, q):
        gather_copy(phase, d, kind, q).wait_recv()
        if kind == 0:
            gather_copy(phase, d, 1, q).start()
        xt = (x + (3 + 2 * d, 2, 1 + 2 * d)[kind]) % 4
        zt = zh if phase == 0 else 1 - zh
        spread(d * QS + q, gath.at[place(xt, zt), rows_of(d * QS + q)], xt, zt)

    mates = [
        remote(precond.at[i], gath.at[place(x, zh), rows_of(i)], GZ, z_r.at[i], zmate) for i in range(PIECES)
    ]
    for kind in (0, 2):
        for q in range(QS):
            for d in range(2):
                if kind == 0:
                    mates[d * QS + q].start()
                gather_copy(0, d, kind, q).start()
    for i in range(PIECES):
        spread(i, precond.at[i], x, zh)
        gath[place(x, zh), rows_of(i)] = precond[i]

    def mate_takes(q):
        for d in range(2):
            i = d * QS + q
            mates[i].wait_recv()
            gather_copy(1, d, 0, q).start()
            gather_copy(1, d, 2, q).start()
            spread(i, gath.at[place(x, 1 - zh), rows_of(i)], x, 1 - zh)

    def takes(phase, kind, qs):
        for q in qs:
            for d in range(2):
                gather_take(phase, d, kind, q)

    takes(0, 0, range(4))
    value = stage_take(1, 0)
    stage_start(1, 1, value)
    mate_takes(0)
    takes(0, 2, range(4))
    value = stage_take(1, 1)
    stage_start(1, 2, value)
    mate_takes(1)

    @pl.when(moves)
    def _():
        received(one_r.at[1], triangle)
        mirror(new_stat)

    takes(0, 1, range(4))
    mate_takes(2)
    takes(1, 0, (0, 1))
    takes(1, 2, (0, 1))
    mate_takes(3)
    takes(1, 0, (2,))
    takes(1, 2, (2,))
    takes(1, 1, (0, 1))
    takes(1, 0, (3,))
    takes(1, 2, (3,))
    takes(1, 1, (2, 3))
    value = stage_take(1, 2)
    prec_sq = total(jnp.where(top & (lane == 0), value, 0.0))
    scale_out[...] = jnp.broadcast_to(jnp.sqrt(grad_sq / (prec_sq + EPS)), (8, 128))

    received(one_r.at[5], acc)
    for kind, size in (
        (PAIR, psend), (RING, ring.at[pl.ds(0, 12 * QS - 3)]), (ZX, ring.at[pl.ds(0, LAST + 4)]), (GRAD, psend.at[0]),
        (SUMS, sums.at[pl.ds(0, 34)]), (ROOT, psend.at[pl.ds(0, 2)]), (GRING, psend.at[pl.ds(0, 6)]),
        (GZ, psend.at[0]), (SPREAD, psend),
    ):
        sent(kind, size)

    @pl.when(moves)
    def _():
        sent(ST, triangle)
        sent(NS, triangle)


def run_main(blocks, act, og, stat):
    dma = pltpu.SemaphoreType.DMA
    ring_count = 12 * QS
    space = pl.BlockSpec
    return pl.pallas_call(
        main_kernel,
        out_shape=(
            jax.ShapeDtypeStruct((16, HALF, BLOCK), f32),
            jax.ShapeDtypeStruct((BLOCK, BLOCK), f32),
            jax.ShapeDtypeStruct((8, 128), f32),
        ),
        in_specs=[
            space(memory_space=pltpu.SMEM), space(memory_space=pltpu.HBM),
            space(memory_space=pltpu.HBM), space(memory_space=pltpu.HBM),
        ],
        out_specs=(space(memory_space=pltpu.VMEM), space(memory_space=pltpu.VMEM), space(memory_space=pltpu.VMEM)),
        scratch_shapes=[
            pltpu.VMEM((HALF, 4096), bf16),
            pltpu.VMEM((HALF, BLOCK), bf16),
            pltpu.VMEM((4, TILE, TILE), f32),
            pltpu.VMEM((8, HALF, BLOCK), f32),
            pltpu.VMEM((8, HALF, BLOCK), f32),
            pltpu.VMEM((8, HALF, BLOCK), f32),
            pltpu.VMEM((ring_count, ROWS, BLOCK), f32),
            pltpu.VMEM((LAST + 4, ROWS, BLOCK), f32),
            pltpu.VMEM((BLOCK, BLOCK), f32),
            pltpu.VMEM((BLOCK, BLOCK), f32),
            pltpu.VMEM((3, BLOCK, BLOCK), f32),
            pltpu.VMEM((2, BLOCK, BLOCK), f32),
            pltpu.VMEM((PIECES, ROWS, BLOCK), f32),
            pltpu.VMEM((40, 8, 128), f32),
            dma((11,)), dma((8,)), dma((ring_count,)), dma((LAST + 4,)), dma((6,)), dma((6,)), dma(()), dma((6,)),
        ],
        compiler_params=pltpu.CompilerParams(
            collective_id=0, has_side_effects=True, vmem_limit_bytes=40 * 1024 * 1024
        ),
        name="shampoo",
    )(blocks, act, og, stat)


def place_kernel(blocks, gath, stat_in, scale, out, stat_out, stage, sem):
    stat_copy = pltpu.make_async_copy(stat_in, stat_out, sem.at[8])
    stat_copy.start()
    copies = []
    for block in range(8):
        pair = jnp.int32(0)
        for p in range(1, 8):
            pair = jnp.where(blocks[0, p] == block, p, pair)
        slot = (pair // 4 + 2 * (pair % 2)) * 2 + (pair // 2) % 2
        for half in range(2):
            stage[block, half * HALF : (half + 1) * HALF] = gath[slot * 2 + half] * scale[0:1, 0:1]
        copy = pltpu.make_async_copy(stage.at[block], out.at[pl.ds(block * BLOCK, BLOCK)], sem.at[block])
        copy.start()
        copies.append(copy)
    for copy in copies:
        copy.wait()
    stat_copy.wait()


def run_place(blocks, gath, stat, scale):
    vmem = pl.BlockSpec(memory_space=pltpu.VMEM)
    hbm = pl.BlockSpec(memory_space=pltpu.HBM)
    return pl.pallas_call(
        place_kernel,
        in_specs=[pl.BlockSpec(memory_space=pltpu.SMEM), vmem, vmem, vmem],
        out_specs=(hbm, hbm),
        out_shape=(
            jax.ShapeDtypeStruct((8 * BLOCK, BLOCK), f32),
            jax.ShapeDtypeStruct((BLOCK, BLOCK), f32),
        ),
        scratch_shapes=[pltpu.VMEM((8, BLOCK, BLOCK), f32), pltpu.SemaphoreType.DMA((9,))],
        compiler_params=pltpu.CompilerParams(vmem_limit_bytes=24 * 1024 * 1024),
        name="place",
    )(blocks, gath, stat, scale)


def per_device(activations, out_grads, statistics, owner_blocks):
    held = [pltpu.with_memory_space_constraint(a, pltpu.HBM) for a in (owner_blocks, activations, out_grads, statistics[0, 0])]
    gath, new_stat, scale = run_main(*held)
    rows, new_stat = run_place(held[0], gath, new_stat, scale)
    return rows, new_stat[None, None]


def solution(mesh):
    return jax.shard_map(
        per_device,
        mesh=mesh,
        in_specs=(P("rep", None), P("rep", "stripe"), P("rep", "stripe", None, None), P("stripe", None)),
        out_specs=(P(None, "stripe"), P("rep", "stripe", None, None)),
        check_vma=False,
    )
```

```python
import functools

import jax
import jax.numpy as jnp
from jax import lax
from jax.experimental import pallas as pl
from jax.experimental.pallas import tpu as pltpu
from jax.sharding import PartitionSpec as P

MESH = pl.DeviceIdType.MESH
f32 = jnp.float32
bf16 = jnp.bfloat16

BLOCK = 512
HALF = 256
TILE = 128
DECAY = 0.95
DAMPING = 0.25
EPS = 1e-06
COUNT = 131072.0

RELATIVE = (2, 3, 1, 0)
SOURCES = ((0, 2, 1), (0, 1, 2))
QS = 4
ROWS = HALF // 2 // QS
PIECES = 2 * QS
LAST = PIECES - 1
PAIR, RING, ZX, GRAD, ST, NS, SUMS, ROOT, GRING, GZ, SPREAD = range(11)


def position():
    rep = lax.axis_index("rep")
    stripe = lax.axis_index("stripe")
    return rep // 4, stripe // 4, (rep // 2) % 2, stripe % 4, rep % 2


def device(x, y, z, c):
    return (x * 4 + (z // 4) * 2 + c, y * 4 + z % 4)


def split(a):
    high = a.astype(bf16)
    low = (a - high.astype(f32)).astype(bf16)
    return high, low


def product(a, b, dims=((1,), (0,))):
    (ah, al), (bh, bl) = a, b

    def dot(u, v):
        return lax.dot_general(u, v, (dims, ((), ())), preferred_element_type=f32)

    return dot(ah, bh) + (dot(ah, bl) + dot(al, bh))


def total(a):
    return jnp.sum(jnp.sum(a, axis=0, keepdims=True), axis=1, keepdims=True)


def eye_mask(n):
    return lax.broadcasted_iota(jnp.int32, (n, n), 0) == lax.broadcasted_iota(jnp.int32, (n, n), 1)


def rows_of(piece):
    return pl.ds(piece * ROWS, ROWS)


def main_kernel(
    blocks, act_in, og_in, stat_in,
    gath, new_stat, scale_out,
    act, og, diag, acc, psend, precv, ring, zbuf, grad, stat, norm, roots, precond, sums,
    send, pair_r, ring_r, z_r, one_r, sum_r, own_s, in_s,
):
    x, y, zh, zl, c = position()
    z = zh * 4 + zl
    sibling = device(x, y, z, 1 - c)
    side = (device((x + 1) % 4, y, z, c), device((x + 3) % 4, y, z, c))
    zmate = device(x, y, (z + 4) % 8, c)
    owner = device((x + 2) % 4, y, z, 1 - c)
    stays = c == x // 2
    moves = c != x // 2

    def remote(src, dst, kind, recv, to):
        return pltpu.make_async_remote_copy(
            src_ref=src, dst_ref=dst, send_sem=send.at[kind], recv_sem=recv, device_id=to, device_id_type=MESH
        )

    def sent(kind, size):
        remote(size, size, kind, one_r.at[0], sibling).wait_send()

    def received(recv, size):
        remote(size, size, 0, recv, sibling).wait_recv()

    groups = (
        [(o, device(x, y, (z + o) % 8, c)) for o in range(1, 8)],
        [(o, device(x, (y + o) % 4, z, c)) for o in range(1, 4)],
        [(o, device(((x * 2 + c + o) % 8) // 2, y, z, (x * 2 + c + o) % 2)) for o in range(1, 8)],
    )
    places = (z, y, x * 2 + c)
    sizes = (8, 4, 8)

    inputs = [pltpu.make_async_copy(act_in, act, in_s.at[0]), pltpu.make_async_copy(og_in, og, in_s.at[1])]
    for i in range(4):
        tile = pl.ds(i * TILE, TILE)
        inputs.append(pltpu.make_async_copy(stat_in.at[tile, tile], diag.at[i], in_s.at[2 + i]))
    for copy in inputs:
        copy.start()
    barrier = pltpu.get_barrier_semaphore()
    for group in groups:
        for _, peer in group:
            pl.semaphore_signal(barrier, inc=1, device_id=peer, device_id_type=MESH)
    pl.semaphore_wait(barrier, sum(len(group) for group in groups))

    stat_local = pltpu.make_async_copy(stat_in, stat, own_s)
    stat_remote = []
    back_remote = []
    for i in range(4):
        rows, cols = pl.ds(i * TILE, TILE), pl.ds(i * TILE, BLOCK - i * TILE)
        stat_remote.append(remote(stat_in.at[rows, cols], stat.at[rows, cols], ST, one_r.at[0], owner))
        back_remote.append(remote(stat.at[rows, cols], new_stat.at[rows, cols], NS, one_r.at[1], owner))

    triangle = ring.at[pl.ds(0, (BLOCK + 3 * TILE + 2 * TILE + TILE) * TILE // (ROWS * BLOCK))]

    def mirror(ref):
        for i in range(4):
            for j in range(i + 1, 4):
                a, b = slice(i * TILE, (i + 1) * TILE), slice(j * TILE, (j + 1) * TILE)
                ref[b, a] = ref[a, b].T

    @pl.when(stays)
    def _():
        stat_local.start()

    def columns(slot, half):
        xt = (x + RELATIVE[slot % 4]) % 4
        zt = (1 - zh) if slot < 4 else zh
        block = blocks[0, (xt % 2) * 4 + zt * 2 + xt // 2]
        return act[:, pl.ds(block * BLOCK + half * HALF, HALF)]

    def partial(slot, half):
        return lax.dot_general(
            columns(slot, half), og[...], (((0,), (0,)), ((), ())), preferred_element_type=f32
        )

    def to_side(d, kind):
        return side[1 - d if kind == 2 else d]

    def ring_copy(phase, d, kind, q):
        index = ((phase * 2 + d) * 3 + kind) * QS + q
        source = acc.at[phase * 4 + SOURCES[d][kind], rows_of(d * QS + q)]
        return remote(source, ring.at[index], RING, ring_r.at[index], to_side(d, kind))

    def halves(phase, q):
        return [d for d in range(2) if phase == 1 or d * QS + q != LAST]

    def ring_start(phase, kind, q):
        for d in halves(phase, q):
            ring_copy(phase, d, kind, q).start()

    def ring_take(phase, d, kind, q):
        index = ((phase * 2 + d) * 3 + kind) * QS + q
        ring_copy(phase, d, kind, q).wait_recv()
        slot = phase * 4 + (SOURCES[d][1] if kind == 0 else 3)
        rows = rows_of(d * QS + q)
        acc[slot, rows] = acc[slot, rows] + ring[index]

    def pair_take(slot):
        pair[slot].wait_recv()
        acc[slot] = acc[slot] + precv[slot]

    for copy in inputs:
        copy.wait()
    pair = []

    def pair_start(slot):
        psend[slot] = partial(slot, 1 - c)
        copy = remote(psend.at[slot], precv.at[slot], PAIR, pair_r.at[slot], sibling)
        copy.start()
        pair.append(copy)

    def make(slot):
        pair_start(slot)
        acc[slot] = partial(slot, c)

    def advance(phase, qs):
        for q in qs:
            ring_start(phase, 2, q)
            for d in halves(phase, q):
                ring_take(phase, d, 0, q)
            ring_start(phase, 1, q)

    zcopies = [remote(acc.at[3, rows_of(i)], zbuf.at[i], ZX, z_r.at[i], zmate) for i in range(LAST)]
    zfirst = [
        remote(acc.at[k, rows_of(LAST)], zbuf.at[LAST + k], ZX, z_r.at[LAST + k], zmate) for k in range(4)
    ]

    def zfirst_take(k):
        zfirst[k].wait_recv()
        acc[4 + k, rows_of(LAST)] = acc[4 + k, rows_of(LAST)] + zbuf[LAST + k]

    pair_start(0)
    pair_start(1)
    pair_start(2)
    acc[0] = partial(0, c)
    pair_take(0)
    for q in range(QS):
        ring_start(0, 0, q)
    zfirst[0].start()
    for slot in range(1, 3):
        acc[slot] = partial(slot, c)
        pair_take(slot)
        zfirst[slot].start()
    advance(0, (0, 1))
    make(3)
    make(4)
    pair_take(3)
    zfirst[3].start()
    advance(0, (2, 3))
    pair_take(4)
    for q in range(QS - 1):
        ring_start(1, 0, q)
    zfirst_take(0)
    ring_start(1, 0, QS - 1)
    for slot in range(5, 8):
        make(slot)
        if slot > 5:
            pair_take(slot - 1)
    pair_take(7)
    for q in range(QS):
        for d in halves(0, q):
            for kind in (2, 1):
                ring_take(0, d, kind, q)
            zcopies[d * QS + q].start()
    for k in range(1, 4):
        zfirst_take(k)
    advance(1, range(4))

    @pl.when(moves)
    def _():
        for copy in stat_remote:
            copy.start()

    for q in range(QS):
        for d in range(2):
            i = d * QS + q
            for kind in (2, 1):
                ring_take(1, d, kind, q)
            here = pl.ds(c * HALF + i * ROWS, ROWS)
            if i == LAST:
                grad[here, :] = acc[7, rows_of(i)]
            else:
                zcopies[i].wait_recv()
                grad[here, :] = acc[7, rows_of(i)] + zbuf[i]
            remote(grad.at[here, :], grad.at[here, :], GRAD, one_r.at[2], sibling).start()

    lane = lax.broadcasted_iota(jnp.int32, (8, 128), 1)

    def stage_start(which, stage, value):
        base = which * 20 + (0, 8, 12)[stage]
        mine = base + places[stage]
        sums[mine] = value
        for _, peer in groups[stage]:
            remote(sums.at[mine], sums.at[mine], SUMS, sum_r.at[which * 3 + stage], peer).start()

    def stage_take(which, stage):
        base = which * 20 + (0, 8, 12)[stage]
        received(sum_r.at[which * 3 + stage], sums.at[pl.ds(base, sizes[stage] - 1)])
        value = sums[base]
        for i in range(1, sizes[stage]):
            value = value + sums[base + i]
        return value

    mask = eye_mask(BLOCK)
    diagonal = diag[0] + diag[1] + diag[2] + diag[3]
    stat_trace = total(jnp.where(eye_mask(TILE), diagonal, 0.0))
    half = grad[pl.ds(c * HALF, HALF), :]
    square = total(half * half)
    stage_start(0, 0, jnp.where(lane == 0, stat_trace, 0.0) + jnp.where(lane == 1, square, 0.0))

    received(one_r.at[2], grad.at[pl.ds(0, HALF), :])
    gsplit = split(grad[...])

    @pl.when(c == 0)
    def _():
        norm[0] = product(gsplit, gsplit, ((1,), (1,)))

    @pl.when(c == 1)
    def _():
        norm[0] = product(gsplit, gsplit, ((0,), (0,)))

    value = stage_take(0, 0)
    stage_start(0, 1, value)
    value = stage_take(0, 1)
    stage_start(0, 2, value)

    @pl.when(stays)
    def _():
        stat_local.wait()

    @pl.when(moves)
    def _():
        received(one_r.at[0], triangle)
        mirror(stat)

    now = DECAY * stat[...] + norm[0]
    stat[...] = now

    square_sum = total(now * now)
    now_trace = total(jnp.where(mask, now, 0.0))
    size = jnp.sqrt(square_sum + EPS)
    first = now * (1.0 / size)
    norm[0] = first
    first_split = split(first)
    second = product(first_split, first_split)
    norm[1] = second
    third = product(split(second), first_split)
    norm[2] = third

    value = stage_take(0, 2)

    @pl.when(stays)
    def _():
        new_stat[...] = stat[...]

    @pl.when(moves)
    def _():
        for copy in back_remote:
            copy.start()

    top = lax.broadcasted_iota(jnp.int32, (8, 128), 0) == 0
    trace_all = total(jnp.where(top & (lane == 0), value, 0.0))
    grad_sq = total(jnp.where(top & (lane == 1), value, 0.0))
    shift = DAMPING * ((DECAY * trace_all + 2.0 * grad_sq) / COUNT)
    frob = jnp.sqrt(square_sum + (2.0 * shift * now_trace + BLOCK * shift * shift) + EPS)
    ratio = size / frob
    e = shift / frob
    gain = 1.0 / jnp.sqrt(jnp.sqrt(frob))
    a = (
        25.0 / 16.0, -5.0 / 16.0 - 3125.0 / 4096.0, 3125.0 / 4096.0, -1250.0 / 4096.0,
        250.0 / 4096.0, -25.0 / 4096.0, 1.0 / 4096.0,
    )
    binomial = (
        (1,), (1, 1), (1, 2, 1), (1, 3, 3, 1), (1, 4, 6, 4, 1), (1, 5, 10, 10, 5, 1), (1, 6, 15, 20, 15, 6, 1),
    )
    coefs = []
    scale = gain
    for j in range(7):
        coef = jnp.full_like(e, a[6] * binomial[6][j])
        for i in range(5, j - 1, -1):
            coef = coef * e + a[i] * binomial[i][j]
        coefs.append(coef * scale)
        scale = scale * ratio
    first, second, third = norm[0], norm[1], norm[2]
    upper = coefs[4] * first + coefs[5] * second + coefs[6] * third
    upper = split(upper)
    low = coefs[1] * first + coefs[2] * second + coefs[3] * third + jnp.where(mask, coefs[0], 0.0)
    for half in (1, 0):
        rows = slice(half * HALF, (half + 1) * HALF)
        roots[c, rows] = low[rows] + product(split(third[rows]), upper)
        part = roots.at[c, pl.ds(half * HALF, HALF)]
        remote(part, part, ROOT, one_r.at[3 + half], sibling).start()
    received(one_r.at[4], grad.at[pl.ds(0, HALF), :])
    left = product(split(roots[0, pl.ds(c * HALF, HALF), :]), gsplit)
    received(one_r.at[3], grad.at[pl.ds(0, HALF), :])
    result = product(split(left), split(roots[1]))
    for i in range(PIECES):
        precond[i] = result[i * ROWS : (i + 1) * ROWS]
    stage_start(1, 0, jnp.where(lane == 0, total(result * result), 0.0))

    def place(xt, zt):
        return (xt * 2 + zt) * 2 + c

    def spread(i, source, xt, zt):
        remote(source, gath.at[place(xt, zt), rows_of(i)], SPREAD, one_r.at[5], sibling).start()

    def gather_copy(phase, d, kind, q):
        index = ((phase * 2 + d) * 3 + kind) * QS + q
        xt = x if kind != 1 else (x + 3 + 2 * d) % 4
        zt = zh if phase == 0 else 1 - zh
        where = gath.at[place(xt, zt), rows_of(d * QS + q)]
        source = precond.at[d * QS + q] if phase == 0 and kind != 1 else where
        return remote(source, where, GRING, ring_r.at[index], to_side(d, kind))

    def gather_take(phase, d, kind, q):
        gather_copy(phase, d, kind, q).wait_recv()
        if kind == 0:
            gather_copy(phase, d, 1, q).start()
        xt = (x + (3 + 2 * d, 2, 1 + 2 * d)[kind]) % 4
        zt = zh if phase == 0 else 1 - zh
        spread(d * QS + q, gath.at[place(xt, zt), rows_of(d * QS + q)], xt, zt)

    mates = [
        remote(precond.at[i], gath.at[place(x, zh), rows_of(i)], GZ, z_r.at[i], zmate) for i in range(PIECES)
    ]
    for kind in (0, 2):
        for q in range(QS):
            for d in range(2):
                if kind == 0:
                    mates[d * QS + q].start()
                gather_copy(0, d, kind, q).start()
    for i in range(PIECES):
        spread(i, precond.at[i], x, zh)
        gath[place(x, zh), rows_of(i)] = precond[i]

    def mate_takes(q):
        for d in range(2):
            i = d * QS + q
            mates[i].wait_recv()
            gather_copy(1, d, 0, q).start()
            gather_copy(1, d, 2, q).start()
            spread(i, gath.at[place(x, 1 - zh), rows_of(i)], x, 1 - zh)

    def takes(phase, kind, qs):
        for q in qs:
            for d in range(2):
                gather_take(phase, d, kind, q)

    takes(0, 0, range(4))
    value = stage_take(1, 0)
    stage_start(1, 1, value)
    mate_takes(0)
    takes(0, 2, range(4))
    value = stage_take(1, 1)
    stage_start(1, 2, value)
    mate_takes(1)

    takes(0, 1, range(4))
    mate_takes(2)
    takes(1, 0, (0, 1))
    takes(1, 2, (0, 1))
    mate_takes(3)
    takes(1, 0, (2,))
    takes(1, 2, (2,))
    takes(1, 1, (0, 1))
    takes(1, 0, (3,))
    takes(1, 2, (3,))

    @pl.when(moves)
    def _():
        received(one_r.at[1], triangle)
        mirror(new_stat)

    takes(1, 1, (2, 3))
    value = stage_take(1, 2)
    prec_sq = total(jnp.where(top & (lane == 0), value, 0.0))
    scale_out[...] = jnp.broadcast_to(jnp.sqrt(grad_sq / (prec_sq + EPS)), (8, 128))

    received(one_r.at[5], acc)
    for kind, size in (
        (PAIR, psend), (RING, ring.at[pl.ds(0, 12 * QS - 3)]), (ZX, ring.at[pl.ds(0, LAST + 4)]), (GRAD, psend.at[0]),
        (SUMS, sums.at[pl.ds(0, 34)]), (ROOT, psend.at[pl.ds(0, 2)]), (GRING, psend.at[pl.ds(0, 6)]),
        (GZ, psend.at[0]), (SPREAD, psend),
    ):
        sent(kind, size)

    @pl.when(moves)
    def _():
        sent(ST, triangle)
        sent(NS, triangle)


def run_main(blocks, act, og, stat):
    dma = pltpu.SemaphoreType.DMA
    ring_count = 12 * QS
    space = pl.BlockSpec
    return pl.pallas_call(
        main_kernel,
        out_shape=(
            jax.ShapeDtypeStruct((16, HALF, BLOCK), f32),
            jax.ShapeDtypeStruct((BLOCK, BLOCK), f32),
            jax.ShapeDtypeStruct((8, 128), f32),
        ),
        in_specs=[
            space(memory_space=pltpu.SMEM), space(memory_space=pltpu.HBM),
            space(memory_space=pltpu.HBM), space(memory_space=pltpu.HBM),
        ],
        out_specs=(space(memory_space=pltpu.VMEM), space(memory_space=pltpu.VMEM), space(memory_space=pltpu.VMEM)),
        scratch_shapes=[
            pltpu.VMEM((HALF, 4096), bf16),
            pltpu.VMEM((HALF, BLOCK), bf16),
            pltpu.VMEM((4, TILE, TILE), f32),
            pltpu.VMEM((8, HALF, BLOCK), f32),
            pltpu.VMEM((8, HALF, BLOCK), f32),
            pltpu.VMEM((8, HALF, BLOCK), f32),
            pltpu.VMEM((ring_count, ROWS, BLOCK), f32),
            pltpu.VMEM((LAST + 4, ROWS, BLOCK), f32),
            pltpu.VMEM((BLOCK, BLOCK), f32),
            pltpu.VMEM((BLOCK, BLOCK), f32),
            pltpu.VMEM((3, BLOCK, BLOCK), f32),
            pltpu.VMEM((2, BLOCK, BLOCK), f32),
            pltpu.VMEM((PIECES, ROWS, BLOCK), f32),
            pltpu.VMEM((40, 8, 128), f32),
            dma((11,)), dma((8,)), dma((ring_count,)), dma((LAST + 4,)), dma((6,)), dma((6,)), dma(()), dma((6,)),
        ],
        compiler_params=pltpu.CompilerParams(
            collective_id=0, has_side_effects=True, vmem_limit_bytes=40 * 1024 * 1024
        ),
        name="shampoo",
    )(blocks, act, og, stat)


def place_kernel(blocks, gath, stat_in, scale, out, stat_out, stage, sem):
    stat_copy = pltpu.make_async_copy(stat_in, stat_out, sem.at[16])
    stat_copy.start()
    copies = []
    for block in range(8):
        pair = jnp.int32(0)
        for p in range(1, 8):
            pair = jnp.where(blocks[0, p] == block, p, pair)
        slot = (pair // 4 + 2 * (pair % 2)) * 2 + (pair // 2) % 2
        for half in range(2):
            i = block * 2 + half
            stage[i] = gath[slot * 2 + half] * scale[0:1, 0:1]
            copy = pltpu.make_async_copy(stage.at[i], out.at[pl.ds(i * HALF, HALF)], sem.at[i])
            copy.start()
            copies.append(copy)
    for copy in copies:
        copy.wait()
    stat_copy.wait()


def run_place(blocks, gath, stat, scale):
    vmem = pl.BlockSpec(memory_space=pltpu.VMEM)
    hbm = pl.BlockSpec(memory_space=pltpu.HBM)
    return pl.pallas_call(
        place_kernel,
        in_specs=[pl.BlockSpec(memory_space=pltpu.SMEM), vmem, vmem, vmem],
        out_specs=(hbm, hbm),
        out_shape=(
            jax.ShapeDtypeStruct((8 * BLOCK, BLOCK), f32),
            jax.ShapeDtypeStruct((BLOCK, BLOCK), f32),
        ),
        scratch_shapes=[pltpu.VMEM((16, HALF, BLOCK), f32), pltpu.SemaphoreType.DMA((17,))],
        compiler_params=pltpu.CompilerParams(vmem_limit_bytes=24 * 1024 * 1024),
        name="place",
    )(blocks, gath, stat, scale)


def per_device(activations, out_grads, statistics, owner_blocks):
    held = [pltpu.with_memory_space_constraint(a, pltpu.HBM) for a in (owner_blocks, activations, out_grads, statistics[0, 0])]
    gath, new_stat, scale = run_main(*held)
    rows, new_stat = run_place(held[0], gath, new_stat, scale)
    return rows, new_stat[None, None]


def solution(mesh):
    return jax.shard_map(
        per_device,
        mesh=mesh,
        in_specs=(P("rep", None), P("rep", "stripe"), P("rep", "stripe", None, None), P("stripe", None)),
        out_specs=(P(None, "stripe"), P("rep", "stripe", None, None)),
        check_vma=False,
    )
```
